32 devices in a mesh: ep: 32 (over z, y, x, core).
Axes of the slice: x: 2, y: 2, z: 4, core: 2. Of those that a mesh axis runs over, the one named last changes fastest.
Arguments:
- x_tok: bfloat16 [16384, 1024], P('ep')
- route_idx: int32 [16384, 8], P('ep')
- gates: bfloat16 [16384, 8], P('ep')
- dy_tok: bfloat16 [16384, 1024], P('ep')
- w_gate: bfloat16 [32, 1024, 512], P('ep')
- w_up: bfloat16 [32, 1024, 512], P('ep')
- w_down: bfloat16 [32, 512, 1024], P('ep')
Outputs:
- output 1: bfloat16 [16384, 1024], P('ep')
- output 2: bfloat16 [16384, 1024], P('ep')
- output 3: float32 [32, 1024, 512], P('ep')
- output 4: float32 [32, 1024, 512], P('ep')
- output 5: float32 [32, 512, 1024], P('ep')
All inputs are finite; a program needn't handle non-finite values.
Results may differ from the reference program's by a relative error of at most 0.0103936.
Values are sent between devices in bfloat16 or wider.
A program may use at most 1 GiB of HBM per device.

```python
import jax
import jax.numpy as jnp
from jax import lax

EXPERTS = 32
TOP_K = 8
MODEL_DIM = 1024
EXPERT_FF = 512
TOK_DEV = 512
EP_SIZE = 32

TOKENS = EP_SIZE * TOK_DEV
SLOT_CAP = 2 * TOK_DEV * TOP_K // (EXPERTS - 2)
HOT_CAP = TOK_DEV // 2
WINDOW = EP_SIZE * max(SLOT_CAP, HOT_CAP)


def source_routes(src_key, count_one, count_two):
    sub_keys = jax.random.split(src_key, 3)
    assigns = TOK_DEV * TOP_K
    remaining = assigns - count_one - count_two
    full_pick = jax.random.randint(sub_keys[0], (), 0, EXPERTS - 2)
    tickets = jax.random.permutation(sub_keys[1], (EXPERTS - 3) * SLOT_CAP)
    others = jnp.sum((tickets < remaining - SLOT_CAP).reshape(EXPERTS - 3, SLOT_CAP), axis=1).astype(jnp.int32)
    places = jnp.arange(EXPERTS - 3) + (jnp.arange(EXPERTS - 3) >= full_pick).astype(jnp.int32)
    middle = jnp.zeros((EXPERTS - 2,), jnp.int32).at[places].set(others).at[full_pick].set(SLOT_CAP)
    counts = jnp.concatenate([count_one[None], middle, count_two[None]]).astype(jnp.int32)
    bounds = jnp.cumsum(counts)
    listing = jnp.searchsorted(bounds, jnp.arange(assigns), side='right').astype(jnp.int32)
    route_table = listing.reshape(TOP_K, TOK_DEV).T
    tok_order = jax.random.permutation(sub_keys[2], TOK_DEV)
    return route_table[tok_order]


def draw_routing(route_key):
    sub_keys = jax.random.split(route_key, 4)
    hot_one = jax.random.randint(sub_keys[0], (EP_SIZE,), HOT_CAP // 4, HOT_CAP + 1)
    hot_two = jax.random.randint(sub_keys[1], (EP_SIZE,), HOT_CAP // 4, HOT_CAP + 1)
    full_src = jax.random.randint(sub_keys[2], (2,), 0, EP_SIZE)
    hot_one = hot_one.at[full_src[0]].set(HOT_CAP)
    hot_two = hot_two.at[full_src[1]].set(HOT_CAP)
    src_keys = jax.random.split(sub_keys[3], EP_SIZE)
    routes = jax.vmap(source_routes)(src_keys, hot_one, hot_two)
    return routes.reshape(TOKENS, TOP_K)


def setup_inputs(seed: int = 0) -> dict:
    root_key = jax.random.key(seed)
    sub_keys = jax.random.split(root_key, 7)
    x_tok = jax.random.normal(sub_keys[0], (TOKENS, MODEL_DIM), jnp.float32)
    route_idx = draw_routing(sub_keys[1])
    gates = jax.random.uniform(sub_keys[2], (TOKENS, TOP_K), jnp.float32, 0.3, 1.0)
    dy_tok = jax.random.normal(sub_keys[3], (TOKENS, MODEL_DIM), jnp.float32)
    w_gate = jax.random.normal(sub_keys[4], (EXPERTS, MODEL_DIM, EXPERT_FF), jnp.float32) * MODEL_DIM ** -0.5
    w_up = jax.random.normal(sub_keys[5], (EXPERTS, MODEL_DIM, EXPERT_FF), jnp.float32) * MODEL_DIM ** -0.5
    w_down = jax.random.normal(sub_keys[6], (EXPERTS, EXPERT_FF, MODEL_DIM), jnp.float32) * EXPERT_FF ** -0.5
    return {'x_tok': x_tok.astype(jnp.bfloat16), 'route_idx': route_idx, 'gates': gates.astype(jnp.bfloat16), 'dy_tok': dy_tok.astype(jnp.bfloat16), 'w_gate': w_gate.astype(jnp.bfloat16), 'w_up': w_up.astype(jnp.bfloat16), 'w_down': w_down.astype(jnp.bfloat16)}


def reference(x_tok, route_idx, gates, dy_tok, w_gate, w_up, w_down):
    flat_route = route_idx.reshape(-1)
    sort_order = jnp.argsort(flat_route, stable=True).astype(jnp.int32)
    counts = jnp.sum((flat_route[:, None] == jnp.arange(EXPERTS)[None, :]).astype(jnp.int32), axis=0)
    starts = jnp.cumsum(counts) - counts
    padded = jnp.concatenate([sort_order, jnp.full((WINDOW,), TOKENS * TOP_K, jnp.int32)])
    flat_gate = gates.reshape(-1)

    def one_expert(acc_pair, expert):
        y_acc, dx_acc = acc_pair
        pick_idx = lax.dynamic_slice(padded, (starts[expert],), (WINDOW,))
        valid_row = jnp.arange(WINDOW) < counts[expert]
        pick_idx = jnp.where(valid_row, pick_idx, TOKENS * TOP_K)
        tok_idx = pick_idx // TOP_K
        gate_rows = jnp.take(flat_gate, pick_idx, mode='fill', fill_value=0).astype(jnp.float32)
        x_rows = jnp.take(x_tok, tok_idx, axis=0, mode='fill', fill_value=0)
        dy_rows = jnp.take(dy_tok, tok_idx, axis=0, mode='fill', fill_value=0)
        gate_mat = w_gate[expert]
        up_mat = w_up[expert]
        down_mat = w_down[expert]
        u_val = jnp.dot(x_rows, gate_mat, preferred_element_type=jnp.float32)
        v_val = jnp.dot(x_rows, up_mat, preferred_element_type=jnp.float32)
        sig_u = jax.nn.sigmoid(u_val)
        act_rows = (u_val * sig_u * v_val).astype(jnp.bfloat16)
        out_rows = jnp.dot(act_rows, down_mat, preferred_element_type=jnp.float32).astype(jnp.bfloat16)
        d_out = (gate_rows[:, None] * dy_rows.astype(jnp.float32)).astype(jnp.bfloat16)
        d_act = jnp.dot(d_out, down_mat.T, preferred_element_type=jnp.float32)
        d_u = (d_act * v_val * sig_u * (1.0 + u_val * (1.0 - sig_u))).astype(jnp.bfloat16)
        d_v = (d_act * u_val * sig_u).astype(jnp.bfloat16)
        dx_rows = (jnp.dot(d_u, gate_mat.T, preferred_element_type=jnp.float32) + jnp.dot(d_v, up_mat.T, preferred_element_type=jnp.float32)).astype(jnp.bfloat16)
        y_acc = y_acc.at[tok_idx].add(gate_rows[:, None] * out_rows.astype(jnp.float32), mode='drop')
        dx_acc = dx_acc.at[tok_idx].add(dx_rows.astype(jnp.float32), mode='drop')
        grads = (jnp.dot(x_rows.T, d_u, preferred_element_type=jnp.float32), jnp.dot(x_rows.T, d_v, preferred_element_type=jnp.float32), jnp.dot(act_rows.T, d_out, preferred_element_type=jnp.float32))
        return (y_acc, dx_acc), grads

    zero_acc = (jnp.zeros((TOKENS, MODEL_DIM), jnp.float32), jnp.zeros((TOKENS, MODEL_DIM), jnp.float32))
    (y_acc, dx_acc), (dw_gate, dw_up, dw_down) = lax.scan(one_expert, zero_acc, jnp.arange(EXPERTS))
    return y_acc.astype(jnp.bfloat16), dx_acc.astype(jnp.bfloat16), dw_gate, dw_up, dw_down
```

```python
import functools

import jax
import jax.numpy as jnp
from jax import lax
from jax.experimental import pallas as pl
from jax.experimental.pallas import tpu as pltpu
from jax.sharding import Mesh, PartitionSpec as P

F32 = jnp.float32
BF16 = jnp.bfloat16
TILE = 256
WIN = 128
ALIGN = 16
GROUP = 2
ROWS = 256


def dot(a, b, dims=((1,), (0,))):
    return lax.dot_general(a, b, (dims, ((), ())), preferred_element_type=F32)


def expert_kernel(
    n_tiles, n_exp, cum_ref, off_ref, row_ref, col_ref, x_ref, dy_ref, wg_ref, wu_ref, wd_ref,
    y_ref, dx_ref, dwg_ref, dwu_ref, dwd_ref, x_rows, g_rows, o_win, d_win,
):
    step = pl.program_id(0)

    def span(tile, exp):
        lo = cum_ref[tile * n_exp + exp]
        hi = cum_ref[(tile + 1) * n_exp + exp]
        start = (lo // ALIGN) * ALIGN
        return lo, hi, start

    @pl.when(step < n_tiles)
    def _gather():
        tile = step

        def window(exp, lo, hi, start):
            place = (lax.broadcasted_iota(jnp.int32, (WIN, TILE), 0) + start).astype(F32)
            hit = row_ref[0, exp : exp + 1, :] == place
            take = jnp.where(hit, 1.0, 0.0).astype(BF16)
            scale = jnp.where(hit, row_ref[0, n_exp + exp : n_exp + exp + 1, :], 0.0).astype(BF16)
            row = lax.broadcasted_iota(jnp.int32, (WIN, 1), 0) + start
            mine = (row >= lo) & (row < hi)
            here = pl.ds(pl.multiple_of(off_ref[exp] + start, ALIGN), WIN)
            x_rows[here, :] = jnp.where(mine, dot(take, x_ref[...]), x_rows[here, :].astype(F32)).astype(BF16)
            g_rows[here, :] = jnp.where(mine, dot(scale, dy_ref[...]), g_rows[here, :].astype(F32)).astype(BF16)

        for exp in range(n_exp):
            lo, hi, start = span(tile, exp)
            window(exp, lo, hi, start)

            @pl.when(hi > start + WIN)
            def _more():
                @pl.loop(1, (hi - start + WIN - 1) // WIN)
                def _(w):
                    window(exp, lo, hi, start + w * WIN)

    @pl.when((step >= n_tiles) & (step < n_tiles + n_exp))
    def _expert():
        exp = step - n_tiles
        count = cum_ref[n_tiles * n_exp + exp]
        base = off_ref[exp]
        dwg_ref[...] = jnp.zeros_like(dwg_ref)
        dwu_ref[...] = jnp.zeros_like(dwu_ref)
        dwd_ref[...] = jnp.zeros_like(dwd_ref)

        @pl.loop(0, (count + ROWS - 1) // ROWS)
        def _(b):
            here = pl.ds(pl.multiple_of(base + b * ROWS, ALIGN), ROWS)
            live = lax.broadcasted_iota(jnp.int32, (ROWS, 1), 0) < count - b * ROWS
            x_old = x_rows[here, :]
            g_old = g_rows[here, :]
            x_blk = jnp.where(live, x_old, jnp.zeros_like(x_old))
            g_blk = jnp.where(live, g_old, jnp.zeros_like(g_old))
            u = dot(x_blk, wg_ref[0])
            v = dot(x_blk, wu_ref[0])
            s = jax.nn.sigmoid(u)
            act = (u * s * v).astype(BF16)
            da = dot(g_blk, wd_ref[0], ((1,), (1,)))
            du = (da * v * s * (1.0 + u * (1.0 - s))).astype(BF16)
            dv = (da * u * s).astype(BF16)
            out = dot(act, wd_ref[0]).astype(BF16)
            dxr = (dot(du, wg_ref[0], ((1,), (1,))) + dot(dv, wu_ref[0], ((1,), (1,)))).astype(BF16)
            dwd_ref[0] += dot(act, g_blk, ((0,), (0,)))
            g_rows[here, :] = jnp.where(live, dxr, g_rows[here, :])
            dwg_ref[0] += dot(x_blk, du, ((0,), (0,)))
            dwu_ref[0] += dot(x_blk, dv, ((0,), (0,)))
            x_rows[here, :] = jnp.where(live, out, x_rows[here, :])

    @pl.when(step >= n_tiles + n_exp)
    def _scatter():
        tile = step - n_tiles - n_exp

        def window(exp, lo, hi, start):
            place = (lax.broadcasted_iota(jnp.int32, (TILE, WIN), 1) + start).astype(F32)
            hit = col_ref[:, exp : exp + 1] == place
            put = jnp.where(hit, 1.0, 0.0).astype(BF16)
            scale = jnp.where(hit, col_ref[:, n_exp + exp : n_exp + exp + 1], 0.0).astype(BF16)
            row = lax.broadcasted_iota(jnp.int32, (WIN, 1), 0) + start
            mine = (row >= lo) & (row < hi)
            here = pl.ds(pl.multiple_of(off_ref[exp] + start, ALIGN), WIN)
            o_blk = x_rows[here, :]
            d_blk = g_rows[here, :]
            o_blk = jnp.where(mine, o_blk, jnp.zeros_like(o_blk))
            d_blk = jnp.where(mine, d_blk, jnp.zeros_like(d_blk))
            return put, scale, o_blk, d_blk

        for part in range(n_exp // GROUP):
            puts, scales = [], []
            for i in range(GROUP):
                exp = part * GROUP + i
                lo, hi, start = span(tile, exp)
                put, scale, o_blk, d_blk = window(exp, lo, hi, start)
                puts.append(put)
                scales.append(scale)
                o_win[i * WIN : (i + 1) * WIN, :] = o_blk
                d_win[i * WIN : (i + 1) * WIN, :] = d_blk
            y_add = dot(jnp.concatenate(scales, axis=1), o_win[...])
            dx_add = dot(jnp.concatenate(puts, axis=1), d_win[...])
            y_ref[...] = y_add if part == 0 else y_ref[...] + y_add
            dx_ref[...] = dx_add if part == 0 else dx_ref[...] + dx_add
        for exp in range(n_exp):
            lo, hi, start = span(tile, exp)

            @pl.when(hi > start + WIN)
            def _more():
                @pl.loop(1, (hi - start + WIN - 1) // WIN)
                def _(w):
                    put, scale, o_blk, d_blk = window(exp, lo, hi, start + w * WIN)
                    y_ref[...] += dot(scale, o_blk)
                    dx_ref[...] += dot(put, d_blk)


def expert_layer(cum, off, table, x_col, dy_col, w_gate, w_up, w_down, cap):
    tokens, dim = x_col.shape
    n_exp, _, ff = w_gate.shape
    n_tiles = tokens // TILE
    total = n_exp * (-(-cap // ALIGN) * ALIGN) + ROWS
    by_tile = table.reshape(n_tiles, TILE, 2 * n_exp).transpose(0, 2, 1)
    first = lambda i: jnp.minimum(i, n_tiles - 1)
    middle = lambda i: jnp.clip(i - n_tiles, 0, n_exp - 1)
    last = lambda i: jnp.maximum(i - n_tiles - n_exp, 0)
    rows = pl.BlockSpec((1, 2 * n_exp, TILE), lambda i, *_: (first(i), 0, 0))
    cols = pl.BlockSpec((TILE, 2 * n_exp), lambda i, *_: (last(i), 0))
    toks_in = pl.BlockSpec((TILE, dim), lambda i, *_: (first(i), 0))
    toks_out = pl.BlockSpec((TILE, dim), lambda i, *_: (last(i), 0))
    wide = pl.BlockSpec((1, dim, ff), lambda i, *_: (middle(i), 0, 0))
    tall = pl.BlockSpec((1, ff, dim), lambda i, *_: (middle(i), 0, 0))
    return pl.pallas_call(
        functools.partial(expert_kernel, n_tiles, n_exp),
        grid_spec=pltpu.PrefetchScalarGridSpec(
            num_scalar_prefetch=2,
            grid=(2 * n_tiles + n_exp,),
            in_specs=[rows, cols, toks_in, toks_in, wide, wide, tall],
            out_specs=[toks_out, toks_out, wide, wide, tall],
            scratch_shapes=[
                pltpu.VMEM((total, dim), BF16),
                pltpu.VMEM((total, dim), BF16),
                pltpu.VMEM((GROUP * WIN, dim), BF16),
                pltpu.VMEM((GROUP * WIN, dim), BF16),
            ],
        ),
        out_shape=[
            jax.ShapeDtypeStruct((tokens, dim), F32),
            jax.ShapeDtypeStruct((tokens, dim), F32),
            jax.ShapeDtypeStruct(w_gate.shape, F32),
            jax.ShapeDtypeStruct(w_up.shape, F32),
            jax.ShapeDtypeStruct(w_down.shape, F32),
        ],
        compiler_params=pltpu.CompilerParams(
            dimension_semantics=("arbitrary",), vmem_limit_bytes=67_000_000,
        ),
        cost_estimate=pl.CostEstimate(flops=60_000_000_000, bytes_accessed=120_000_000, transcendentals=3_000_000),
        name="experts",
    )(cum, off, by_tile, table, x_col, dy_col, w_gate, w_up, w_down)


def plan(route, gates, first_exp, n_exp):
    hits = route[:, :, None] == first_exp + jnp.arange(n_exp, dtype=jnp.int32)[None, None, :]
    member = jnp.any(hits, axis=1)
    gate = jnp.sum(jnp.where(hits, gates[:, :, None].astype(F32), 0.0), axis=1)
    tiles = member.reshape(-1, TILE, n_exp)
    per_tile = jnp.sum(tiles.astype(jnp.int32), axis=1)
    cum = jnp.concatenate([jnp.zeros((1, n_exp), jnp.int32), jnp.cumsum(per_tile, axis=0)])
    lower = jnp.tril(jnp.ones((TILE, TILE), BF16), -1)
    inner = jnp.einsum('ab,ibe->iae', lower, tiles.astype(BF16), preferred_element_type=F32).astype(jnp.int32)
    rank = jnp.where(tiles, inner + cum[:-1, None, :], -(1 << 20)).reshape(-1, n_exp)
    count = cum[-1]
    padded = (count + ALIGN - 1) // ALIGN * ALIGN
    off = jnp.cumsum(padded) - padded
    return cum.reshape(-1), off.astype(jnp.int32), jnp.concatenate([rank.astype(F32), gate], axis=1)


def solution(mesh):
    n_dev = mesh.devices.size
    depth = n_dev // 8
    grid = Mesh(mesh.devices.reshape(depth, 2, 2, 2), ('z', 'y', 'x', 'c'))
    plane = ('y', 'x', 'c')
    spec = P(('z', 'y', 'x', 'c'))

    def local_step(x_tok, route_idx, gates, dy_tok, w_gate, w_up, w_down):
        tok_loc, top_k = route_idx.shape
        cap = depth * (2 * tok_loc * top_k // (n_dev * w_gate.shape[0] - 2))
        n_exp = 8 * w_gate.shape[0]
        gather_z = lambda a: lax.all_gather(a, 'z', axis=0, tiled=True)
        gather_p = lambda a: lax.all_gather(a, plane, axis=0, tiled=True)
        route = gather_z(route_idx)
        gate_all = gather_z(gates)
        cum, off, table = plan(route, gate_all, lax.axis_index('z') * n_exp, n_exp)
        x_col = gather_z(x_tok)
        dy_col = gather_z(dy_tok)
        y, dx, g_gate, g_up, g_down = expert_layer(
            cum, off, table, x_col, dy_col, gather_p(w_gate), gather_p(w_up), gather_p(w_down), cap
        )
        sum_z = lambda a: lax.psum_scatter(a, 'z', scatter_dimension=0, tiled=True)
        sum_p = lambda a: lax.psum_scatter(a, plane, scatter_dimension=0, tiled=True)
        return sum_z(y).astype(BF16), sum_z(dx).astype(BF16), sum_p(g_gate), sum_p(g_up), sum_p(g_down)

    return jax.shard_map(local_step, mesh=grid, in_specs=(spec,) * 7, out_specs=(spec,) * 5, check_vma=False)
```

```python
import functools

import jax
import jax.numpy as jnp
from jax import lax
from jax.experimental import pallas as pl
from jax.experimental.pallas import tpu as pltpu
from jax.sharding import Mesh, PartitionSpec as P

F32 = jnp.float32
BF16 = jnp.bfloat16
TILE = 256
WIN = 128
ALIGN = 16
GROUP = 2
ROWS = 256


def dot(a, b, dims=((1,), (0,))):
    return lax.dot_general(a, b, (dims, ((), ())), preferred_element_type=F32)


MESH = pl.DeviceIdType.MESH


def hop(src, dst, send_sem, recv_sem, **where):
    return pltpu.make_async_remote_copy(
        src_ref=src, dst_ref=dst, send_sem=send_sem, recv_sem=recv_sem, device_id=where, device_id_type=MESH
    )


def meet(depth, z, y, x, c):
    barrier = pltpu.get_barrier_semaphore()
    for where in ({'y': 1 - y}, {'x': 1 - x}, {'c': 1 - c}):
        pl.semaphore_signal(barrier, inc=1, device_id=where, device_id_type=MESH)

    @pl.when(z > 0)
    def _():
        pl.semaphore_signal(barrier, inc=1, device_id={'z': z - 1}, device_id_type=MESH)

    @pl.when(z < depth - 1)
    def _():
        pl.semaphore_signal(barrier, inc=1, device_id={'z': z + 1}, device_id_type=MESH)

    inner = (z > 0) & (z < depth - 1)

    @pl.when(inner)
    def _():
        pl.semaphore_wait(barrier, 5)

    @pl.when(jnp.logical_not(inner))
    def _():
        pl.semaphore_wait(barrier, 4)


def make_plan(experts, route_ref, gate_ref, plan):
    top_k, toks = route_ref.shape
    route = route_ref[...]
    gates = gate_ref[...]
    below = lax.broadcasted_iota(jnp.int32, (TILE, TILE), 0) < lax.broadcasted_iota(jnp.int32, (TILE, TILE), 1)
    below = jnp.where(below, 1.0, 0.0).astype(BF16)
    ones = jnp.ones((8, TILE), BF16)
    ids = lax.broadcasted_iota(jnp.int32, (experts, toks), 0)
    member = jnp.zeros((experts, toks), F32)
    gate = jnp.zeros((experts, toks), F32)
    for k in range(top_k):
        hit = jnp.broadcast_to(route[k : k + 1, :], (experts, toks)) == ids
        member = jnp.where(hit, 1.0, member)
        gate = jnp.where(hit, jnp.broadcast_to(gates[k : k + 1, :], (experts, toks)), gate)
    plan[experts : 2 * experts, :] = gate
    plan[2 * experts :, :] = jnp.zeros((8, toks), F32)
    for t in range(toks // TILE):
        cols = slice(t * TILE, (t + 1) * TILE)
        part = member[:, cols]
        rank = dot(part.astype(BF16), below)
        plan[:experts, cols] = jnp.where(part > 0.5, rank, -4096.0)
        plan[2 * experts + t : 2 * experts + t + 1, :experts] = dot(ones, part.astype(BF16), ((1,), (1,)))[:1]


def spread_kernel(
    depth, experts, x_ref, dy_ref, route_ref, gate_ref, wg_ref, wu_ref, wd_ref,
    x_out, dy_out, plan_out, wg_out, wu_out, wd_out,
    stage_t, stage_w, stage_d, plan, own_sem, z_send, z_recv, p_send, p_recv, c_send, c_recv,
):
    z, y, x, c = (lax.axis_index(a) for a in 'zyxc')
    slot = lambda yy, xx: yy * 4 + xx * 2 + c
    own, by_x, by_y, far = slot(y, x), slot(y, 1 - x), slot(1 - y, x), slot(1 - y, 1 - x)
    weights = ((wg_ref, wg_out), (wu_ref, wu_out), (wd_ref, wd_out))
    arrays = ((x_ref, x_out), (plan, plan_out), (dy_ref, dy_out))
    sent = []

    def half(ref, where, h):
        rows = ref.shape[1] // 2
        return ref.at[where, pl.ds(h * rows, rows), :]

    def own_half(part, h, side):
        src, out = weights[part]
        where = {'x': 1 - x} if side == 0 else {'y': 1 - y}
        return hop(half(src, 0, h), half(out, own, h), p_send.at[side, part, h], p_recv.at[side, part, h], **where)

    def onward(part, h):
        at = half(weights[part][1], by_x if h == 0 else by_y, h)
        where = {'y': 1 - y} if h == 0 else {'x': 1 - x}
        return hop(at, at, p_send.at[2, part, h], p_recv.at[2, part, h], **where)

    def landed(part, h, kind):
        at = half(weights[part][1], (by_x, by_y, far)[kind], h)
        hop(at, at, p_send.at[kind, part, h], p_recv.at[kind, part, h], c=1 - c).wait_recv()

    def across(part, h, kind):
        at = half(weights[part][1], (by_x, by_y, far)[kind], h)
        return hop(at, at, c_send.at[kind, part, h], c_recv.at[kind, part, h], c=1 - c)

    def across_own(part, h):
        src, out = weights[part]
        return hop(half(src, 0, h), half(out, own, h), c_send.at[3, part, h], c_recv.at[3, part, h], c=1 - c)

    def crossed(part, h, kind):
        twin = lambda yy, xx: yy * 4 + xx * 2 + 1 - c
        where = (twin(y, 1 - x), twin(1 - y, x), twin(1 - y, 1 - x), twin(y, x))[kind]
        at = half(weights[part][1], where, h)
        hop(at, at, c_send.at[kind, part, h], c_recv.at[kind, part, h], c=1 - c).wait_recv()

    def go(copy):
        copy.start()
        sent.append((None, copy))

    def along(k, dist, up):
        src, out = arrays[k]
        at = out.at[z - dist if up else z + dist]
        side = 0 if up else 1
        return hop(src if dist == 0 else at, at, z_send.at[side, k, dist], z_recv.at[side, k, dist], z=z + 1 if up else z - 1)

    def start_along(k, dist):
        for up in (True, False):
            cond = (z >= dist) & (z < depth - 1) if up else (z + dist < depth) & (z > 0)

            @pl.when(cond)
            def _(up=up):
                along(k, dist, up).start()

            sent.append((cond, along(k, dist, up)))

    def await_along(k, dist):
        for up in (True, False):
            @pl.when(z > dist if up else z + dist + 1 < depth)
            def _(up=up):
                at = arrays[k][1].at[z - dist - 1 if up else z + dist + 1]
                side = 0 if up else 1
                hop(at, at, z_send.at[side, k, dist], z_recv.at[side, k, dist], c=1 - c).wait_recv()

        if dist + 1 < depth - 1:
            start_along(k, dist + 1)

    copies = []
    for i, (src, buf, out) in enumerate((
        (x_ref, stage_t.at[0], x_out.at[z]), (dy_ref, stage_t.at[1], dy_out.at[z]),
        (wg_ref.at[0], stage_w.at[0], wg_out.at[own]), (wu_ref.at[0], stage_w.at[1], wu_out.at[own]),
        (wd_ref.at[0], stage_d, wd_out.at[own]),
    )):
        copies.append((pltpu.make_async_copy(src, buf, own_sem.at[i]), pltpu.make_async_copy(buf, out, own_sem.at[i])))
        copies[-1][0].start()

    meet(depth, z, y, x, c)
    start_along(0, 0)
    for part in range(3):
        go(own_half(part, 0, 0))
        go(own_half(part, 1, 1))
    for part in range(3):
        go(own_half(part, 1, 0))
        go(own_half(part, 0, 1))
    for part in range(3):
        for h in range(2):
            go(across_own(part, h))
    make_plan(experts, route_ref, gate_ref, plan)
    start_along(1, 0)
    start_along(2, 0)
    copies.append((None, pltpu.make_async_copy(plan, plan_out.at[z], own_sem.at[5])))
    for i, (load, store) in enumerate(copies):
        if load is not None:
            load.wait()
        store.start()

    def relay(part, h):
        landed(part, h, h)
        go(onward(part, h))
        go(across(part, h, h))

    def relay_twin(part, h):
        landed(part, h, 1 - h)
        go(across(part, h, 1 - h))

    for part in range(2):
        relay(part, 0)
        relay(part, 1)
    await_along(0, 0)
    await_along(1, 0)
    relay(2, 0)
    relay(2, 1)
    await_along(2, 0)
    for part in range(3):
        relay_twin(part, 1)
        relay_twin(part, 0)
    await_along(0, 1)
    await_along(1, 1)
    for part in range(3):
        for h in range(2):
            landed(part, h, 2)
            go(across(part, h, 2))
    await_along(2, 1)
    for k in range(3):
        await_along(k, 2)
    for part in range(3):
        for h in range(2):
            for kind in range(4):
                crossed(part, h, kind)
    for cond, copy in sent:
        if cond is None:
            copy.wait_send()
        else:
            @pl.when(cond)
            def _(copy=copy):
                copy.wait_send()
    for _, store in copies:
        store.wait()


def spread(depth, experts, x_tok, dy_tok, route, gate, w_gate, w_up, w_down):
    toks, dim = x_tok.shape
    ff = w_down.shape[1]
    any_space = pl.BlockSpec(memory_space=pl.ANY)
    vmem = pl.BlockSpec(memory_space=pltpu.VMEM)
    rows = 2 * experts + 8
    shape = jax.ShapeDtypeStruct
    dma = pltpu.SemaphoreType.DMA
    return pl.pallas_call(
        functools.partial(spread_kernel, depth, experts),
        in_specs=[any_space, any_space, vmem, vmem, any_space, any_space, any_space],
        out_specs=[any_space] * 6,
        out_shape=[
            shape((depth, toks, dim), BF16), shape((depth, toks, dim), BF16), shape((depth, rows, toks), F32),
            shape((8, dim, ff), BF16), shape((8, dim, ff), BF16), shape((8, ff, dim), BF16),
        ],
        scratch_shapes=[
            pltpu.VMEM((2, toks, dim), BF16), pltpu.VMEM((2, dim, ff), BF16), pltpu.VMEM((ff, dim), BF16),
            pltpu.VMEM((rows, toks), F32), dma((6,)), dma((2, 3, depth)), dma((2, 3, depth)),
            dma((3, 3, 2)), dma((3, 3, 2)), dma((4, 3, 2)), dma((4, 3, 2)),
        ],
        compiler_params=pltpu.CompilerParams(collective_id=0, has_side_effects=True),
        name="spread",
    )(x_tok, dy_tok, route, gate, w_gate, w_up, w_down)


def expert_kernel(
    n_tiles, n_exp, count_ref, place_ref, rank_ref, gate_ref, x_ref, dy_ref, wg_ref, wu_ref, wd_ref,
    y_ref, dx_ref, dwg_ref, dwu_ref, dwd_ref, x_rows, g_rows, o_win, d_win, cum_ref, off_ref,
):
    step = pl.program_id(0)

    @pl.when(step == 0)
    def _count():
        base = jnp.int32(0)
        for exp in range(n_exp):
            run = jnp.int32(0)
            cum_ref[exp] = run
            for tile in range(n_tiles):
                run += count_ref[tile * n_exp + exp]
                cum_ref[(tile + 1) * n_exp + exp] = run
            off_ref[exp] = base
            base += ((run + ALIGN - 1) // ALIGN) * ALIGN

    def span(tile, exp):
        lo = cum_ref[tile * n_exp + exp]
        hi = cum_ref[(tile + 1) * n_exp + exp]
        start = (lo // ALIGN) * ALIGN
        return lo, hi, start

    @pl.when(step < n_tiles)
    def _gather():
        tile = step

        def window(exp, lo, hi, start):
            first = (start - lo).astype(F32)
            place = lax.broadcasted_iota(jnp.int32, (WIN, TILE), 0).astype(F32) + first
            hit = rank_ref[0, exp : exp + 1, :] == place
            take = jnp.where(hit, 1.0, 0.0).astype(BF16)
            scale = jnp.where(hit, gate_ref[0, exp : exp + 1, :], 0.0).astype(BF16)
            row = lax.broadcasted_iota(jnp.int32, (WIN, 1), 0) + start
            mine = (row >= lo) & (row < hi)
            here = pl.ds(pl.multiple_of(off_ref[exp] + start, ALIGN), WIN)
            x_rows[here, :] = jnp.where(mine, dot(take, x_ref[...]), x_rows[here, :].astype(F32)).astype(BF16)
            g_rows[here, :] = jnp.where(mine, dot(scale, dy_ref[...]), g_rows[here, :].astype(F32)).astype(BF16)

        for exp in range(n_exp):
            lo, hi, start = span(tile, exp)
            window(exp, lo, hi, start)

            @pl.when(hi > start + WIN)
            def _more():
                @pl.loop(1, (hi - start + WIN - 1) // WIN)
                def _(w):
                    window(exp, lo, hi, start + w * WIN)

    @pl.when((step >= n_tiles) & (step < n_tiles + n_exp))
    def _expert():
        exp = step - n_tiles
        count = cum_ref[n_tiles * n_exp + exp]
        base = off_ref[exp]
        dwg_ref[...] = jnp.zeros_like(dwg_ref)
        dwu_ref[...] = jnp.zeros_like(dwu_ref)
        dwd_ref[...] = jnp.zeros_like(dwd_ref)

        @pl.loop(0, (count + ROWS - 1) // ROWS)
        def _(b):
            here = pl.ds(pl.multiple_of(base + b * ROWS, ALIGN), ROWS)
            live = lax.broadcasted_iota(jnp.int32, (ROWS, 1), 0) < count - b * ROWS
            x_old = x_rows[here, :]
            g_old = g_rows[here, :]
            x_blk = jnp.where(live, x_old, jnp.zeros_like(x_old))
            g_blk = jnp.where(live, g_old, jnp.zeros_like(g_old))
            u = dot(x_blk, wg_ref[0])
            v = dot(x_blk, wu_ref[0])
            s = jax.nn.sigmoid(u)
            act = (u * s * v).astype(BF16)
            da = dot(g_blk, wd_ref[0], ((1,), (1,)))
            du = (da * v * s * (1.0 + u * (1.0 - s))).astype(BF16)
            dv = (da * u * s).astype(BF16)
            out = dot(act, wd_ref[0]).astype(BF16)
            dxr = (dot(du, wg_ref[0], ((1,), (1,))) + dot(dv, wu_ref[0], ((1,), (1,)))).astype(BF16)
            dwd_ref[0] += dot(act, g_blk, ((0,), (0,)))
            g_rows[here, :] = jnp.where(live, dxr, g_rows[here, :])
            dwg_ref[0] += dot(x_blk, du, ((0,), (0,)))
            dwu_ref[0] += dot(x_blk, dv, ((0,), (0,)))
            x_rows[here, :] = jnp.where(live, out, x_rows[here, :])

    @pl.when(step >= n_tiles + n_exp)
    def _scatter():
        tile = step - n_tiles - n_exp

        def window(exp, lo, hi, start):
            first = (start - lo).astype(F32)
            place = lax.broadcasted_iota(jnp.int32, (WIN, TILE), 0).astype(F32) + first
            hit = rank_ref[0, exp : exp + 1, :] == place
            put = jnp.where(hit, 1.0, 0.0).astype(BF16)
            scale = jnp.where(hit, gate_ref[0, exp : exp + 1, :], 0.0).astype(BF16)
            row = lax.broadcasted_iota(jnp.int32, (WIN, 1), 0) + start
            mine = (row >= lo) & (row < hi)
            here = pl.ds(pl.multiple_of(off_ref[exp] + start, ALIGN), WIN)
            o_blk = x_rows[here, :]
            d_blk = g_rows[here, :]
            o_blk = jnp.where(mine, o_blk, jnp.zeros_like(o_blk))
            d_blk = jnp.where(mine, d_blk, jnp.zeros_like(d_blk))
            return put, scale, o_blk, d_blk

        for part in range(n_exp // GROUP):
            puts, scales = [], []
            for i in range(GROUP):
                exp = part * GROUP + i
                lo, hi, start = span(tile, exp)
                put, scale, o_blk, d_blk = window(exp, lo, hi, start)
                puts.append(put)
                scales.append(scale)
                o_win[i * WIN : (i + 1) * WIN, :] = o_blk
                d_win[i * WIN : (i + 1) * WIN, :] = d_blk
            y_add = dot(jnp.concatenate(scales, axis=0), o_win[...], ((0,), (0,)))
            dx_add = dot(jnp.concatenate(puts, axis=0), d_win[...], ((0,), (0,)))
            y_ref[...] = y_add if part == 0 else y_ref[...] + y_add
            dx_ref[...] = dx_add if part == 0 else dx_ref[...] + dx_add
        for exp in range(n_exp):
            lo, hi, start = span(tile, exp)

            @pl.when(hi > start + WIN)
            def _more():
                @pl.loop(1, (hi - start + WIN - 1) // WIN)
                def _(w):
                    put, scale, o_blk, d_blk = window(exp, lo, hi, start + w * WIN)
                    y_ref[...] += dot(scale, o_blk, ((0,), (0,)))
                    dx_ref[...] += dot(put, d_blk, ((0,), (0,)))


def expert_layer(counts, place, plan_col, x_col, dy_col, w_gate, w_up, w_down, cap, n_dev):
    tokens, dim = x_col.shape
    n_exp, _, ff = w_gate.shape
    n_tiles = tokens // TILE
    total = n_exp * (-(-cap // ALIGN) * ALIGN) + ROWS
    per = plan_col.shape[2] // TILE
    first = lambda i: jnp.minimum(i, n_tiles - 1)
    middle = lambda i: jnp.clip(i - n_tiles, 0, n_exp - 1)
    last = lambda i: jnp.maximum(i - n_tiles - n_exp, 0)
    tile_of = lambda i: jnp.where(i < n_tiles, i, last(i))
    plan_at = lambda part: lambda i, counts, place: (tile_of(i) // per, place[0] + part, tile_of(i) % per)
    ranks = pl.BlockSpec((1, n_exp, TILE), plan_at(0))
    gates = pl.BlockSpec((1, n_exp, TILE), plan_at(n_dev // n_exp))
    toks_in = pl.BlockSpec((TILE, dim), lambda i, *_: (first(i), 0))
    toks_out = pl.BlockSpec((TILE, dim), lambda i, *_: (last(i), 0))
    wide = pl.BlockSpec((1, dim, ff), lambda i, *_: (middle(i), 0, 0))
    tall = pl.BlockSpec((1, ff, dim), lambda i, *_: (middle(i), 0, 0))
    return pl.pallas_call(
        functools.partial(expert_kernel, n_tiles, n_exp),
        grid_spec=pltpu.PrefetchScalarGridSpec(
            num_scalar_prefetch=2,
            grid=(2 * n_tiles + n_exp,),
            in_specs=[ranks, gates, toks_in, toks_in, wide, wide, tall],
            out_specs=[toks_out, toks_out, wide, wide, tall],
            scratch_shapes=[
                pltpu.VMEM((total, dim), BF16),
                pltpu.VMEM((total, dim), BF16),
                pltpu.VMEM((GROUP * WIN, dim), BF16),
                pltpu.VMEM((GROUP * WIN, dim), BF16),
                pltpu.SMEM(((n_tiles + 1) * n_exp,), jnp.int32),
                pltpu.SMEM((n_exp,), jnp.int32),
            ],
        ),
        out_shape=[
            jax.ShapeDtypeStruct((tokens, dim), F32),
            jax.ShapeDtypeStruct((tokens, dim), F32),
            jax.ShapeDtypeStruct(w_gate.shape, F32),
            jax.ShapeDtypeStruct(w_up.shape, F32),
            jax.ShapeDtypeStruct(w_down.shape, F32),
        ],
        compiler_params=pltpu.CompilerParams(
            dimension_semantics=("arbitrary",), vmem_limit_bytes=67_000_000,
        ),
        cost_estimate=pl.CostEstimate(flops=60_000_000_000, bytes_accessed=120_000_000, transcendentals=3_000_000),
        name="experts",
    )(counts, place, plan_col, plan_col, x_col, dy_col, w_gate, w_up, w_down)


def solution(mesh):
    n_dev = mesh.devices.size
    depth = n_dev // 8
    grid = Mesh(mesh.devices.reshape(depth, 2, 2, 2), ('z', 'y', 'x', 'c'))
    plane = ('y', 'x', 'c')
    spec = P(('z', 'y', 'x', 'c'))

    def local_step(x_tok, route_idx, gates, dy_tok, w_gate, w_up, w_down):
        tok_loc, top_k = route_idx.shape
        cap = depth * (2 * tok_loc * top_k // (n_dev * w_gate.shape[0] - 2))
        n_exp = 8 * w_gate.shape[0]
        x_col, dy_col, plan_col, wg_all, wu_all, wd_all = spread(
            depth, n_dev, x_tok, dy_tok, route_idx.T, gates.T.astype(F32), w_gate, w_up, w_down
        )
        place = lax.axis_index('z')
        per = tok_loc // TILE
        counts = lax.dynamic_slice(plan_col[:, 2 * n_dev : 2 * n_dev + per, :n_dev], (0, 0, place * n_exp), (depth, per, n_exp))
        y, dx, g_gate, g_up, g_down = expert_layer(
            counts.reshape(-1).astype(jnp.int32), place.reshape(1), plan_col, x_col.reshape(-1, x_tok.shape[1]),
            dy_col.reshape(-1, x_tok.shape[1]), wg_all, wu_all, wd_all, cap, n_dev
        )
        sum_z = lambda a: lax.psum_scatter(a, 'z', scatter_dimension=0, tiled=True)
        sum_p = lambda a: lax.psum_scatter(a, plane, scatter_dimension=0, tiled=True)
        return sum_z(y).astype(BF16), sum_z(dx).astype(BF16), sum_p(g_gate), sum_p(g_up), sum_p(g_down)

    return jax.shard_map(local_step, mesh=grid, in_specs=(spec,) * 7, out_specs=(spec,) * 5, check_vma=False)
```

```python
import functools

import jax
import jax.numpy as jnp
from jax import lax
from jax.experimental import pallas as pl
from jax.experimental.pallas import tpu as pltpu
from jax.sharding import Mesh, PartitionSpec as P

F32 = jnp.float32
BF16 = jnp.bfloat16
TILE = 256
WIN = 128
ALIGN = 16
GROUP = 2
ROWS = 256


def dot(a, b, dims=((1,), (0,))):
    return lax.dot_general(a, b, (dims, ((), ())), preferred_element_type=F32)


MESH = pl.DeviceIdType.MESH


def hop(src, dst, send_sem, recv_sem, **where):
    return pltpu.make_async_remote_copy(
        src_ref=src, dst_ref=dst, send_sem=send_sem, recv_sem=recv_sem, device_id=where, device_id_type=MESH
    )


def meet(depth, z, y, x, c):
    barrier = pltpu.get_barrier_semaphore()
    for where in ({'y': 1 - y}, {'x': 1 - x}, {'c': 1 - c}):
        pl.semaphore_signal(barrier, inc=1, device_id=where, device_id_type=MESH)

    @pl.when(z > 0)
    def _():
        pl.semaphore_signal(barrier, inc=1, device_id={'z': z - 1}, device_id_type=MESH)

    @pl.when(z < depth - 1)
    def _():
        pl.semaphore_signal(barrier, inc=1, device_id={'z': z + 1}, device_id_type=MESH)

    inner = (z > 0) & (z < depth - 1)

    @pl.when(inner)
    def _():
        pl.semaphore_wait(barrier, 5)

    @pl.when(jnp.logical_not(inner))
    def _():
        pl.semaphore_wait(barrier, 4)


def make_plan(experts, route_ref, gate_ref, plan):
    top_k, toks = route_ref.shape
    route = route_ref[...]
    gates = gate_ref[...]
    below = lax.broadcasted_iota(jnp.int32, (TILE, TILE), 0) < lax.broadcasted_iota(jnp.int32, (TILE, TILE), 1)
    below = jnp.where(below, 1.0, 0.0).astype(BF16)
    ones = jnp.ones((8, TILE), BF16)
    ids = lax.broadcasted_iota(jnp.int32, (experts, toks), 0)
    member = jnp.zeros((experts, toks), F32)
    gate = jnp.zeros((experts, toks), F32)
    for k in range(top_k):
        hit = jnp.broadcast_to(route[k : k + 1, :], (experts, toks)) == ids
        member = jnp.where(hit, 1.0, member)
        gate = jnp.where(hit, jnp.broadcast_to(gates[k : k + 1, :], (experts, toks)), gate)
    plan[experts : 2 * experts, :] = gate
    plan[2 * experts :, :] = jnp.zeros((8, toks), F32)
    for t in range(toks // TILE):
        cols = slice(t * TILE, (t + 1) * TILE)
        part = member[:, cols]
        rank = dot(part.astype(BF16), below)
        plan[:experts, cols] = jnp.where(part > 0.5, rank, -4096.0)
        plan[2 * experts + t : 2 * experts + t + 1, :experts] = dot(ones, part.astype(BF16), ((1,), (1,)))[:1]


def spread_kernel(
    depth, experts, x_ref, dy_ref, route_ref, gate_ref, wg_ref, wu_ref, wd_ref,
    x_out, dy_out, plan_out, wg_out, wu_out, wd_out,
    stage_t, stage_w, stage_d, plan, own_sem, z_send, z_recv, p_send, p_recv, c_send, c_recv,
):
    z, y, x, c = (lax.axis_index(a) for a in 'zyxc')
    slot = lambda yy, xx: yy * 4 + xx * 2 + c
    own, by_x, by_y, far = slot(y, x), slot(y, 1 - x), slot(1 - y, x), slot(1 - y, 1 - x)
    weights = ((wg_ref, wg_out), (wu_ref, wu_out), (wd_ref, wd_out))
    arrays = ((x_ref, x_out), (plan, plan_out), (dy_ref, dy_out))
    sent = []

    def half(ref, where, h):
        rows = ref.shape[1] // 2
        return ref.at[where, pl.ds(h * rows, rows), :]

    def own_half(part, h, side):
        src, out = weights[part]
        where = {'x': 1 - x} if side == 0 else {'y': 1 - y}
        return hop(half(src, 0, h), half(out, own, h), p_send.at[side, part, h], p_recv.at[side, part, h], **where)

    def onward(part, h):
        at = half(weights[part][1], by_x if h == 0 else by_y, h)
        where = {'y': 1 - y} if h == 0 else {'x': 1 - x}
        return hop(at, at, p_send.at[2, part, h], p_recv.at[2, part, h], **where)

    def landed(part, h, kind):
        at = half(weights[part][1], (by_x, by_y, far)[kind], h)
        hop(at, at, p_send.at[kind, part, h], p_recv.at[kind, part, h], c=1 - c).wait_recv()

    def across(part, h, kind):
        at = half(weights[part][1], (by_x, by_y, far)[kind], h)
        return hop(at, at, c_send.at[kind, part, h], c_recv.at[kind, part, h], c=1 - c)

    def across_own(part, h):
        src, out = weights[part]
        return hop(half(src, 0, h), half(out, own, h), c_send.at[3, part, h], c_recv.at[3, part, h], c=1 - c)

    def crossed(part, h, kind):
        twin = lambda yy, xx: yy * 4 + xx * 2 + 1 - c
        where = (twin(y, 1 - x), twin(1 - y, x), twin(1 - y, 1 - x), twin(y, x))[kind]
        at = half(weights[part][1], where, h)
        hop(at, at, c_send.at[kind, part, h], c_recv.at[kind, part, h], c=1 - c).wait_recv()

    def go(copy):
        copy.start()
        sent.append((None, copy))

    def along(k, dist, up):
        src, out = arrays[k]
        at = out.at[z - dist if up else z + dist]
        side = 0 if up else 1
        return hop(src if dist == 0 else at, at, z_send.at[side, k, dist], z_recv.at[side, k, dist], z=z + 1 if up else z - 1)

    def start_along(k, dist):
        for up in (True, False):
            cond = (z >= dist) & (z < depth - 1) if up else (z + dist < depth) & (z > 0)

            @pl.when(cond)
            def _(up=up):
                along(k, dist, up).start()

            sent.append((cond, along(k, dist, up)))

    def await_along(k, dist):
        for up in (True, False):
            @pl.when(z > dist if up else z + dist + 1 < depth)
            def _(up=up):
                at = arrays[k][1].at[z - dist - 1 if up else z + dist + 1]
                side = 0 if up else 1
                hop(at, at, z_send.at[side, k, dist], z_recv.at[side, k, dist], c=1 - c).wait_recv()

        if dist + 1 < depth - 1:
            start_along(k, dist + 1)

    copies = []
    for i, (src, buf, out) in enumerate((
        (x_ref, stage_t.at[0], x_out.at[z]), (dy_ref, stage_t.at[1], dy_out.at[z]),
        (wg_ref.at[0], stage_w.at[0], wg_out.at[own]), (wu_ref.at[0], stage_w.at[1], wu_out.at[own]),
        (wd_ref.at[0], stage_d, wd_out.at[own]),
    )):
        copies.append((pltpu.make_async_copy(src, buf, own_sem.at[i]), pltpu.make_async_copy(buf, out, own_sem.at[i])))
        copies[-1][0].start()

    meet(depth, z, y, x, c)
    start_along(0, 0)
    for part in range(3):
        go(own_half(part, 0, 0))
        go(own_half(part, 1, 1))
    for part in range(3):
        go(own_half(part, 1, 0))
        go(own_half(part, 0, 1))
    for part in range(3):
        for h in range(2):
            go(across_own(part, h))
    make_plan(experts, route_ref, gate_ref, plan)
    start_along(1, 0)
    start_along(2, 0)
    copies.append((None, pltpu.make_async_copy(plan, plan_out.at[z], own_sem.at[5])))
    for i, (load, store) in enumerate(copies):
        if load is not None:
            load.wait()
        store.start()

    def relay(part, h):
        landed(part, h, h)
        go(onward(part, h))
        go(across(part, h, h))

    def relay_twin(part, h):
        landed(part, h, 1 - h)
        go(across(part, h, 1 - h))

    for part in range(2):
        relay(part, 0)
        relay(part, 1)
    await_along(0, 0)
    await_along(1, 0)
    relay(2, 0)
    relay(2, 1)
    await_along(2, 0)
    for part in range(3):
        relay_twin(part, 1)
        relay_twin(part, 0)
    await_along(0, 1)
    await_along(1, 1)
    for part in range(3):
        for h in range(2):
            landed(part, h, 2)
            go(across(part, h, 2))
    await_along(2, 1)
    for k in range(3):
        await_along(k, 2)
    for part in range(3):
        for h in range(2):
            for kind in range(4):
                crossed(part, h, kind)
    for cond, copy in sent:
        if cond is None:
            copy.wait_send()
        else:
            @pl.when(cond)
            def _(copy=copy):
                copy.wait_send()
    for _, store in copies:
        store.wait()


def spread(depth, experts, x_tok, dy_tok, route, gate, w_gate, w_up, w_down):
    toks, dim = x_tok.shape
    ff = w_down.shape[1]
    any_space = pl.BlockSpec(memory_space=pl.ANY)
    vmem = pl.BlockSpec(memory_space=pltpu.VMEM)
    rows = 2 * experts + 8
    shape = jax.ShapeDtypeStruct
    dma = pltpu.SemaphoreType.DMA
    return pl.pallas_call(
        functools.partial(spread_kernel, depth, experts),
        in_specs=[any_space, any_space, vmem, vmem, any_space, any_space, any_space],
        out_specs=[any_space] * 6,
        out_shape=[
            shape((depth, toks, dim), BF16), shape((depth, toks, dim), BF16), shape((depth, rows, toks), F32),
            shape((8, dim, ff), BF16), shape((8, dim, ff), BF16), shape((8, ff, dim), BF16),
        ],
        scratch_shapes=[
            pltpu.VMEM((2, toks, dim), BF16), pltpu.VMEM((2, dim, ff), BF16), pltpu.VMEM((ff, dim), BF16),
            pltpu.VMEM((rows, toks), F32), dma((6,)), dma((2, 3, depth)), dma((2, 3, depth)),
            dma((3, 3, 2)), dma((3, 3, 2)), dma((4, 3, 2)), dma((4, 3, 2)),
        ],
        compiler_params=pltpu.CompilerParams(collective_id=0, has_side_effects=True),
        name="spread",
    )(x_tok, dy_tok, route, gate, w_gate, w_up, w_down)


CHUNK = 128
BAND = 64
LAG = 3
RING = 6


def collect_kernel(
    depth, yd_ref, g_ref, y_out, dx_out, g_out, twin,
    z_land, x_land, y_land, x_last, y_last, total, x_buf, y_buf, f_buf, z_buf,
    t_sem, x_load, y_load, f_load, z_load, z_send, z_recv, x_send, x_recv, y_send, y_recv, c_send, c_recv,
):
    z, y, x, c = (lax.axis_index(a) for a in 'zyxc')
    cell = lambda yy, xx: yy * 2 + xx
    mine, by_x, by_y, far = cell(y, x), cell(y, 1 - x), cell(1 - y, x), cell(1 - y, 1 - x)
    bands = yd_ref.shape[2] // BAND
    n_part = g_ref.shape[1] // CHUNK // 2
    n_col = 2 * (depth - 1) * bands
    n_link = 3 * n_part
    piece = 4 * CHUNK
    order = (far, by_x, by_y, mine)
    rows = lambda i: pl.ds(pl.multiple_of(i * CHUNK, CHUNK), CHUNK)

    def swap(kind, q):
        at = pl.ds(q * piece, piece)
        return hop(g_ref.at[2 * order[kind] + 1 - c, at, :], twin.at[order[kind], at, :], c_send.at[kind, q], c_recv.at[kind, q], c=1 - c)

    half = n_part // 4
    swaps = [(0, q + h * half) for q in range(half) for h in range(2)]
    swaps += [(1 + h, q + h * half) for q in range(half) for h in range(2)]
    swaps += [(2 - h, q + h * half) for q in range(half) for h in range(2)]
    swaps += [(3, q + h * half) for q in range(half) for h in range(2)]

    own_total = [pltpu.make_async_copy(yd_ref.at[k, z], total.at[k], t_sem.at[k]) for k in range(2)]
    for copy in own_total:
        copy.start()
    meet(depth, z, y, x, c)
    for kind, q in swaps:
        swap(kind, q).start()

    def link_item(side, i):
        leg = i // n_part
        j = i % n_part
        near, other = (by_x, by_y) if side == 0 else (by_y, by_x)
        kind_near, kind_other = (1, 2) if side == 0 else (2, 1)
        first = jnp.where(leg < 2, side, 1 - side)
        chunk = first * n_part + j
        expert = jnp.where(leg == 0, far, near)
        kind = jnp.where(leg == 0, 0, kind_near)
        return leg, j, chunk, expert, kind

    def fetch(chunk, expert, kind, fresh, buf, sems):
        @pl.when(fresh)
        def _():
            for k in range(4):
                @pl.when(kind == k)
                def _(k=k):
                    at = pl.ds(pl.multiple_of(chunk // 4 * piece, piece), piece)
                    q = chunk // 4
                    hop(twin.at[order[k], at, :], twin.at[order[k], at, :], c_send.at[k, q], c_recv.at[k, q], c=1 - c).wait_recv()

        pltpu.make_async_copy(g_ref.at[2 * expert + c, rows(chunk), :], buf.at[0], sems.at[0]).start()
        pltpu.make_async_copy(twin.at[expert, rows(chunk), :], buf.at[1], sems.at[1]).start()

    def fetched(buf, sems):
        pltpu.make_async_copy(g_ref.at[0, rows(0), :], buf.at[0], sems.at[0]).wait()
        pltpu.make_async_copy(twin.at[0, rows(0), :], buf.at[1], sems.at[1]).wait()

    links = (
        (x_buf, x_load, x_send, x_recv, x_land, x_last, {'x': 1 - x}),
        (y_buf, y_load, y_send, y_recv, y_land, y_last, {'y': 1 - y}),
    )

    def landing(side, i):
        land, last = links[side][4], links[side][5]
        return land, last

    def link_send(side, i, wait_only=False):
        buf, _, send, recv, land, last, where = links[side]
        src = buf.at[i % RING, 0]

        @pl.when(i < 2 * n_part)
        def _():
            copy = hop(src, land.at[jnp.minimum(i, 2 * n_part - 1)], send.at[i], recv.at[i], **where)
            copy.wait_send() if wait_only else copy.start()

        @pl.when(i >= 2 * n_part)
        def _():
            copy = hop(src, last.at[jnp.maximum(i - 2 * n_part, 0)], send.at[i], recv.at[i], **where)
            copy.wait_send() if wait_only else copy.start()

    def landed(side, ref, i):
        recv, send = links[side][3], links[side][2]
        hop(ref, ref, send.at[i], recv.at[i], c=1 - c).wait_recv()

    def link_prepare(side, i):
        buf, load = links[side][0], links[side][1]

        @pl.when((i >= RING) & (i < n_link))
        def _():
            link_send(side, i - RING, wait_only=True)

        @pl.when(i < n_link)
        def _():
            leg, j, chunk, expert, kind = link_item(side, i)
            fetch(chunk, expert, kind, j % 4 == 0, buf.at[i % RING], load.at[i % RING])

    def link_turn(side, i):
        buf, load = links[side][0], links[side][1]
        other_land = links[1 - side][4]

        @pl.when(i < n_link)
        def _():
            b = i % RING
            fetched(buf.at[b], load.at[b])
            buf[b, 0] += buf[b, 1]

            @pl.when(i >= 2 * n_part)
            def _():
                j = i - 2 * n_part
                landed(1 - side, other_land.at[j], j)
                buf[b, 0] += other_land[j]

            link_send(side, i)

    def last_prepare(h, j):
        @pl.when((j >= 0) & (j < n_part))
        def _():
            fetch(h * n_part + j, mine, 3, j % 4 == 0, f_buf.at[h, j % 2], f_load.at[h, j % 2])

    def last_turn(h, j):
        @pl.when((j >= 0) & (j < n_part))
        def _():
            land, last = links[h][4], links[1 - h][5]
            fetched(f_buf.at[h, j % 2], f_load.at[h, j % 2])
            landed(h, land.at[n_part + j], n_part + j)
            landed(1 - h, last.at[j], 2 * n_part + j)
            value = f_buf[h, j % 2, 0] + f_buf[h, j % 2, 1] + (land[n_part + j] + last[j])
            g_out[rows(h * n_part + j), :] = value

    def column(side, k):
        role = z if side == 0 else depth - 1 - z
        arr = k // ((depth - 1) * bands)
        goal = depth - 1 - (k // bands) % (depth - 1)
        block = goal if side == 0 else depth - 1 - goal
        slot = block + 1 if side == 0 else block
        at = pl.ds(pl.multiple_of(k % bands * BAND, BAND), BAND)
        return role, arr, goal, block, slot, at

    def column_copy(side, k, src):
        _, arr, _, _, slot, at = column(side, k)
        return hop(src, z_land.at[arr, slot, at, :], z_send.at[side, k], z_recv.at[side, k], z=z + 1 if side == 0 else z - 1)

    def turn_of(side, t):
        role = z if side == 0 else depth - 1 - z
        return t - LAG * role

    def column_prepare(side, t):
        k = turn_of(side, t)
        kk = jnp.clip(k, 0, n_col - 1)
        role, arr, goal, block, slot, at = column(side, kk)

        @pl.when((k >= 0) & (k < n_col) & (role > 0) & (goal > role))
        def _():
            pltpu.make_async_copy(yd_ref.at[arr, block, at, :], z_buf.at[side, kk % 2], z_load.at[side, kk % 2]).start()

    def column_turn(side, t):
        k = turn_of(side, t)
        kk = jnp.clip(k, 0, n_col - 1)
        role, arr, goal, block, slot, at = column(side, kk)
        live = (k >= 0) & (k < n_col) & (goal >= role)

        @pl.when(live & (role == 0))
        def _():
            column_copy(side, kk, yd_ref.at[arr, block, at, :]).start()

        @pl.when(live & (role > 0))
        def _():
            here = z_land.at[arr, slot, at, :]
            hop(here, here, z_send.at[side, kk], z_recv.at[side, kk], c=1 - c).wait_recv()

            @pl.when(goal > role)
            def _():
                pltpu.make_async_copy(yd_ref.at[arr, block, at, :], z_buf.at[side, kk % 2], z_load.at[side, kk % 2]).wait()
                z_land[arr, slot, at, :] += z_buf[side, kk % 2]
                column_copy(side, kk, here).start()

            @pl.when(goal == role)
            def _():
                total[arr, at, :] += z_land[arr, slot, at, :]

    def prepare(t):
        for side in range(2):
            link_prepare(side, t)
            column_prepare(side, t)
            last_prepare(side, t - 2 * n_part - LAG)

    prepare(jnp.int32(0))
    for copy in own_total:
        copy.wait()
    steps = max(n_col + LAG * (depth - 1), n_link + LAG)

    @pl.loop(0, steps)
    def _(t):
        prepare(t + 1)
        for side in range(2):
            link_turn(side, t)
        for side in range(2):
            column_turn(side, t)
        for side in range(2):
            last_turn(side, t - 2 * n_part - LAG)

    y_out[...] = total[0].astype(BF16)
    dx_out[...] = total[1].astype(BF16)

    @pl.loop(n_link - RING, n_link)
    def _(i):
        for side in range(2):
            link_send(side, i, wait_only=True)

    @pl.loop(0, n_col)
    def _(k):
        for side in range(2):
            role, arr, goal, block, slot, at = column(side, k)

            @pl.when(goal > role)
            def _():
                column_copy(side, k, z_land.at[arr, slot, at, :]).wait_send()

    for kind, q in swaps:
        swap(kind, q).wait_send()


def collect(depth, yd, grads):
    toks, dim = yd.shape[2:]
    height, ff = grads.shape[1:]
    n_part = height // CHUNK // 2
    n_col = 2 * (depth - 1) * (toks // BAND)
    any_space = pl.BlockSpec(memory_space=pl.ANY)
    vmem = pl.BlockSpec(memory_space=pltpu.VMEM)
    shape = jax.ShapeDtypeStruct
    dma = pltpu.SemaphoreType.DMA
    message = (CHUNK, ff)
    return pl.pallas_call(
        functools.partial(collect_kernel, depth),
        in_specs=[any_space, any_space],
        out_specs=[vmem, vmem, vmem, any_space],
        out_shape=[shape((toks, dim), BF16), shape((toks, dim), BF16), shape((height, ff), F32), shape((4, height, ff), F32)],
        scratch_shapes=[
            pltpu.VMEM((2, depth + 1, toks, dim), F32),
            pltpu.VMEM((2 * n_part, *message), F32), pltpu.VMEM((2 * n_part, *message), F32),
            pltpu.VMEM((n_part, *message), F32), pltpu.VMEM((n_part, *message), F32),
            pltpu.VMEM((2, toks, dim), F32),
            pltpu.VMEM((RING, 2, *message), F32), pltpu.VMEM((RING, 2, *message), F32),
            pltpu.VMEM((2, 2, 2, *message), F32), pltpu.VMEM((2, 2, BAND, dim), F32),
            dma((2,)), dma((RING, 2)), dma((RING, 2)), dma((2, 2, 2)), dma((2, 2)),
            dma((2, n_col)), dma((2, n_col)), dma((3 * n_part,)), dma((3 * n_part,)), dma((3 * n_part,)), dma((3 * n_part,)),
            dma((4, height // CHUNK // 4)), dma((4, height // CHUNK // 4)),
        ],
        compiler_params=pltpu.CompilerParams(collective_id=1, has_side_effects=True, vmem_limit_bytes=66_000_000),
        name="collect",
    )(yd, grads)[:3]


def expert_kernel(
    n_tiles, n_exp, count_ref, place_ref, rank_ref, gate_ref, x_ref, dy_ref, wg_ref, wu_ref, wd_ref,
    yd_ref, dw_ref, x_rows, g_rows, o_win, d_win, cum_ref, off_ref,
):
    step = pl.program_id(0)

    @pl.when(step == 0)
    def _count():
        base = jnp.int32(0)
        for exp in range(n_exp):
            run = jnp.int32(0)
            cum_ref[exp] = run
            for tile in range(n_tiles):
                run += count_ref[tile * n_exp + exp]
                cum_ref[(tile + 1) * n_exp + exp] = run
            off_ref[exp] = base
            base += ((run + ALIGN - 1) // ALIGN) * ALIGN

    def span(tile, exp):
        lo = cum_ref[tile * n_exp + exp]
        hi = cum_ref[(tile + 1) * n_exp + exp]
        start = (lo // ALIGN) * ALIGN
        return lo, hi, start

    @pl.when(step < n_tiles)
    def _gather():
        tile = step

        def window(exp, lo, hi, start):
            first = (start - lo).astype(F32)
            place = lax.broadcasted_iota(jnp.int32, (WIN, TILE), 0).astype(F32) + first
            hit = rank_ref[0, exp : exp + 1, :] == place
            take = jnp.where(hit, 1.0, 0.0).astype(BF16)
            scale = jnp.where(hit, gate_ref[0, exp : exp + 1, :], 0.0).astype(BF16)
            row = lax.broadcasted_iota(jnp.int32, (WIN, 1), 0) + start
            mine = (row >= lo) & (row < hi)
            here = pl.ds(pl.multiple_of(off_ref[exp] + start, ALIGN), WIN)
            x_rows[here, :] = jnp.where(mine, dot(take, x_ref[...]), x_rows[here, :].astype(F32)).astype(BF16)
            g_rows[here, :] = jnp.where(mine, dot(scale, dy_ref[...]), g_rows[here, :].astype(F32)).astype(BF16)

        for exp in range(n_exp):
            lo, hi, start = span(tile, exp)
            window(exp, lo, hi, start)

            @pl.when(hi > start + WIN)
            def _more():
                @pl.loop(1, (hi - start + WIN - 1) // WIN)
                def _(w):
                    window(exp, lo, hi, start + w * WIN)

    @pl.when((step >= n_tiles) & (step < n_tiles + n_exp))
    def _expert():
        exp = step - n_tiles
        count = cum_ref[n_tiles * n_exp + exp]
        base = off_ref[exp]
        dw_ref[...] = jnp.zeros_like(dw_ref)
        dim, ff = wg_ref.shape[1:]

        @pl.loop(0, (count + ROWS - 1) // ROWS)
        def _(b):
            here = pl.ds(pl.multiple_of(base + b * ROWS, ALIGN), ROWS)
            live = lax.broadcasted_iota(jnp.int32, (ROWS, 1), 0) < count - b * ROWS
            x_old = x_rows[here, :]
            g_old = g_rows[here, :]
            x_blk = jnp.where(live, x_old, jnp.zeros_like(x_old))
            g_blk = jnp.where(live, g_old, jnp.zeros_like(g_old))
            u = dot(x_blk, wg_ref[0])
            v = dot(x_blk, wu_ref[0])
            s = jax.nn.sigmoid(u)
            act = (u * s * v).astype(BF16)
            da = dot(g_blk, wd_ref[0], ((1,), (1,)))
            du = (da * v * s * (1.0 + u * (1.0 - s))).astype(BF16)
            dv = (da * u * s).astype(BF16)
            out = dot(act, wd_ref[0]).astype(BF16)
            dxr = (dot(du, wg_ref[0], ((1,), (1,))) + dot(dv, wu_ref[0], ((1,), (1,)))).astype(BF16)
            dw_ref[0, 2 * dim : 2 * dim + ff] += dot(act, g_blk[:, :ff], ((0,), (0,)))
            dw_ref[0, 2 * dim + ff :] += dot(act, g_blk[:, ff:], ((0,), (0,)))
            g_rows[here, :] = jnp.where(live, dxr, g_rows[here, :])
            dw_ref[0, :dim] += dot(x_blk, du, ((0,), (0,)))
            dw_ref[0, dim : 2 * dim] += dot(x_blk, dv, ((0,), (0,)))
            x_rows[here, :] = jnp.where(live, out, x_rows[here, :])

    @pl.when(step >= n_tiles + n_exp)
    def _scatter():
        tile = step - n_tiles - n_exp

        def window(exp, lo, hi, start):
            first = (start - lo).astype(F32)
            place = lax.broadcasted_iota(jnp.int32, (WIN, TILE), 0).astype(F32) + first
            hit = rank_ref[0, exp : exp + 1, :] == place
            put = jnp.where(hit, 1.0, 0.0).astype(BF16)
            scale = jnp.where(hit, gate_ref[0, exp : exp + 1, :], 0.0).astype(BF16)
            row = lax.broadcasted_iota(jnp.int32, (WIN, 1), 0) + start
            mine = (row >= lo) & (row < hi)
            here = pl.ds(pl.multiple_of(off_ref[exp] + start, ALIGN), WIN)
            o_blk = x_rows[here, :]
            d_blk = g_rows[here, :]
            o_blk = jnp.where(mine, o_blk, jnp.zeros_like(o_blk))
            d_blk = jnp.where(mine, d_blk, jnp.zeros_like(d_blk))
            return put, scale, o_blk, d_blk

        for part in range(n_exp // GROUP):
            puts, scales = [], []
            for i in range(GROUP):
                exp = part * GROUP + i
                lo, hi, start = span(tile, exp)
                put, scale, o_blk, d_blk = window(exp, lo, hi, start)
                puts.append(put)
                scales.append(scale)
                o_win[i * WIN : (i + 1) * WIN, :] = o_blk
                d_win[i * WIN : (i + 1) * WIN, :] = d_blk
            y_add = dot(jnp.concatenate(scales, axis=0), o_win[...], ((0,), (0,)))
            dx_add = dot(jnp.concatenate(puts, axis=0), d_win[...], ((0,), (0,)))
            yd_ref[0] = y_add if part == 0 else yd_ref[0] + y_add
            yd_ref[1] = dx_add if part == 0 else yd_ref[1] + dx_add
        for exp in range(n_exp):
            lo, hi, start = span(tile, exp)

            @pl.when(hi > start + WIN)
            def _more():
                @pl.loop(1, (hi - start + WIN - 1) // WIN)
                def _(w):
                    put, scale, o_blk, d_blk = window(exp, lo, hi, start + w * WIN)
                    yd_ref[0] += dot(scale, o_blk, ((0,), (0,)))
                    yd_ref[1] += dot(put, d_blk, ((0,), (0,)))


def expert_layer(counts, place, plan_col, x_col, dy_col, w_gate, w_up, w_down, cap, n_dev):
    tokens, dim = x_col.shape
    n_exp, _, ff = w_gate.shape
    n_tiles = tokens // TILE
    total = n_exp * (-(-cap // ALIGN) * ALIGN) + ROWS
    per = plan_col.shape[2] // TILE
    first = lambda i: jnp.minimum(i, n_tiles - 1)
    middle = lambda i: jnp.clip(i - n_tiles, 0, n_exp - 1)
    last = lambda i: jnp.maximum(i - n_tiles - n_exp, 0)
    tile_of = lambda i: jnp.where(i < n_tiles, i, last(i))
    plan_at = lambda part: lambda i, counts, place: (tile_of(i) // per, place[0] + part, tile_of(i) % per)
    ranks = pl.BlockSpec((1, n_exp, TILE), plan_at(0))
    gates = pl.BlockSpec((1, n_exp, TILE), plan_at(n_dev // n_exp))
    toks_in = pl.BlockSpec((TILE, dim), lambda i, *_: (first(i), 0))
    toks_out = pl.BlockSpec((2, TILE, dim), lambda i, *_: (0, last(i), 0))
    grads = pl.BlockSpec((1, 3 * dim, ff), lambda i, *_: (middle(i), 0, 0))
    wide = pl.BlockSpec((1, dim, ff), lambda i, *_: (middle(i), 0, 0))
    tall = pl.BlockSpec((1, ff, dim), lambda i, *_: (middle(i), 0, 0))
    return pl.pallas_call(
        functools.partial(expert_kernel, n_tiles, n_exp),
        grid_spec=pltpu.PrefetchScalarGridSpec(
            num_scalar_prefetch=2,
            grid=(2 * n_tiles + n_exp,),
            in_specs=[ranks, gates, toks_in, toks_in, wide, wide, tall],
            out_specs=[toks_out, grads],
            scratch_shapes=[
                pltpu.VMEM((total, dim), BF16),
                pltpu.VMEM((total, dim), BF16),
                pltpu.VMEM((GROUP * WIN, dim), BF16),
                pltpu.VMEM((GROUP * WIN, dim), BF16),
                pltpu.SMEM(((n_tiles + 1) * n_exp,), jnp.int32),
                pltpu.SMEM((n_exp,), jnp.int32),
            ],
        ),
        out_shape=[
            jax.ShapeDtypeStruct((2, tokens, dim), F32),
            jax.ShapeDtypeStruct((n_exp, 3 * dim, ff), F32),
        ],
        compiler_params=pltpu.CompilerParams(
            dimension_semantics=("arbitrary",), vmem_limit_bytes=67_000_000,
        ),
        cost_estimate=pl.CostEstimate(flops=60_000_000_000, bytes_accessed=120_000_000, transcendentals=3_000_000),
        name="experts",
    )(counts, place, plan_col, plan_col, x_col, dy_col, w_gate, w_up, w_down)


def solution(mesh):
    n_dev = mesh.devices.size
    depth = n_dev // 8
    grid = Mesh(mesh.devices.reshape(depth, 2, 2, 2), ('z', 'y', 'x', 'c'))
    plane = ('y', 'x', 'c')
    spec = P(('z', 'y', 'x', 'c'))

    def local_step(x_tok, route_idx, gates, dy_tok, w_gate, w_up, w_down):
        tok_loc, top_k = route_idx.shape
        cap = depth * (2 * tok_loc * top_k // (n_dev * w_gate.shape[0] - 2))
        n_exp = 8 * w_gate.shape[0]
        x_col, dy_col, plan_col, wg_all, wu_all, wd_all = spread(
            depth, n_dev, x_tok, dy_tok, route_idx.T, gates.T.astype(F32), w_gate, w_up, w_down
        )
        place = lax.axis_index('z')
        per = tok_loc // TILE
        counts = lax.dynamic_slice(plan_col[:, 2 * n_dev : 2 * n_dev + per, :n_dev], (0, 0, place * n_exp), (depth, per, n_exp))
        yd, grads = expert_layer(
            counts.reshape(-1).astype(jnp.int32), place.reshape(1), plan_col, x_col.reshape(-1, x_tok.shape[1]),
            dy_col.reshape(-1, x_tok.shape[1]), wg_all, wu_all, wd_all, cap, n_dev
        )
        y, dx, dw = collect(depth, yd.reshape(2, depth, tok_loc, -1), grads)
        dim, ff = w_gate.shape[1:]
        g_down = jnp.concatenate([dw[2 * dim : 2 * dim + ff], dw[2 * dim + ff :]], axis=1)
        return y, dx, dw[None, :dim], dw[None, dim : 2 * dim], g_down[None]

    return jax.shard_map(local_step, mesh=grid, in_specs=(spec,) * 7, out_specs=(spec,) * 5, check_vma=False)
```

```python
import functools

import jax
import jax.numpy as jnp
from jax import lax
from jax.experimental import pallas as pl
from jax.experimental.pallas import tpu as pltpu
from jax.sharding import Mesh, PartitionSpec as P

F32 = jnp.float32
BF16 = jnp.bfloat16
TILE = 256
WIN = 128
ALIGN = 16
ROWS = 512


def dot(a, b, dims=((1,), (0,))):
    return lax.dot_general(a, b, (dims, ((), ())), preferred_element_type=F32)


MESH = pl.DeviceIdType.MESH


def hop(src, dst, send_sem, recv_sem, **where):
    return pltpu.make_async_remote_copy(
        src_ref=src, dst_ref=dst, send_sem=send_sem, recv_sem=recv_sem, device_id=where, device_id_type=MESH
    )


def meet(depth, z, y, x, c):
    barrier = pltpu.get_barrier_semaphore()
    for where in ({'y': 1 - y}, {'x': 1 - x}, {'c': 1 - c}):
        pl.semaphore_signal(barrier, inc=1, device_id=where, device_id_type=MESH)

    @pl.when(z > 0)
    def _():
        pl.semaphore_signal(barrier, inc=1, device_id={'z': z - 1}, device_id_type=MESH)

    @pl.when(z < depth - 1)
    def _():
        pl.semaphore_signal(barrier, inc=1, device_id={'z': z + 1}, device_id_type=MESH)

    inner = (z > 0) & (z < depth - 1)

    @pl.when(inner)
    def _():
        pl.semaphore_wait(barrier, 5)

    @pl.when(jnp.logical_not(inner))
    def _():
        pl.semaphore_wait(barrier, 4)


def make_plan(experts, route_ref, gate_ref, plan):
    top_k, toks = route_ref.shape
    route = route_ref[...]
    gates = gate_ref[...]
    below = lax.broadcasted_iota(jnp.int32, (TILE, TILE), 0) < lax.broadcasted_iota(jnp.int32, (TILE, TILE), 1)
    below = jnp.where(below, 1.0, 0.0).astype(BF16)
    ones = jnp.ones((8, TILE), BF16)
    ids = lax.broadcasted_iota(jnp.int32, (experts, toks), 0)
    member = jnp.zeros((experts, toks), F32)
    gate = jnp.zeros((experts, toks), F32)
    for k in range(top_k):
        hit = jnp.broadcast_to(route[k : k + 1, :], (experts, toks)) == ids
        member = jnp.where(hit, 1.0, member)
        gate = jnp.where(hit, jnp.broadcast_to(gates[k : k + 1, :], (experts, toks)), gate)
    plan[experts : 2 * experts, :] = gate
    plan[2 * experts :, :] = jnp.zeros((8, toks), F32)
    for t in range(toks // TILE):
        cols = slice(t * TILE, (t + 1) * TILE)
        part = member[:, cols]
        rank = dot(part.astype(BF16), below)
        plan[:experts, cols] = jnp.where(part > 0.5, rank, -4096.0)
        plan[2 * experts + t : 2 * experts + t + 1, :experts] = dot(ones, part.astype(BF16), ((1,), (1,)))[:1]


def spread_kernel(
    depth, experts, x_ref, dy_ref, route_ref, gate_ref, wg_ref, wu_ref, wd_ref,
    x_out, dy_out, plan_out, wg_out, wu_out, wd_out,
    stage_t, stage_w, stage_d, plan, own_sem, z_send, z_recv, p_send, p_recv, c_send, c_recv,
):
    z, y, x, c = (lax.axis_index(a) for a in 'zyxc')
    slot = lambda yy, xx: yy * 4 + xx * 2 + c
    own, by_x, by_y, far = slot(y, x), slot(y, 1 - x), slot(1 - y, x), slot(1 - y, 1 - x)
    weights = ((wg_ref, wg_out), (wu_ref, wu_out), (wd_ref, wd_out))
    dy_head = dy_ref.at[pl.ds(0, dy_out.shape[1]), :]
    arrays = ((x_ref, x_out), (plan, plan_out), (dy_head, dy_out))
    sent = []

    def half(ref, where, h):
        rows = ref.shape[1] // 2
        return ref.at[where, pl.ds(h * rows, rows), :]

    def own_half(part, h, side):
        src, out = weights[part]
        where = {'x': 1 - x} if side == 0 else {'y': 1 - y}
        return hop(half(src, 0, h), half(out, own, h), p_send.at[side, part, h], p_recv.at[side, part, h], **where)

    def onward(part, h):
        at = half(weights[part][1], by_x if h == 0 else by_y, h)
        where = {'y': 1 - y} if h == 0 else {'x': 1 - x}
        return hop(at, at, p_send.at[2, part, h], p_recv.at[2, part, h], **where)

    def landed(part, h, kind):
        at = half(weights[part][1], (by_x, by_y, far)[kind], h)
        hop(at, at, p_send.at[kind, part, h], p_recv.at[kind, part, h], c=1 - c).wait_recv()

    def across(part, h, kind):
        at = half(weights[part][1], (by_x, by_y, far)[kind], h)
        return hop(at, at, c_send.at[kind, part, h], c_recv.at[kind, part, h], c=1 - c)

    def across_own(part, h):
        src, out = weights[part]
        return hop(half(src, 0, h), half(out, own, h), c_send.at[3, part, h], c_recv.at[3, part, h], c=1 - c)

    def crossed(part, h, kind):
        twin = lambda yy, xx: yy * 4 + xx * 2 + 1 - c
        where = (twin(y, 1 - x), twin(1 - y, x), twin(1 - y, 1 - x), twin(y, x))[kind]
        at = half(weights[part][1], where, h)
        hop(at, at, c_send.at[kind, part, h], c_recv.at[kind, part, h], c=1 - c).wait_recv()

    def go(copy):
        copy.start()
        sent.append((None, copy))

    def along(k, dist, up):
        src, out = arrays[k]
        at = out.at[z - dist if up else z + dist]
        side = 0 if up else 1
        return hop(src if dist == 0 else at, at, z_send.at[side, k, dist], z_recv.at[side, k, dist], z=z + 1 if up else z - 1)

    def start_along(k, dist):
        for up in (True, False):
            cond = (z >= dist) & (z < depth - 1) if up else (z + dist < depth) & (z > 0)

            @pl.when(cond)
            def _(up=up):
                along(k, dist, up).start()

            sent.append((cond, along(k, dist, up)))

    def await_along(k, dist):
        for up in (True, False):
            @pl.when(z > dist if up else z + dist + 1 < depth)
            def _(up=up):
                at = arrays[k][1].at[z - dist - 1 if up else z + dist + 1]
                side = 0 if up else 1
                hop(at, at, z_send.at[side, k, dist], z_recv.at[side, k, dist], c=1 - c).wait_recv()

        if dist + 1 < depth - 1:
            start_along(k, dist + 1)

    copies = []
    for i, (src, buf, out) in enumerate((
        (x_ref, stage_t.at[0], x_out.at[z]), (dy_head, stage_t.at[1, pl.ds(0, dy_out.shape[1]), :], dy_out.at[z]),
        (wg_ref.at[0], stage_w.at[0], wg_out.at[own]), (wu_ref.at[0], stage_w.at[1], wu_out.at[own]),
        (wd_ref.at[0], stage_d, wd_out.at[own]),
    )):
        copies.append((pltpu.make_async_copy(src, buf, own_sem.at[i]), pltpu.make_async_copy(buf, out, own_sem.at[i])))
        copies[-1][0].start()

    meet(depth, z, y, x, c)
    start_along(0, 0)
    for part in range(3):
        go(own_half(part, 0, 0))
        go(own_half(part, 1, 1))
    for part in range(3):
        go(own_half(part, 1, 0))
        go(own_half(part, 0, 1))
    for part in range(3):
        for h in range(2):
            go(across_own(part, h))
    make_plan(experts, route_ref, gate_ref, plan)
    start_along(1, 0)
    start_along(2, 0)
    copies.append((None, pltpu.make_async_copy(plan, plan_out.at[z], own_sem.at[5])))
    for i, (load, store) in enumerate(copies):
        if load is not None:
            load.wait()
        store.start()

    def relay(part, h):
        landed(part, h, h)
        go(onward(part, h))
        go(across(part, h, h))

    def relay_twin(part, h):
        landed(part, h, 1 - h)
        go(across(part, h, 1 - h))

    for part in range(2):
        relay(part, 0)
        relay(part, 1)
    await_along(0, 0)
    await_along(1, 0)
    relay(2, 0)
    relay(2, 1)
    await_along(2, 0)
    for part in range(3):
        relay_twin(part, 1)
        relay_twin(part, 0)
    await_along(0, 1)
    await_along(1, 1)
    for part in range(3):
        for h in range(2):
            landed(part, h, 2)
            go(across(part, h, 2))
    await_along(2, 1)
    for k in range(3):
        await_along(k, 2)
    for part in range(3):
        for h in range(2):
            for kind in range(4):
                crossed(part, h, kind)
    for cond, copy in sent:
        if cond is None:
            copy.wait_send()
        else:
            @pl.when(cond)
            def _(copy=copy):
                copy.wait_send()
    for _, store in copies:
        store.wait()


def spread(depth, experts, head, x_tok, dy_tok, route, gate, w_gate, w_up, w_down):
    toks, dim = x_tok.shape
    ff = w_down.shape[1]
    any_space = pl.BlockSpec(memory_space=pl.ANY)
    vmem = pl.BlockSpec(memory_space=pltpu.VMEM)
    rows = 2 * experts + 8
    shape = jax.ShapeDtypeStruct
    dma = pltpu.SemaphoreType.DMA
    return pl.pallas_call(
        functools.partial(spread_kernel, depth, experts),
        in_specs=[any_space, any_space, vmem, vmem, any_space, any_space, any_space],
        out_specs=[any_space] * 6,
        out_shape=[
            shape((depth, toks, dim), BF16), shape((depth, head, dim), BF16), shape((depth, rows, toks), F32),
            shape((8, dim, ff), BF16), shape((8, dim, ff), BF16), shape((8, ff, dim), BF16),
        ],
        scratch_shapes=[
            pltpu.VMEM((2, toks, dim), BF16), pltpu.VMEM((2, dim, ff), BF16), pltpu.VMEM((ff, dim), BF16),
            pltpu.VMEM((rows, toks), F32), dma((6,)), dma((2, 3, depth)), dma((2, 3, depth)),
            dma((3, 3, 2)), dma((3, 3, 2)), dma((4, 3, 2)), dma((4, 3, 2)),
        ],
        compiler_params=pltpu.CompilerParams(collective_id=0, has_side_effects=True),
        name="spread",
    )(x_tok, dy_tok, route, gate, w_gate, w_up, w_down)


CHUNK = 128
BAND = 64
LAG = 3
DELAY = 18
RING = 6


def collect_kernel(
    depth, dx_ref, g_ref, dx_out, g_out, twin,
    z_land, x_land, y_land, x_last, y_last, total, x_buf, y_buf, f_buf, z_buf,
    t_sem, x_load, y_load, f_load, z_load, z_send, z_recv, x_send, x_recv, y_send, y_recv, c_send, c_recv,
):
    z, y, x, c = (lax.axis_index(a) for a in 'zyxc')
    cell = lambda yy, xx: yy * 2 + xx
    mine, by_x, by_y, far = cell(y, x), cell(y, 1 - x), cell(1 - y, x), cell(1 - y, 1 - x)
    bands = dx_ref.shape[1] // BAND
    n_part = g_ref.shape[1] // CHUNK // 2
    n_col = (depth - 1) * bands
    n_link = 3 * n_part
    piece = 4 * CHUNK
    order = (far, by_x, by_y, mine)
    rows = lambda i: pl.ds(pl.multiple_of(i * CHUNK, CHUNK), CHUNK)

    def swap(kind, q):
        at = pl.ds(q * piece, piece)
        return hop(g_ref.at[2 * order[kind] + 1 - c, at, :], twin.at[order[kind], at, :], c_send.at[kind, q], c_recv.at[kind, q], c=1 - c)

    half = n_part // 4
    swaps = [(0, q + h * half) for q in range(half) for h in range(2)]
    swaps += [(1 + h, q + h * half) for q in range(half) for h in range(2)]
    swaps += [(2 - h, q + h * half) for q in range(half) for h in range(2)]
    swaps += [(3, q + h * half) for q in range(half) for h in range(2)]

    own_total = pltpu.make_async_copy(dx_ref.at[z], total, t_sem)
    own_total.start()
    meet(depth, z, y, x, c)
    for kind, q in swaps:
        swap(kind, q).start()

    def link_item(side, i):
        leg = i // n_part
        j = i % n_part
        near, other = (by_x, by_y) if side == 0 else (by_y, by_x)
        kind_near, kind_other = (1, 2) if side == 0 else (2, 1)
        first = jnp.where(leg < 2, side, 1 - side)
        chunk = first * n_part + j
        expert = jnp.where(leg == 0, far, near)
        kind = jnp.where(leg == 0, 0, kind_near)
        return leg, j, chunk, expert, kind

    def fetch(chunk, expert, kind, fresh, buf, sems):
        @pl.when(fresh)
        def _():
            for k in range(4):
                @pl.when(kind == k)
                def _(k=k):
                    at = pl.ds(pl.multiple_of(chunk // 4 * piece, piece), piece)
                    q = chunk // 4
                    hop(twin.at[order[k], at, :], twin.at[order[k], at, :], c_send.at[k, q], c_recv.at[k, q], c=1 - c).wait_recv()

        pltpu.make_async_copy(g_ref.at[2 * expert + c, rows(chunk), :], buf.at[0], sems.at[0]).start()
        pltpu.make_async_copy(twin.at[expert, rows(chunk), :], buf.at[1], sems.at[1]).start()

    def fetched(buf, sems):
        pltpu.make_async_copy(g_ref.at[0, rows(0), :], buf.at[0], sems.at[0]).wait()
        pltpu.make_async_copy(twin.at[0, rows(0), :], buf.at[1], sems.at[1]).wait()

    links = (
        (x_buf, x_load, x_send, x_recv, x_land, x_last, {'x': 1 - x}),
        (y_buf, y_load, y_send, y_recv, y_land, y_last, {'y': 1 - y}),
    )

    def landing(side, i):
        land, last = links[side][4], links[side][5]
        return land, last

    def link_send(side, i, wait_only=False):
        buf, _, send, recv, land, last, where = links[side]
        src = buf.at[i % RING, 0]

        @pl.when(i < 2 * n_part)
        def _():
            copy = hop(src, land.at[jnp.minimum(i, 2 * n_part - 1)], send.at[i], recv.at[i], **where)
            copy.wait_send() if wait_only else copy.start()

        @pl.when(i >= 2 * n_part)
        def _():
            copy = hop(src, last.at[jnp.maximum(i - 2 * n_part, 0)], send.at[i], recv.at[i], **where)
            copy.wait_send() if wait_only else copy.start()

    def landed(side, ref, i):
        recv, send = links[side][3], links[side][2]
        hop(ref, ref, send.at[i], recv.at[i], c=1 - c).wait_recv()

    def link_prepare(side, i):
        buf, load = links[side][0], links[side][1]

        @pl.when((i >= RING) & (i < n_link))
        def _():
            link_send(side, i - RING, wait_only=True)

        @pl.when(i < n_link)
        def _():
            leg, j, chunk, expert, kind = link_item(side, i)
            fetch(chunk, expert, kind, j % 4 == 0, buf.at[i % RING], load.at[i % RING])

    def link_turn(side, i):
        buf, load = links[side][0], links[side][1]
        other_land = links[1 - side][4]

        @pl.when(i < n_link)
        def _():
            b = i % RING
            fetched(buf.at[b], load.at[b])
            buf[b, 0] += buf[b, 1]

            @pl.when(i >= 2 * n_part)
            def _():
                j = i - 2 * n_part
                landed(1 - side, other_land.at[j], j)
                buf[b, 0] += other_land[j]

            link_send(side, i)

    def last_prepare(h, j):
        @pl.when((j >= 0) & (j < n_part))
        def _():
            fetch(h * n_part + j, mine, 3, j % 4 == 0, f_buf.at[h, j % 2], f_load.at[h, j % 2])

    def last_turn(h, j):
        @pl.when((j >= 0) & (j < n_part))
        def _():
            land, last = links[h][4], links[1 - h][5]
            fetched(f_buf.at[h, j % 2], f_load.at[h, j % 2])
            landed(h, land.at[n_part + j], n_part + j)
            landed(1 - h, last.at[j], 2 * n_part + j)
            value = f_buf[h, j % 2, 0] + f_buf[h, j % 2, 1] + (land[n_part + j] + last[j])
            g_out[rows(h * n_part + j), :] = value

    def column(side, k):
        role = z if side == 0 else depth - 1 - z
        goal = depth - 1 - k // bands
        block = goal if side == 0 else depth - 1 - goal
        slot = block + 1 if side == 0 else block
        at = pl.ds(pl.multiple_of(k % bands * BAND, BAND), BAND)
        return role, goal, block, slot, at

    def column_copy(side, k, src):
        _, _, _, slot, at = column(side, k)
        return hop(src, z_land.at[slot, at, :], z_send.at[side, k], z_recv.at[side, k], z=z + 1 if side == 0 else z - 1)

    def turn_of(side, t):
        role = z if side == 0 else depth - 1 - z
        return t - DELAY - LAG * role

    def column_prepare(side, t):
        k = turn_of(side, t)
        kk = jnp.clip(k, 0, n_col - 1)
        role, goal, block, slot, at = column(side, kk)

        @pl.when((k >= 0) & (k < n_col) & (role > 0) & (goal > role))
        def _():
            pltpu.make_async_copy(dx_ref.at[block, at, :], z_buf.at[side, kk % 2], z_load.at[side, kk % 2]).start()

    def column_turn(side, t):
        k = turn_of(side, t)
        kk = jnp.clip(k, 0, n_col - 1)
        role, goal, block, slot, at = column(side, kk)
        live = (k >= 0) & (k < n_col) & (goal >= role)

        @pl.when(live & (role == 0))
        def _():
            column_copy(side, kk, dx_ref.at[block, at, :]).start()

        @pl.when(live & (role > 0))
        def _():
            here = z_land.at[slot, at, :]
            hop(here, here, z_send.at[side, kk], z_recv.at[side, kk], c=1 - c).wait_recv()

            @pl.when(goal > role)
            def _():
                pltpu.make_async_copy(dx_ref.at[block, at, :], z_buf.at[side, kk % 2], z_load.at[side, kk % 2]).wait()
                z_land[slot, at, :] += z_buf[side, kk % 2]
                column_copy(side, kk, here).start()

            @pl.when(goal == role)
            def _():
                total[at, :] += z_land[slot, at, :]

    def prepare(t):
        for side in range(2):
            link_prepare(side, t)
            column_prepare(side, t)
            last_prepare(side, t - 2 * n_part - LAG)

    prepare(jnp.int32(0))
    own_total.wait()
    steps = max(DELAY + n_col + LAG * (depth - 1), n_link + LAG)

    @pl.loop(0, steps)
    def _(t):
        prepare(t + 1)
        for side in range(2):
            link_turn(side, t)
        for side in range(2):
            column_turn(side, t)
        for side in range(2):
            last_turn(side, t - 2 * n_part - LAG)

    dx_out[...] = total[...].astype(BF16)

    @pl.loop(n_link - RING, n_link)
    def _(i):
        for side in range(2):
            link_send(side, i, wait_only=True)

    @pl.loop(0, n_col)
    def _(k):
        for side in range(2):
            role, goal, block, slot, at = column(side, k)

            @pl.when(goal > role)
            def _():
                column_copy(side, k, z_land.at[slot, at, :]).wait_send()

    for kind, q in swaps:
        swap(kind, q).wait_send()


def collect(depth, dx_part, grads):
    toks, dim = dx_part.shape[1:]
    height, ff = grads.shape[1:]
    n_part = height // CHUNK // 2
    n_col = (depth - 1) * (toks // BAND)
    any_space = pl.BlockSpec(memory_space=pl.ANY)
    vmem = pl.BlockSpec(memory_space=pltpu.VMEM)
    shape = jax.ShapeDtypeStruct
    dma = pltpu.SemaphoreType.DMA
    message = (CHUNK, ff)
    return pl.pallas_call(
        functools.partial(collect_kernel, depth),
        in_specs=[any_space, any_space],
        out_specs=[vmem, vmem, any_space],
        out_shape=[shape((toks, dim), BF16), shape((height, ff), F32), shape((4, height, ff), F32)],
        scratch_shapes=[
            pltpu.VMEM((depth + 1, toks, dim), F32),
            pltpu.VMEM((2 * n_part, *message), F32), pltpu.VMEM((2 * n_part, *message), F32),
            pltpu.VMEM((n_part, *message), F32), pltpu.VMEM((n_part, *message), F32),
            pltpu.VMEM((toks, dim), F32),
            pltpu.VMEM((RING, 2, *message), F32), pltpu.VMEM((RING, 2, *message), F32),
            pltpu.VMEM((2, 2, 2, *message), F32), pltpu.VMEM((2, 2, BAND, dim), F32),
            dma, dma((RING, 2)), dma((RING, 2)), dma((2, 2, 2)), dma((2, 2)),
            dma((2, n_col)), dma((2, n_col)), dma((3 * n_part,)), dma((3 * n_part,)), dma((3 * n_part,)), dma((3 * n_part,)),
            dma((4, height // CHUNK // 4)), dma((4, height // CHUNK // 4)),
        ],
        compiler_params=pltpu.CompilerParams(collective_id=1, has_side_effects=True, vmem_limit_bytes=66_000_000),
        name="collect",
    )(dx_part, grads)[:2]


def count_up(n_tiles, n_exp, count_ref, cum_ref, off_ref, blk_ref):
    base = jnp.int32(0)
    block = jnp.int32(0)
    for exp in range(n_exp):
        run = jnp.int32(0)
        cum_ref[exp] = run
        for tile in range(n_tiles):
            run += count_ref[tile * n_exp + exp]
            cum_ref[(tile + 1) * n_exp + exp] = run
        off_ref[exp] = base
        blk_ref[exp] = block
        big, rest = blocks_of(run)
        block += big + rest
        base += jnp.maximum(big * ROWS + rest * (ROWS // 2), (run + ALIGN - 1) // ALIGN * ALIGN + WIN)
    blk_ref[n_exp] = block


def blocks_of(count):
    big = (count + ROWS // 2 - 1) // ROWS
    return big, (count > big * ROWS).astype(jnp.int32)


def span(n_exp, cum_ref, tile, exp):
    lo = cum_ref[tile * n_exp + exp]
    hi = cum_ref[(tile + 1) * n_exp + exp]
    return lo, hi, (lo // ALIGN) * ALIGN


def pick(ref, exp, cols, lo, start):
    place = lax.broadcasted_iota(jnp.int32, (WIN, TILE), 0).astype(F32) + (start - lo).astype(F32)
    return ref[0, exp : exp + 1, cols] == place


def gather_tile(n_exp, cum_ref, off_ref, rank_ref, gate_ref, tile, cols, toks, rows_ref):
    def window(exp, lo, start):
        hit = pick(rank_ref, exp, cols, lo, start)
        value = 1.0 if gate_ref is None else gate_ref[0, exp : exp + 1, cols]
        take = jnp.where(hit, value, 0.0).astype(BF16)
        return dot(take, toks[...]).astype(BF16)

    def rows_at(exp, start, size):
        return pl.ds(pl.multiple_of(off_ref[exp] + start, ALIGN), size)

    spans = [span(n_exp, cum_ref, tile, exp) for exp in range(n_exp)]
    for exp, (lo, hi, start) in enumerate(spans):
        value = window(exp, lo, start)
        head = rows_at(exp, start, ALIGN)
        fresh = lax.broadcasted_iota(jnp.int32, (ALIGN, 1), 0) + start >= lo
        rows_ref[head, :] = jnp.where(fresh, value[:ALIGN], rows_ref[head, :])
        rows_ref[rows_at(exp, start + ALIGN, WIN - ALIGN), :] = value[ALIGN:]
    most = functools.reduce(jnp.maximum, [hi - start for lo, hi, start in spans])

    @pl.when(most > WIN)
    def _more():
        for exp, (lo, hi, start) in enumerate(spans):
            @pl.loop(1, (hi - start + WIN - 1) // WIN)
            def _(w):
                rows_ref[rows_at(exp, start + w * WIN, WIN), :] = window(exp, lo, start + w * WIN)


def scatter_tile(n_exp, cum_ref, off_ref, rank_ref, gate_ref, tile, cols, rows_ref, win_ref, out_ref):
    def window(exp, lo, start):
        hit = pick(rank_ref, exp, cols, lo, start)
        value = 1.0 if gate_ref is None else gate_ref[0, exp : exp + 1, cols]
        put = jnp.where(hit, value, 0.0).astype(BF16)
        return put, rows_ref[pl.ds(pl.multiple_of(off_ref[exp] + start, ALIGN), WIN), :]

    spans = [span(n_exp, cum_ref, tile, exp) for exp in range(n_exp)]
    puts = []
    for exp, (lo, hi, start) in enumerate(spans):
        put, block = window(exp, lo, start)
        puts.append(put)
        win_ref[exp * WIN : (exp + 1) * WIN, :] = block
    out_ref[cols, :] = dot(jnp.concatenate(puts, axis=0), win_ref[...], ((0,), (0,)))
    most = functools.reduce(jnp.maximum, [hi - start for lo, hi, start in spans])

    @pl.when(most > WIN)
    def _more():
        for exp, (lo, hi, start) in enumerate(spans):
            @pl.loop(1, (hi - start + WIN - 1) // WIN)
            def _(w):
                put, block = window(exp, lo, start + w * WIN)
                out_ref[cols, :] += dot(put, block, ((0,), (0,)))


def forward_kernel(
    depth, n_tiles, n_exp, count_ref, z_ref, rank_ref, gate_ref, x_ref, wg_ref, wu_ref, wd_ref,
    *refs,
):
    y_refs, (xs_ref, uv_ref, rows_ref, win_ref, x_out, uv_out, cum_ref, off_ref, blk_ref, x_sem, uv_sem) = refs[:depth], refs[depth:]
    step = pl.program_id(0)
    per = n_tiles // depth

    @pl.when(step == 0)
    def _():
        count_up(n_tiles, n_exp, count_ref, cum_ref, off_ref, blk_ref)

    @pl.when(step < depth)
    def _():
        for i in range(per):
            cols = slice(i * TILE, (i + 1) * TILE)
            gather_tile(n_exp, cum_ref, off_ref, rank_ref, None, step * per + i, cols, x_ref.at[cols, :], rows_ref)

    def saves(block):
        side = block % 2
        return (
            pltpu.make_async_copy(x_out.at[side], xs_ref.at[block], x_sem.at[side]),
            pltpu.make_async_copy(uv_out.at[side], uv_ref.at[block], uv_sem.at[side]),
        )

    @pl.when((step >= depth) & (step < depth + n_exp))
    def _():
        exp = step - depth
        count = cum_ref[n_tiles * n_exp + exp]
        big, rest = blocks_of(count)

        def run(b, size):
            block = blk_ref[exp] + b
            side = block % 2

            @pl.when(block >= 2)
            def _():
                for copy in saves(block - 2):
                    copy.wait()

            here = pl.ds(pl.multiple_of(off_ref[exp] + b * ROWS, ALIGN), size)
            live = lax.broadcasted_iota(jnp.int32, (size, 1), 0) < count - b * ROWS
            x_old = rows_ref[here, :]
            x_out[side, :size] = jnp.where(live, x_old, jnp.zeros_like(x_old))
            u = dot(x_out[side, :size], wg_ref[0])
            v = dot(x_out[side, :size], wu_ref[0])
            uv_out[side, 0, :size] = u
            uv_out[side, 1, :size] = v
            act = (u * jax.nn.sigmoid(u) * v).astype(BF16)
            rows_ref[here, :] = dot(act, wd_ref[0]).astype(BF16)
            for copy in saves(block):
                copy.start()

        @pl.loop(0, big)
        def _(b):
            run(b, ROWS)

        @pl.when(rest > 0)
        def _():
            run(big, ROWS // 2)

    @pl.when(step == depth + n_exp)
    def _():
        total = blk_ref[n_exp]
        for back in (2, 1):
            @pl.when(total >= back)
            def _():
                for copy in saves(total - back):
                    copy.wait()

    for d in range(depth):
        @pl.when(step == depth + n_exp + d)
        def _():
            for i in range(per):
                tile = ((z_ref[0] + d) % depth) * per + i
                cols = slice(i * TILE, (i + 1) * TILE)
                scatter_tile(n_exp, cum_ref, off_ref, rank_ref, gate_ref, tile, cols, rows_ref, win_ref, y_refs[d])


def backward_kernel(
    depth, n_tiles, n_exp, count_ref, z_ref, rank_ref, gate_ref, head_ref, *refs,
):
    tails, refs = refs[:depth], refs[depth:]
    wg_ref, wu_ref, wd_ref, xs_ref, uv_ref, dx_ref, dw_ref = refs[:7]
    rows_ref, win_ref, x_in, uv_in, tail_ref, cum_ref, off_ref, blk_ref, x_sem, uv_sem = refs[7:]
    step = pl.program_id(0)
    per = n_tiles // depth

    @pl.when(step == 0)
    def _():
        count_up(n_tiles, n_exp, count_ref, cum_ref, off_ref, blk_ref)

    @pl.when(step < depth)
    def _():
        for d in range(depth):
            @pl.when((z_ref[0] + depth - step) % depth == d)
            def _():
                tail_ref[...] = tails[d][...]

        split = head_ref.shape[0]
        for i in range(per):
            cols = slice(i * TILE, (i + 1) * TILE)
            toks = head_ref.at[cols, :] if i * TILE < split else tail_ref.at[slice(i * TILE - split, (i + 1) * TILE - split), :]
            gather_tile(n_exp, cum_ref, off_ref, rank_ref, gate_ref, step * per + i, cols, toks, rows_ref)

    def loads(block):
        side = block % 2
        return (
            pltpu.make_async_copy(xs_ref.at[block], x_in.at[side], x_sem.at[side]),
            pltpu.make_async_copy(uv_ref.at[block], uv_in.at[side], uv_sem.at[side]),
        )

    @pl.when((step == depth - 1) & (blk_ref[n_exp] > 0))
    def _():
        for copy in loads(0):
            copy.start()

    @pl.when((step >= depth) & (step < depth + n_exp))
    def _():
        exp = step - depth
        count = cum_ref[n_tiles * n_exp + exp]
        big, rest = blocks_of(count)
        dim, ff = wg_ref.shape[1:]

        @pl.when(count == 0)
        def _():
            dw_ref[...] = jnp.zeros_like(dw_ref)

        def run(b, size):
            block = blk_ref[exp] + b
            side = block % 2

            @pl.when(block + 1 < blk_ref[n_exp])
            def _():
                for copy in loads(block + 1):
                    copy.start()

            def add(at, value):
                dw_ref[0, at, :] = jnp.where(b == 0, 0.0, dw_ref[0, at, :]) + value

            here = pl.ds(pl.multiple_of(off_ref[exp] + b * ROWS, ALIGN), size)
            live = lax.broadcasted_iota(jnp.int32, (size, 1), 0) < count - b * ROWS
            g_old = rows_ref[here, :]
            g_blk = jnp.where(live, g_old, jnp.zeros_like(g_old))
            da = dot(g_blk, wd_ref[0], ((1,), (1,)))
            for copy in loads(block):
                copy.wait()
            u = uv_in[side, 0, :size]
            v = uv_in[side, 1, :size]
            s = jax.nn.sigmoid(u)
            act = (u * s * v).astype(BF16)
            du = (da * v * s * (1.0 + u * (1.0 - s))).astype(BF16)
            dv = (da * u * s).astype(BF16)
            add(slice(2 * dim, 2 * dim + ff), dot(act, g_blk[:, :ff], ((0,), (0,))))
            add(slice(2 * dim + ff, 3 * dim), dot(act, g_blk[:, ff:], ((0,), (0,))))
            dxr = dot(du, wg_ref[0], ((1,), (1,))) + dot(dv, wu_ref[0], ((1,), (1,)))
            rows_ref[here, :] = dxr.astype(BF16)
            add(slice(0, dim), dot(x_in[side, :size], du, ((0,), (0,))))
            add(slice(dim, 2 * dim), dot(x_in[side, :size], dv, ((0,), (0,))))

        @pl.loop(0, big)
        def _(b):
            run(b, ROWS)

        @pl.when(rest > 0)
        def _():
            run(big, ROWS // 2)

    @pl.when(step >= depth + n_exp)
    def _():
        for i in range(per):
            tile = (step - depth - n_exp) * per + i
            cols = slice(i * TILE, (i + 1) * TILE)
            scatter_tile(n_exp, cum_ref, off_ref, rank_ref, None, tile, cols, rows_ref, win_ref, dx_ref)


def layer_sizes(depth, toks, w_gate, cap):
    tokens = depth * toks
    n_exp = w_gate.shape[0]
    n_tiles = tokens // TILE
    rows = n_exp * max(-(-cap // (ROWS // 2)) * (ROWS // 2), -(-cap // ALIGN) * ALIGN + WIN) + ROWS
    return n_tiles, n_exp, rows, n_exp * -(-cap // ROWS)


def expert_forward(depth, n_dev, counts, place, plan_col, x_col, w_gate, w_up, w_down, cap):
    n_tiles, n_exp, rows, blocks = layer_sizes(depth, x_col.shape[1], w_gate, cap)
    toks, dim = x_col.shape[1:]
    ff = w_gate.shape[2]
    first = lambda i: jnp.minimum(i, depth - 1)
    middle = lambda i: jnp.clip(i - depth, 0, n_exp - 1)
    last = lambda i: jnp.maximum(i - depth - n_exp, 0)

    def plan_at(part):
        return lambda i, counts, place: (jnp.where(i < depth, i, (place[0] + last(i)) % depth), place[0] + part, 0)

    wide = pl.BlockSpec((1, dim, ff), lambda i, *_: (middle(i), 0, 0))
    tall = pl.BlockSpec((1, ff, dim), lambda i, *_: (middle(i), 0, 0))
    any_space = pl.BlockSpec(memory_space=pl.ANY)
    outs = [pl.BlockSpec((toks, dim), lambda i, *_: (0, 0)) for d in range(depth)]
    shape = jax.ShapeDtypeStruct
    dma = pltpu.SemaphoreType.DMA
    result = pl.pallas_call(
        functools.partial(forward_kernel, depth, n_tiles, n_exp),
        grid_spec=pltpu.PrefetchScalarGridSpec(
            num_scalar_prefetch=2,
            grid=(2 * depth + n_exp,),
            in_specs=[
                pl.BlockSpec((1, n_exp, toks), plan_at(0)), pl.BlockSpec((1, n_exp, toks), plan_at(n_dev // n_exp)),
                pl.BlockSpec((toks, dim), lambda i, *_: (first(i), 0)), wide, wide, tall,
            ],
            out_specs=outs + [any_space, any_space],
            scratch_shapes=[
                pltpu.VMEM((rows, dim), BF16), pltpu.VMEM((n_exp * WIN, dim), BF16),
                pltpu.VMEM((2, ROWS, dim), BF16), pltpu.VMEM((2, 2, ROWS, ff), F32),
                pltpu.SMEM(((n_tiles + 1) * n_exp,), jnp.int32), pltpu.SMEM((n_exp,), jnp.int32),
                pltpu.SMEM((n_exp + 1,), jnp.int32), dma((2,)), dma((2,)),
            ],
        ),
        out_shape=[shape((toks, dim), F32)] * depth + [shape((blocks, ROWS, dim), BF16), shape((blocks, 2, ROWS, ff), F32)],
        compiler_params=pltpu.CompilerParams(dimension_semantics=("arbitrary",), vmem_limit_bytes=64_000_000),
        cost_estimate=pl.CostEstimate(flops=25_000_000_000, bytes_accessed=80_000_000, transcendentals=3_000_000),
        name="forward",
    )(counts, place, plan_col, plan_col, x_col.reshape(-1, dim), w_gate, w_up, w_down)
    return result[:depth], result[depth], result[depth + 1]


def expert_backward(depth, n_dev, counts, place, plan_col, dy_head, dy_tails, w_gate, w_up, w_down, x_saved, uv_saved, cap):
    n_tiles, n_exp, rows, blocks = layer_sizes(depth, plan_col.shape[2], w_gate, cap)
    head, dim = dy_head.shape[1:]
    tail = dy_tails[0].shape[0]
    toks = head + tail
    ff = w_gate.shape[2]
    first = lambda i: jnp.minimum(i, depth - 1)
    middle = lambda i: jnp.clip(i - depth, 0, n_exp - 1)
    last = lambda i: jnp.maximum(i - depth - n_exp, 0)

    def plan_at(part):
        return lambda i, counts, place: (jnp.where(i < depth, i, last(i)), place[0] + part, 0)

    wide = pl.BlockSpec((1, dim, ff), lambda i, *_: (middle(i), 0, 0))
    tall = pl.BlockSpec((1, ff, dim), lambda i, *_: (middle(i), 0, 0))
    any_space = pl.BlockSpec(memory_space=pl.ANY)
    shape = jax.ShapeDtypeStruct
    dma = pltpu.SemaphoreType.DMA
    return pl.pallas_call(
        functools.partial(backward_kernel, depth, n_tiles, n_exp),
        grid_spec=pltpu.PrefetchScalarGridSpec(
            num_scalar_prefetch=2,
            grid=(2 * depth + n_exp,),
            in_specs=[
                pl.BlockSpec((1, n_exp, toks), plan_at(0)), pl.BlockSpec((1, n_exp, toks), plan_at(n_dev // n_exp)),
                pl.BlockSpec((head, dim), lambda i, *_: (first(i), 0)),
                *[pl.BlockSpec((tail, dim), lambda i, *_: (0, 0))] * depth, wide, wide, tall, any_space, any_space,
            ],
            out_specs=[
                pl.BlockSpec((toks, dim), lambda i, *_: (last(i), 0)),
                pl.BlockSpec((1, 3 * dim, ff), lambda i, *_: (middle(i), 0, 0)),
            ],
            scratch_shapes=[
                pltpu.VMEM((rows, dim), BF16), pltpu.VMEM((n_exp * WIN, dim), BF16),
                pltpu.VMEM((2, ROWS, dim), BF16), pltpu.VMEM((2, 2, ROWS, ff), F32), pltpu.VMEM((tail, dim), BF16),
                pltpu.SMEM(((n_tiles + 1) * n_exp,), jnp.int32), pltpu.SMEM((n_exp,), jnp.int32),
                pltpu.SMEM((n_exp + 1,), jnp.int32), dma((2,)), dma((2,)),
            ],
        ),
        out_shape=[shape((depth * toks, dim), F32), shape((n_exp, 3 * dim, ff), F32)],
        compiler_params=pltpu.CompilerParams(dimension_semantics=("arbitrary",), vmem_limit_bytes=66_000_000),
        cost_estimate=pl.CostEstimate(flops=50_000_000_000, bytes_accessed=150_000_000, transcendentals=3_000_000),
        name="backward",
    )(counts, place, plan_col, plan_col, dy_head.reshape(-1, dim), *dy_tails, w_gate, w_up, w_down, x_saved, uv_saved)


def solution(mesh):
    n_dev = mesh.devices.size
    depth = n_dev // 8
    grid = Mesh(mesh.devices.reshape(depth, 2, 2, 2), ('z', 'y', 'x', 'c'))
    plane = ('y', 'x', 'c')
    spec = P(('z', 'y', 'x', 'c'))

    def local_step(x_tok, route_idx, gates, dy_tok, w_gate, w_up, w_down):
        tok_loc, top_k = route_idx.shape
        cap = depth * (2 * tok_loc * top_k // (n_dev * w_gate.shape[0] - 2))
        n_exp = 8 * w_gate.shape[0]
        head = tok_loc // 2
        x_col, dy_head, plan_col, wg_all, wu_all, wd_all = spread(
            depth, n_dev, head, x_tok, dy_tok, route_idx.T, gates.T.astype(F32), w_gate, w_up, w_down
        )
        turn = lambda a, d: lax.ppermute(a, 'z', [(i, (i + d) % depth) for i in range(depth)])
        x_col, dy_tail = lax.optimization_barrier((x_col, dy_tok[head:]))
        dy_tails = [dy_tail] + [turn(dy_tail, d) for d in range(1, depth)]
        place = lax.axis_index('z')
        per = tok_loc // TILE
        counts = lax.dynamic_slice(plan_col[:, 2 * n_dev : 2 * n_dev + per, :n_dev], (0, 0, place * n_exp), (depth, per, n_exp))
        where = (counts.reshape(-1).astype(jnp.int32), place.reshape(1), plan_col)
        y_parts, x_saved, uv_saved = expert_forward(depth, n_dev, *where, x_col, wg_all, wu_all, wd_all, cap)
        y_sum = y_parts[0]
        turned = [turn(y_parts[d], d) for d in range(1, depth)]
        dx_part, grads = expert_backward(
            depth, n_dev, *where, dy_head, dy_tails, wg_all, wu_all, wd_all, x_saved, uv_saved, cap
        )
        dx, dw = collect(depth, dx_part.reshape(depth, tok_loc, -1), grads)
        y_sum, turned, dx, dw = lax.optimization_barrier((y_sum, turned, dx, dw))
        y = functools.reduce(jnp.add, turned, y_sum).astype(BF16)
        dim, ff = w_gate.shape[1:]
        g_down = jnp.concatenate([dw[2 * dim : 2 * dim + ff], dw[2 * dim + ff :]], axis=1)
        return y, dx, dw[None, :dim], dw[None, dim : 2 * dim], g_down[None]

    return jax.shard_map(local_step, mesh=grid, in_specs=(spec,) * 7, out_specs=(spec,) * 5, check_vma=False)
```

```python
import functools

import jax
import jax.numpy as jnp
from jax import lax
from jax.experimental import pallas as pl
from jax.experimental.pallas import tpu as pltpu
from jax.sharding import Mesh, PartitionSpec as P

F32 = jnp.float32
BF16 = jnp.bfloat16
TILE = 256
WIN = 128
ALIGN = 16
ROWS = 512


def dot(a, b, dims=((1,), (0,))):
    return lax.dot_general(a, b, (dims, ((), ())), preferred_element_type=F32)


MESH = pl.DeviceIdType.MESH


def hop(src, dst, send_sem, recv_sem, **where):
    return pltpu.make_async_remote_copy(
        src_ref=src, dst_ref=dst, send_sem=send_sem, recv_sem=recv_sem, device_id=where, device_id_type=MESH
    )


def meet(depth, z, y, x, c):
    barrier = pltpu.get_barrier_semaphore()
    for where in ({'y': 1 - y}, {'x': 1 - x}, {'c': 1 - c}):
        pl.semaphore_signal(barrier, inc=1, device_id=where, device_id_type=MESH)

    @pl.when(z > 0)
    def _():
        pl.semaphore_signal(barrier, inc=1, device_id={'z': z - 1}, device_id_type=MESH)

    @pl.when(z < depth - 1)
    def _():
        pl.semaphore_signal(barrier, inc=1, device_id={'z': z + 1}, device_id_type=MESH)

    inner = (z > 0) & (z < depth - 1)

    @pl.when(inner)
    def _():
        pl.semaphore_wait(barrier, 5)

    @pl.when(jnp.logical_not(inner))
    def _():
        pl.semaphore_wait(barrier, 4)


def make_plan(experts, route_ref, gate_ref, plan):
    top_k, toks = route_ref.shape
    route = route_ref[...]
    gates = gate_ref[...].astype(F32)
    below = lax.broadcasted_iota(jnp.int32, (TILE, TILE), 0) < lax.broadcasted_iota(jnp.int32, (TILE, TILE), 1)
    below = jnp.where(below, 1.0, 0.0).astype(BF16)
    ones = jnp.ones((16, TILE), BF16)
    ids = lax.broadcasted_iota(jnp.int32, (experts, toks), 0)
    member = jnp.zeros((experts, toks), F32)
    gate = jnp.zeros((experts, toks), F32)
    for k in range(top_k):
        hit = jnp.broadcast_to(route[k : k + 1, :], (experts, toks)) == ids
        member = jnp.where(hit, 1.0, member)
        gate = jnp.where(hit, jnp.broadcast_to(gates[k : k + 1, :], (experts, toks)), gate)
    ranks, counts = [], []
    for t in range(toks // TILE):
        part = member[:, t * TILE : (t + 1) * TILE]
        ranks.append(jnp.where(part > 0.5, dot(part.astype(BF16), below), -4096.0))
        counts.append(dot(ones, part.astype(BF16), ((1,), (1,))))
    rank = jnp.concatenate(ranks, axis=1)
    for p in range(experts // 8):
        both = jnp.concatenate([rank[8 * p : 8 * p + 8], gate[8 * p : 8 * p + 8]], axis=0)
        plan[16 * p : 16 * p + 16, :] = both.astype(BF16)
    which = lax.broadcasted_iota(jnp.int32, (16, experts), 0)
    count = functools.reduce(jnp.add, [jnp.where(which == t, c, 0.0) for t, c in enumerate(counts)])
    plan[2 * experts :, :] = jnp.zeros((16, toks), BF16)
    plan[2 * experts :, :experts] = count.astype(BF16)


def spread_kernel(
    depth, experts, x_ref, dy_ref, route_ref, gate_ref, wg_ref, wu_ref, wd_ref,
    x_out, dy_out, tail_out, plan_out, wg_out, wu_out, wd_out,
    stage_t, stage_w, stage_d, plan, own_sem, z_send, z_recv, p_send, p_recv, c_send, c_recv,
):
    z, y, x, c = (lax.axis_index(a) for a in 'zyxc')
    slot = lambda yy, xx: yy * 4 + xx * 2 + c
    own, by_x, by_y, far = slot(y, x), slot(y, 1 - x), slot(1 - y, x), slot(1 - y, 1 - x)
    weights = ((wg_ref, wg_out), (wu_ref, wu_out), (wd_ref, wd_out))
    dy_head = dy_ref.at[pl.ds(0, dy_out.shape[1]), :]
    arrays = ((x_ref, x_out), (plan, plan_out), (dy_head, dy_out))
    sent = []

    def half(ref, where, h):
        rows = ref.shape[1] // 2
        return ref.at[where, pl.ds(h * rows, rows), :]

    def own_half(part, h, side):
        src, out = weights[part]
        where = {'x': 1 - x} if side == 0 else {'y': 1 - y}
        return hop(half(src, 0, h), half(out, own, h), p_send.at[side, part, h], p_recv.at[side, part, h], **where)

    def onward(part, h):
        at = half(weights[part][1], by_x if h == 0 else by_y, h)
        where = {'y': 1 - y} if h == 0 else {'x': 1 - x}
        return hop(at, at, p_send.at[2, part, h], p_recv.at[2, part, h], **where)

    def landed(part, h, kind):
        at = half(weights[part][1], (by_x, by_y, far)[kind], h)
        hop(at, at, p_send.at[kind, part, h], p_recv.at[kind, part, h], c=1 - c).wait_recv()

    def across(part, h, kind):
        at = half(weights[part][1], (by_x, by_y, far)[kind], h)
        return hop(at, at, c_send.at[kind, part, h], c_recv.at[kind, part, h], c=1 - c)

    def across_own(part, h):
        src, out = weights[part]
        return hop(half(src, 0, h), half(out, own, h), c_send.at[3, part, h], c_recv.at[3, part, h], c=1 - c)

    def crossed(part, h, kind):
        twin = lambda yy, xx: yy * 4 + xx * 2 + 1 - c
        where = (twin(y, 1 - x), twin(1 - y, x), twin(1 - y, 1 - x), twin(y, x))[kind]
        at = half(weights[part][1], where, h)
        hop(at, at, c_send.at[kind, part, h], c_recv.at[kind, part, h], c=1 - c).wait_recv()

    def go(copy):
        copy.start()
        sent.append((None, copy))

    def along(k, dist, up):
        src, out = arrays[k]
        at = out.at[z - dist if up else z + dist]
        side = 0 if up else 1
        return hop(src if dist == 0 else at, at, z_send.at[side, k, dist], z_recv.at[side, k, dist], z=z + 1 if up else z - 1)

    def start_along(k, dist):
        for up in (True, False):
            cond = (z >= dist) & (z < depth - 1) if up else (z + dist < depth) & (z > 0)

            @pl.when(cond)
            def _(up=up):
                along(k, dist, up).start()

            sent.append((cond, along(k, dist, up)))

    def await_along(k, dist):
        for up in (True, False):
            @pl.when(z > dist if up else z + dist + 1 < depth)
            def _(up=up):
                at = arrays[k][1].at[z - dist - 1 if up else z + dist + 1]
                side = 0 if up else 1
                hop(at, at, z_send.at[side, k, dist], z_recv.at[side, k, dist], c=1 - c).wait_recv()

        if dist + 1 < depth - 1:
            start_along(k, dist + 1)

    copies = []
    for i, (src, buf, out) in enumerate((
        (x_ref, stage_t.at[0], x_out.at[z]), (dy_head, stage_t.at[1, pl.ds(0, dy_out.shape[1]), :], dy_out.at[z]),
        (dy_ref.at[pl.ds(dy_out.shape[1], tail_out.shape[0]), :], stage_t.at[1, pl.ds(dy_out.shape[1], tail_out.shape[0]), :], tail_out),
        (wg_ref.at[0], stage_w.at[0], wg_out.at[own]), (wu_ref.at[0], stage_w.at[1], wu_out.at[own]),
        (wd_ref.at[0], stage_d, wd_out.at[own]),
    )):
        copies.append((pltpu.make_async_copy(src, buf, own_sem.at[i]), pltpu.make_async_copy(buf, out, own_sem.at[i])))
        copies[-1][0].start()

    meet(depth, z, y, x, c)
    start_along(0, 0)
    for part in range(3):
        go(own_half(part, 0, 0))
        go(own_half(part, 1, 1))
    for part in range(3):
        go(own_half(part, 1, 0))
        go(own_half(part, 0, 1))
    for part in range(3):
        for h in range(2):
            go(across_own(part, h))
    make_plan(experts, route_ref, gate_ref, plan)
    start_along(1, 0)
    start_along(2, 0)
    copies.append((None, pltpu.make_async_copy(plan, plan_out.at[z], own_sem.at[6])))
    for i, (load, store) in enumerate(copies):
        if load is not None:
            load.wait()
        store.start()

    def relay(part, h):
        landed(part, h, h)
        go(onward(part, h))
        go(across(part, h, h))

    def relay_twin(part, h):
        landed(part, h, 1 - h)
        go(across(part, h, 1 - h))

    def relay_far(part):
        for h in range(2):
            landed(part, h, 2)
            go(across(part, h, 2))

    for part in range(2):
        relay(part, 0)
        relay(part, 1)
    await_along(0, 0)
    await_along(1, 0)
    relay(2, 0)
    relay(2, 1)
    await_along(2, 0)
    for part in range(2):
        relay_twin(part, 1)
        relay_twin(part, 0)
    await_along(0, 1)
    await_along(1, 1)
    relay_twin(2, 1)
    relay_twin(2, 0)
    await_along(2, 1)
    relay_far(0)
    relay_far(1)
    await_along(0, 2)
    await_along(1, 2)
    relay_far(2)
    await_along(2, 2)
    for part in range(3):
        for h in range(2):
            for kind in range(4):
                crossed(part, h, kind)
    for cond, copy in sent:
        if cond is None:
            copy.wait_send()
        else:
            @pl.when(cond)
            def _(copy=copy):
                copy.wait_send()
    for _, store in copies:
        store.wait()


def spread(depth, experts, head, x_tok, dy_tok, route, gate, w_gate, w_up, w_down):
    toks, dim = x_tok.shape
    ff = w_down.shape[1]
    any_space = pl.BlockSpec(memory_space=pl.ANY)
    vmem = pl.BlockSpec(memory_space=pltpu.VMEM)
    rows = 2 * experts + 16
    shape = jax.ShapeDtypeStruct
    dma = pltpu.SemaphoreType.DMA
    return pl.pallas_call(
        functools.partial(spread_kernel, depth, experts),
        in_specs=[any_space, any_space, vmem, vmem, any_space, any_space, any_space],
        out_specs=[any_space] * 7,
        out_shape=[
            shape((depth, toks, dim), BF16), shape((depth, head, dim), BF16), shape((toks - head, dim), BF16), shape((depth, rows, toks), BF16),
            shape((8, dim, ff), BF16), shape((8, dim, ff), BF16), shape((8, ff, dim), BF16),
        ],
        scratch_shapes=[
            pltpu.VMEM((2, toks, dim), BF16), pltpu.VMEM((2, dim, ff), BF16), pltpu.VMEM((ff, dim), BF16),
            pltpu.VMEM((rows, toks), BF16), dma((7,)), dma((2, 3, depth)), dma((2, 3, depth)),
            dma((3, 3, 2)), dma((3, 3, 2)), dma((4, 3, 2)), dma((4, 3, 2)),
        ],
        compiler_params=pltpu.CompilerParams(collective_id=0, has_side_effects=True),
        name="spread",
    )(x_tok, dy_tok, route, gate, w_gate, w_up, w_down)


CHUNK = 128
BAND = 64
TURNS = (4, 14, 20, 22)
FINISH = 3
RING = 6


def collect_kernel(
    depth, dx_ref, g_ref, dx_out, gate_out, up_out, down_out, twin,
    z_land, x_land, y_land, x_last, y_last, total, x_buf, y_buf, f_buf, z_buf,
    t_sem, x_load, y_load, f_load, z_load, z_send, z_recv, x_send, x_recv, y_send, y_recv, c_send, c_recv,
):
    z, y, x, c = (lax.axis_index(a) for a in 'zyxc')
    cell = lambda yy, xx: yy * 2 + xx
    mine, by_x, by_y, far = cell(y, x), cell(y, 1 - x), cell(1 - y, x), cell(1 - y, 1 - x)
    bands = dx_ref.shape[1] // BAND
    n_part = g_ref.shape[1] // CHUNK // 2
    n_col = (depth - 1) * bands
    n_link = 3 * n_part
    piece = 4 * CHUNK
    order = (far, by_x, by_y, mine)
    rows = lambda i: pl.ds(pl.multiple_of(i * CHUNK, CHUNK), CHUNK)

    def swap(kind, q):
        at = pl.ds(q * piece, piece)
        return hop(g_ref.at[2 * order[kind] + 1 - c, at, :], twin.at[order[kind], at, :], c_send.at[kind, q], c_recv.at[kind, q], c=1 - c)

    half = n_part // 4
    swaps = [(0, q + h * half) for q in range(half) for h in range(2)]
    swaps += [(1 + h, q + h * half) for q in range(half) for h in range(2)]
    swaps += [(2 - h, q + h * half) for q in range(half) for h in range(2)]
    swaps += [(3, q + h * half) for q in range(half) for h in range(2)]

    own_total = pltpu.make_async_copy(dx_ref.at[z], total, t_sem)
    own_total.start()
    meet(depth, z, y, x, c)
    for kind, q in swaps:
        swap(kind, q).start()

    def link_item(side, i):
        leg = i // n_part
        j = i % n_part
        near, other = (by_x, by_y) if side == 0 else (by_y, by_x)
        kind_near, kind_other = (1, 2) if side == 0 else (2, 1)
        first = jnp.where(leg < 2, side, 1 - side)
        chunk = first * n_part + j
        expert = jnp.where(leg == 0, far, near)
        kind = jnp.where(leg == 0, 0, kind_near)
        return leg, j, chunk, expert, kind

    def fetch(chunk, expert, kind, fresh, buf, sems):
        @pl.when(fresh)
        def _():
            for k in range(4):
                @pl.when(kind == k)
                def _(k=k):
                    at = pl.ds(pl.multiple_of(chunk // 4 * piece, piece), piece)
                    q = chunk // 4
                    hop(twin.at[order[k], at, :], twin.at[order[k], at, :], c_send.at[k, q], c_recv.at[k, q], c=1 - c).wait_recv()

        pltpu.make_async_copy(g_ref.at[2 * expert + c, rows(chunk), :], buf.at[0], sems.at[0]).start()
        pltpu.make_async_copy(twin.at[expert, rows(chunk), :], buf.at[1], sems.at[1]).start()

    def fetched(buf, sems):
        pltpu.make_async_copy(g_ref.at[0, rows(0), :], buf.at[0], sems.at[0]).wait()
        pltpu.make_async_copy(twin.at[0, rows(0), :], buf.at[1], sems.at[1]).wait()

    links = (
        (x_buf, x_load, x_send, x_recv, x_land, x_last, {'x': 1 - x}),
        (y_buf, y_load, y_send, y_recv, y_land, y_last, {'y': 1 - y}),
    )

    def landing(side, i):
        land, last = links[side][4], links[side][5]
        return land, last

    def link_send(side, i, wait_only=False):
        buf, _, send, recv, land, last, where = links[side]
        src = buf.at[i % RING, 0]

        @pl.when(i < 2 * n_part)
        def _():
            copy = hop(src, land.at[jnp.minimum(i, 2 * n_part - 1)], send.at[i], recv.at[i], **where)
            copy.wait_send() if wait_only else copy.start()

        @pl.when(i >= 2 * n_part)
        def _():
            copy = hop(src, last.at[jnp.maximum(i - 2 * n_part, 0)], send.at[i], recv.at[i], **where)
            copy.wait_send() if wait_only else copy.start()

    def landed(side, ref, i):
        recv, send = links[side][3], links[side][2]
        hop(ref, ref, send.at[i], recv.at[i], c=1 - c).wait_recv()

    def link_prepare(side, i):
        buf, load = links[side][0], links[side][1]

        @pl.when((i >= RING) & (i < n_link))
        def _():
            link_send(side, i - RING, wait_only=True)

        @pl.when(i < n_link)
        def _():
            leg, j, chunk, expert, kind = link_item(side, i)
            fetch(chunk, expert, kind, j % 4 == 0, buf.at[i % RING], load.at[i % RING])

    def link_turn(side, i):
        buf, load = links[side][0], links[side][1]
        other_land = links[1 - side][4]

        @pl.when(i < n_link)
        def _():
            b = i % RING
            fetched(buf.at[b], load.at[b])
            buf[b, 0] += buf[b, 1]

            @pl.when(i >= 2 * n_part)
            def _():
                j = i - 2 * n_part
                landed(1 - side, other_land.at[j], j)
                buf[b, 0] += other_land[j]

            link_send(side, i)

    def last_prepare(h, j):
        @pl.when((j >= 0) & (j < n_part))
        def _():
            fetch(h * n_part + j, mine, 3, j % 4 == 0, f_buf.at[h, j % 2], f_load.at[h, j % 2])

    def last_turn(h, j):
        @pl.when((j >= 0) & (j < n_part))
        def _():
            land, last = links[h][4], links[1 - h][5]
            fetched(f_buf.at[h, j % 2], f_load.at[h, j % 2])
            landed(h, land.at[n_part + j], n_part + j)
            landed(1 - h, last.at[j], 2 * n_part + j)
            value = f_buf[h, j % 2, 0] + f_buf[h, j % 2, 1] + (land[n_part + j] + last[j])
            chunk = h * n_part + j
            tall = gate_out.shape[0] // CHUNK
            places = ((0, tall, gate_out, 0), (tall, 2 * tall, up_out, 0), (2 * tall, 5 * tall // 2, down_out, 0), (5 * tall // 2, 3 * tall, down_out, 1))
            for first, end, out, side in places:
                if first < (h + 1) * n_part and end > h * n_part:
                    @pl.when((chunk >= first) & (chunk < end))
                    def _(first=first, out=out, side=side):
                        cols = pl.ds(side * value.shape[1], value.shape[1])
                        out[rows(chunk - first), cols] = value

    def column(side, k):
        role = z if side == 0 else depth - 1 - z
        goal = depth - 1 - k // bands
        block = goal if side == 0 else depth - 1 - goal
        slot = block + 1 if side == 0 else block
        at = pl.ds(pl.multiple_of(k % bands * BAND, BAND), BAND)
        return role, goal, block, slot, at

    def column_copy(side, k, src):
        _, _, _, slot, at = column(side, k)
        return hop(src, z_land.at[slot, at, :], z_send.at[side, k], z_recv.at[side, k], z=z + 1 if side == 0 else z - 1)

    def turn_of(side, t):
        role = z if side == 0 else depth - 1 - z
        return t - functools.reduce(lambda late, r: jnp.where(role == r, TURNS[r], late), range(1, depth), TURNS[0])

    def column_prepare(side, t):
        k = turn_of(side, t)
        kk = jnp.clip(k, 0, n_col - 1)
        role, goal, block, slot, at = column(side, kk)

        @pl.when((k >= 0) & (k < n_col) & (role > 0) & (goal > role))
        def _():
            pltpu.make_async_copy(dx_ref.at[block, at, :], z_buf.at[side, kk % 2], z_load.at[side, kk % 2]).start()

    def column_turn(side, t):
        k = turn_of(side, t)
        kk = jnp.clip(k, 0, n_col - 1)
        role, goal, block, slot, at = column(side, kk)
        live = (k >= 0) & (k < n_col) & (goal >= role)

        @pl.when(live & (role == 0))
        def _():
            column_copy(side, kk, dx_ref.at[block, at, :]).start()

        @pl.when(live & (role > 0))
        def _():
            here = z_land.at[slot, at, :]
            hop(here, here, z_send.at[side, kk], z_recv.at[side, kk], c=1 - c).wait_recv()

            @pl.when(goal > role)
            def _():
                pltpu.make_async_copy(dx_ref.at[block, at, :], z_buf.at[side, kk % 2], z_load.at[side, kk % 2]).wait()
                z_land[slot, at, :] += z_buf[side, kk % 2]
                column_copy(side, kk, here).start()

            @pl.when(goal == role)
            def _():
                total[at, :] += z_land[slot, at, :]

    def prepare(t):
        for side in range(2):
            link_prepare(side, t)
            column_prepare(side, t)
            last_prepare(side, t - 2 * n_part - FINISH)

    prepare(jnp.int32(0))
    own_total.wait()
    steps = max(max(TURNS) + n_col, n_link + FINISH)

    @pl.loop(0, steps)
    def _(t):
        prepare(t + 1)
        for side in range(2):
            link_turn(side, t)
        for side in range(2):
            column_turn(side, t)
        for side in range(2):
            last_turn(side, t - 2 * n_part - FINISH)

    dx_out[...] = total[...].astype(BF16)

    @pl.loop(n_link - RING, n_link)
    def _(i):
        for side in range(2):
            link_send(side, i, wait_only=True)

    @pl.loop(0, n_col)
    def _(k):
        for side in range(2):
            role, goal, block, slot, at = column(side, k)

            @pl.when(goal > role)
            def _():
                column_copy(side, k, z_land.at[slot, at, :]).wait_send()

    for kind, q in swaps:
        swap(kind, q).wait_send()


def collect(depth, dx_part, grads):
    toks, dim = dx_part.shape[1:]
    height, ff = grads.shape[1:]
    n_part = height // CHUNK // 2
    n_col = (depth - 1) * (toks // BAND)
    any_space = pl.BlockSpec(memory_space=pl.ANY)
    vmem = pl.BlockSpec(memory_space=pltpu.VMEM)
    shape = jax.ShapeDtypeStruct
    dma = pltpu.SemaphoreType.DMA
    message = (CHUNK, ff)
    return pl.pallas_call(
        functools.partial(collect_kernel, depth),
        in_specs=[any_space, any_space],
        out_specs=[vmem, vmem, vmem, vmem, any_space],
        out_shape=[pltpu.VMEM((toks, dim), BF16), pltpu.VMEM((dim, ff), F32), pltpu.VMEM((dim, ff), F32), pltpu.VMEM((ff, dim), F32), shape((4, height, ff), F32)],
        scratch_shapes=[
            pltpu.VMEM((depth + 1, toks, dim), F32),
            pltpu.VMEM((2 * n_part, *message), F32), pltpu.VMEM((2 * n_part, *message), F32),
            pltpu.VMEM((n_part, *message), F32), pltpu.VMEM((n_part, *message), F32),
            pltpu.VMEM((toks, dim), F32),
            pltpu.VMEM((RING, 2, *message), F32), pltpu.VMEM((RING, 2, *message), F32),
            pltpu.VMEM((2, 2, 2, *message), F32), pltpu.VMEM((2, 2, BAND, dim), F32),
            dma, dma((RING, 2)), dma((RING, 2)), dma((2, 2, 2)), dma((2, 2)),
            dma((2, n_col)), dma((2, n_col)), dma((3 * n_part,)), dma((3 * n_part,)), dma((3 * n_part,)), dma((3 * n_part,)),
            dma((4, height // CHUNK // 4)), dma((4, height // CHUNK // 4)),
        ],
        compiler_params=pltpu.CompilerParams(collective_id=1, has_side_effects=True, vmem_limit_bytes=46_000_000),
        name="collect",
    )(dx_part, grads)[:4]


def count_up(n_tiles, n_exp, count_ref, cum_ref, off_ref, blk_ref):
    base = jnp.int32(0)
    block = jnp.int32(0)
    for exp in range(n_exp):
        run = jnp.int32(0)
        cum_ref[exp] = run
        for tile in range(n_tiles):
            run += count_ref[tile * n_exp + exp]
            cum_ref[(tile + 1) * n_exp + exp] = run
        off_ref[exp] = base
        blk_ref[exp] = block
        big, rest = blocks_of(run)
        block += big + rest
        base += jnp.maximum(big * ROWS + rest * (ROWS // 2), (run + ALIGN - 1) // ALIGN * ALIGN + WIN)
    blk_ref[n_exp] = block


def blocks_of(count):
    big = (count + ROWS // 2 - 1) // ROWS
    return big, (count > big * ROWS).astype(jnp.int32)


def span(n_exp, cum_ref, tile, exp):
    lo = cum_ref[tile * n_exp + exp]
    hi = cum_ref[(tile + 1) * n_exp + exp]
    return lo, hi, (lo // ALIGN) * ALIGN


def gather_tile(n_exp, cum_ref, off_ref, plan, gated, tile, cols, toks, rows_ref):
    rank, gate = plan[:n_exp, cols], plan[n_exp:, cols]
    row = lax.broadcasted_iota(jnp.int32, (WIN, TILE), 0).astype(F32)

    def window(exp, lo, start):
        hit = rank[exp : exp + 1] == row + (start - lo).astype(F32)
        take = jnp.where(hit, gate[exp : exp + 1] if gated else 1.0, 0.0).astype(BF16)
        return dot(take, toks[...]).astype(BF16)

    def rows_at(exp, start, size):
        return pl.ds(pl.multiple_of(off_ref[exp] + start, ALIGN), size)

    spans = [span(n_exp, cum_ref, tile, exp) for exp in range(n_exp)]
    for exp, (lo, hi, start) in enumerate(spans):
        value = window(exp, lo, start)
        head = rows_at(exp, start, ALIGN)
        fresh = lax.broadcasted_iota(jnp.int32, (ALIGN, 1), 0) + start >= lo
        rows_ref[head, :] = jnp.where(fresh, value[:ALIGN], rows_ref[head, :])
        rows_ref[rows_at(exp, start + ALIGN, WIN - ALIGN), :] = value[ALIGN:]
    most = functools.reduce(jnp.maximum, [hi - start for lo, hi, start in spans])

    @pl.when(most > WIN)
    def _more():
        for exp, (lo, hi, start) in enumerate(spans):
            @pl.loop(1, (hi - start + WIN - 1) // WIN)
            def _(w):
                rows_ref[rows_at(exp, start + w * WIN, WIN), :] = window(exp, lo, start + w * WIN)


def scatter_tile(n_exp, cum_ref, off_ref, plan_t, gated, tile, cols, rows_ref, win_ref, out_ref):
    column = lax.broadcasted_iota(jnp.int32, (TILE, WIN), 1).astype(F32)

    def window(exp, lo, start):
        hit = plan_t[cols, exp : exp + 1] == column + (start - lo).astype(F32)
        put = jnp.where(hit, plan_t[cols, n_exp + exp : n_exp + exp + 1] if gated else 1.0, 0.0).astype(BF16)
        return put, rows_ref[pl.ds(pl.multiple_of(off_ref[exp] + start, ALIGN), WIN), :]

    spans = [span(n_exp, cum_ref, tile, exp) for exp in range(n_exp)]
    puts = []
    for exp, (lo, hi, start) in enumerate(spans):
        put, block = window(exp, lo, start)
        puts.append(put)
        win_ref[exp * WIN : (exp + 1) * WIN, :] = block
    out_ref[cols, :] = dot(jnp.concatenate(puts, axis=1), win_ref[...])
    most = functools.reduce(jnp.maximum, [hi - start for lo, hi, start in spans])

    @pl.when(most > WIN)
    def _more():
        for exp, (lo, hi, start) in enumerate(spans):
            @pl.loop(1, (hi - start + WIN - 1) // WIN)
            def _(w):
                put, block = window(exp, lo, start + w * WIN)
                out_ref[cols, :] += dot(put, block)


def forward_kernel(
    depth, n_tiles, n_exp, count_ref, z_ref, plan_ref, x_ref, wg_ref, wu_ref, wd_ref,
    *refs,
):
    y_refs, refs = refs[:depth], refs[depth:]
    xs_ref, uv_ref, rows_ref, win_ref, x_out, uv_out, y_buf, cum_ref, off_ref, blk_ref, x_sem, uv_sem, y_sem = refs
    step = pl.program_id(0)
    per = n_tiles // depth

    @pl.when(step == 0)
    def _():
        count_up(n_tiles, n_exp, count_ref, cum_ref, off_ref, blk_ref)

    @pl.when(step < depth)
    def _():
        plan = plan_ref[0].astype(F32)
        for i in range(per):
            cols = slice(i * TILE, (i + 1) * TILE)
            gather_tile(n_exp, cum_ref, off_ref, plan, False, step * per + i, cols, x_ref.at[cols, :], rows_ref)

    def saves(block):
        side = block % 2
        return (
            pltpu.make_async_copy(x_out.at[side], xs_ref.at[block], x_sem.at[side]),
            pltpu.make_async_copy(uv_out.at[side], uv_ref.at[block], uv_sem.at[side]),
        )

    @pl.when((step >= depth) & (step < depth + n_exp))
    def _():
        exp = step - depth
        count = cum_ref[n_tiles * n_exp + exp]
        big, rest = blocks_of(count)

        def run(b, size):
            block = blk_ref[exp] + b
            side = block % 2

            @pl.when(block >= 2)
            def _():
                for copy in saves(block - 2):
                    copy.wait()

            here = pl.ds(pl.multiple_of(off_ref[exp] + b * ROWS, ALIGN), size)
            live = lax.broadcasted_iota(jnp.int32, (size, 1), 0) < count - b * ROWS
            x_old = rows_ref[here, :]
            x_out[side, :size] = jnp.where(live, x_old, jnp.zeros_like(x_old))
            u = dot(x_out[side, :size], wg_ref[0])
            v = dot(x_out[side, :size], wu_ref[0])
            uv_out[side, 0, :size] = u
            uv_out[side, 1, :size] = v
            act = (u * jax.nn.sigmoid(u) * v).astype(BF16)
            rows_ref[here, :] = dot(act, wd_ref[0]).astype(BF16)
            for copy in saves(block):
                copy.start()

        @pl.loop(0, big)
        def _(b):
            run(b, ROWS)

        @pl.when(rest > 0)
        def _():
            run(big, ROWS // 2)

    @pl.when(step == depth + n_exp)
    def _():
        total = blk_ref[n_exp]
        for back in (2, 1):
            @pl.when(total >= back)
            def _():
                for copy in saves(total - back):
                    copy.wait()

    d = step - depth - n_exp

    def y_copy(d, k):
        return pltpu.make_async_copy(y_buf.at[k % 2], y_refs[k], y_sem.at[k % 2])

    @pl.when(d >= 0)
    def _():
        for k in range(2, depth):
            @pl.when(d == k)
            def _(k=k):
                y_copy(d, k - 2).wait()

        plan_t = jnp.transpose(plan_ref[0].astype(F32))
        for i in range(per):
            tile = ((z_ref[0] + d) % depth) * per + i
            cols = slice(i * TILE, (i + 1) * TILE)
            scatter_tile(n_exp, cum_ref, off_ref, plan_t, True, tile, cols, rows_ref, win_ref, y_buf.at[d % 2])
        for k in range(depth):
            @pl.when(d == k)
            def _(k=k):
                y_copy(d, k).start()

    @pl.when(d == depth - 1)
    def _():
        y_copy(d, depth - 2).wait()
        y_copy(d, depth - 1).wait()


def backward_kernel(
    depth, n_tiles, n_exp, count_ref, z_ref, plan_ref, head_ref, *refs,
):
    tails, refs = refs[:depth], refs[depth:]
    wg_ref, wu_ref, wd_ref, xs_ref, uv_ref, dx_ref, dw_ref = refs[:7]
    rows_ref, win_ref, x_in, uv_in, tail_ref, cum_ref, off_ref, blk_ref, x_sem, uv_sem = refs[7:]
    step = pl.program_id(0)
    per = n_tiles // depth

    @pl.when(step == 0)
    def _():
        count_up(n_tiles, n_exp, count_ref, cum_ref, off_ref, blk_ref)

    @pl.when(step < depth)
    def _():
        for d in range(depth):
            @pl.when((z_ref[0] + depth - step) % depth == d)
            def _():
                tail_ref[...] = tails[d][...]

        plan = plan_ref[0].astype(F32)
        split = head_ref.shape[0]
        for i in range(per):
            cols = slice(i * TILE, (i + 1) * TILE)
            toks = head_ref.at[cols, :] if i * TILE < split else tail_ref.at[slice(i * TILE - split, (i + 1) * TILE - split), :]
            gather_tile(n_exp, cum_ref, off_ref, plan, True, step * per + i, cols, toks, rows_ref)

    def loads(block):
        side = block % 2
        return (
            pltpu.make_async_copy(xs_ref.at[block], x_in.at[side], x_sem.at[side]),
            pltpu.make_async_copy(uv_ref.at[block], uv_in.at[side], uv_sem.at[side]),
        )

    @pl.when((step == depth - 1) & (blk_ref[n_exp] > 0))
    def _():
        for copy in loads(0):
            copy.start()

    @pl.when((step >= depth) & (step < depth + n_exp))
    def _():
        exp = step - depth
        count = cum_ref[n_tiles * n_exp + exp]
        big, rest = blocks_of(count)
        dim, ff = wg_ref.shape[1:]

        @pl.when(count == 0)
        def _():
            dw_ref[...] = jnp.zeros_like(dw_ref)

        def run(b, size):
            block = blk_ref[exp] + b
            side = block % 2

            @pl.when(block + 1 < blk_ref[n_exp])
            def _():
                for copy in loads(block + 1):
                    copy.start()

            def add(at, value):
                dw_ref[0, at, :] = jnp.where(b == 0, 0.0, dw_ref[0, at, :]) + value

            here = pl.ds(pl.multiple_of(off_ref[exp] + b * ROWS, ALIGN), size)
            live = lax.broadcasted_iota(jnp.int32, (size, 1), 0) < count - b * ROWS
            g_old = rows_ref[here, :]
            g_blk = jnp.where(live, g_old, jnp.zeros_like(g_old))
            da = dot(g_blk, wd_ref[0], ((1,), (1,)))
            for copy in loads(block):
                copy.wait()
            u = uv_in[side, 0, :size]
            v = uv_in[side, 1, :size]
            s = jax.nn.sigmoid(u)
            act = (u * s * v).astype(BF16)
            du = (da * v * s * (1.0 + u * (1.0 - s))).astype(BF16)
            dv = (da * u * s).astype(BF16)
            add(slice(2 * dim, 2 * dim + ff), dot(act, g_blk[:, :ff], ((0,), (0,))))
            add(slice(2 * dim + ff, 3 * dim), dot(act, g_blk[:, ff:], ((0,), (0,))))
            dxr = dot(du, wg_ref[0], ((1,), (1,))) + dot(dv, wu_ref[0], ((1,), (1,)))
            rows_ref[here, :] = dxr.astype(BF16)
            add(slice(0, dim), dot(x_in[side, :size], du, ((0,), (0,))))
            add(slice(dim, 2 * dim), dot(x_in[side, :size], dv, ((0,), (0,))))

        @pl.loop(0, big)
        def _(b):
            run(b, ROWS)

        @pl.when(rest > 0)
        def _():
            run(big, ROWS // 2)

    @pl.when(step >= depth + n_exp)
    def _():
        plan_t = jnp.transpose(plan_ref[0].astype(F32))
        for i in range(per):
            tile = (step - depth - n_exp) * per + i
            cols = slice(i * TILE, (i + 1) * TILE)
            scatter_tile(n_exp, cum_ref, off_ref, plan_t, False, tile, cols, rows_ref, win_ref, dx_ref)


def layer_sizes(depth, toks, w_gate, cap):
    tokens = depth * toks
    n_exp = w_gate.shape[0]
    n_tiles = tokens // TILE
    rows = n_exp * max(-(-cap // (ROWS // 2)) * (ROWS // 2), -(-cap // ALIGN) * ALIGN + WIN) + ROWS
    return n_tiles, n_exp, rows, n_exp * -(-cap // ROWS)


def expert_forward(depth, counts, place, plan_col, x_col, w_gate, w_up, w_down, cap):
    n_tiles, n_exp, rows, blocks = layer_sizes(depth, x_col.shape[1], w_gate, cap)
    toks, dim = x_col.shape[1:]
    ff = w_gate.shape[2]
    first = lambda i: jnp.minimum(i, depth - 1)
    middle = lambda i: jnp.clip(i - depth, 0, n_exp - 1)
    last = lambda i: jnp.maximum(i - depth - n_exp, 0)

    plan_at = lambda i, counts, place: (jnp.where(i < depth, i, (place[0] + last(i)) % depth), place[0], 0)

    wide = pl.BlockSpec((1, dim, ff), lambda i, *_: (middle(i), 0, 0))
    tall = pl.BlockSpec((1, ff, dim), lambda i, *_: (middle(i), 0, 0))
    any_space = pl.BlockSpec(memory_space=pl.ANY)
    shape = jax.ShapeDtypeStruct
    dma = pltpu.SemaphoreType.DMA
    result = pl.pallas_call(
        functools.partial(forward_kernel, depth, n_tiles, n_exp),
        grid_spec=pltpu.PrefetchScalarGridSpec(
            num_scalar_prefetch=2,
            grid=(2 * depth + n_exp,),
            in_specs=[
                pl.BlockSpec((1, 2 * n_exp, toks), plan_at),
                pl.BlockSpec((toks, dim), lambda i, *_: (first(i), 0)), wide, wide, tall,
            ],
            out_specs=[any_space] * (depth + 2),
            scratch_shapes=[
                pltpu.VMEM((rows, dim), BF16), pltpu.VMEM((n_exp * WIN, dim), BF16),
                pltpu.VMEM((2, ROWS, dim), BF16), pltpu.VMEM((2, 2, ROWS, ff), F32), pltpu.VMEM((2, toks, dim), F32),
                pltpu.SMEM(((n_tiles + 1) * n_exp,), jnp.int32), pltpu.SMEM((n_exp,), jnp.int32),
                pltpu.SMEM((n_exp + 1,), jnp.int32), dma((2,)), dma((2,)), dma((2,)),
            ],
        ),
        out_shape=[shape((toks, dim), F32)] * depth + [shape((blocks, ROWS, dim), BF16), shape((blocks, 2, ROWS, ff), F32)],
        compiler_params=pltpu.CompilerParams(dimension_semantics=("arbitrary",), vmem_limit_bytes=64_000_000),
        cost_estimate=pl.CostEstimate(flops=25_000_000_000, bytes_accessed=80_000_000, transcendentals=3_000_000),
        name="forward",
    )(counts, place, plan_col, x_col.reshape(-1, dim), w_gate, w_up, w_down)
    return result[:depth], result[depth], result[depth + 1]


def expert_backward(depth, counts, place, plan_col, dy_head, dy_tails, w_gate, w_up, w_down, x_saved, uv_saved, cap):
    n_tiles, n_exp, rows, blocks = layer_sizes(depth, plan_col.shape[2], w_gate, cap)
    head, dim = dy_head.shape[1:]
    tail = dy_tails[0].shape[0]
    toks = head + tail
    ff = w_gate.shape[2]
    first = lambda i: jnp.minimum(i, depth - 1)
    middle = lambda i: jnp.clip(i - depth, 0, n_exp - 1)
    last = lambda i: jnp.maximum(i - depth - n_exp, 0)

    plan_at = lambda i, counts, place: (jnp.where(i < depth, i, last(i)), place[0], 0)

    wide = pl.BlockSpec((1, dim, ff), lambda i, *_: (middle(i), 0, 0))
    tall = pl.BlockSpec((1, ff, dim), lambda i, *_: (middle(i), 0, 0))
    any_space = pl.BlockSpec(memory_space=pl.ANY)
    shape = jax.ShapeDtypeStruct
    dma = pltpu.SemaphoreType.DMA
    return pl.pallas_call(
        functools.partial(backward_kernel, depth, n_tiles, n_exp),
        grid_spec=pltpu.PrefetchScalarGridSpec(
            num_scalar_prefetch=2,
            grid=(2 * depth + n_exp,),
            in_specs=[
                pl.BlockSpec((1, 2 * n_exp, toks), plan_at),
                pl.BlockSpec((head, dim), lambda i, *_: (first(i), 0)),
                *[pl.BlockSpec((tail, dim), lambda i, *_: (0, 0))] * depth, wide, wide, tall, any_space, any_space,
            ],
            out_specs=[
                pl.BlockSpec((toks, dim), lambda i, *_: (last(i), 0)),
                pl.BlockSpec((1, 3 * dim, ff), lambda i, *_: (middle(i), 0, 0)),
            ],
            scratch_shapes=[
                pltpu.VMEM((rows, dim), BF16), pltpu.VMEM((n_exp * WIN, dim), BF16),
                pltpu.VMEM((2, ROWS, dim), BF16), pltpu.VMEM((2, 2, ROWS, ff), F32), pltpu.VMEM((tail, dim), BF16),
                pltpu.SMEM(((n_tiles + 1) * n_exp,), jnp.int32), pltpu.SMEM((n_exp,), jnp.int32),
                pltpu.SMEM((n_exp + 1,), jnp.int32), dma((2,)), dma((2,)),
            ],
        ),
        out_shape=[shape((depth * toks, dim), F32), shape((n_exp, 3 * dim, ff), F32)],
        compiler_params=pltpu.CompilerParams(dimension_semantics=("arbitrary",), vmem_limit_bytes=66_000_000),
        cost_estimate=pl.CostEstimate(flops=50_000_000_000, bytes_accessed=150_000_000, transcendentals=3_000_000),
        name="backward",
    )(counts, place, plan_col, dy_head.reshape(-1, dim), *dy_tails, w_gate, w_up, w_down, x_saved, uv_saved)


def solution(mesh):
    n_dev = mesh.devices.size
    depth = n_dev // 8
    grid = Mesh(mesh.devices.reshape(depth, 2, 2, 2), ('z', 'y', 'x', 'c'))
    plane = ('y', 'x', 'c')
    spec = P(('z', 'y', 'x', 'c'))

    def local_step(x_tok, route_idx, gates, dy_tok, w_gate, w_up, w_down):
        tok_loc, top_k = route_idx.shape
        cap = depth * (2 * tok_loc * top_k // (n_dev * w_gate.shape[0] - 2))
        n_exp = 8 * w_gate.shape[0]
        head = tok_loc // 2
        x_col, dy_head, dy_tail, plan_col, wg_all, wu_all, wd_all = spread(
            depth, n_dev, head, x_tok, dy_tok, route_idx.T, gates.T, w_gate, w_up, w_down
        )
        turn = lambda a, d: lax.ppermute(a, 'z', [(i, (i + d) % depth) for i in range(depth)])
        dy_tails = [dy_tail] + [turn(dy_tail, d) for d in range(1, depth)]
        place = lax.axis_index('z')
        per = tok_loc // TILE
        counts = lax.dynamic_slice(plan_col[:, 2 * n_dev : 2 * n_dev + per, :n_dev], (0, 0, place * n_exp), (depth, per, n_exp))
        where = (counts.reshape(-1).astype(jnp.int32), place.reshape(1), plan_col)
        y_parts, x_saved, uv_saved = expert_forward(depth, *where, x_col, wg_all, wu_all, wd_all, cap)
        y_sum = y_parts[0]
        turned = [turn(y_parts[d], d) for d in range(1, depth)]
        dx_part, grads = expert_backward(
            depth, *where, dy_head, dy_tails, wg_all, wu_all, wd_all, x_saved, uv_saved, cap
        )
        dx, *dw = collect(depth, dx_part.reshape(depth, tok_loc, -1), grads)
        y_sum, turned, dx, dw = lax.optimization_barrier((y_sum, turned, dx, dw))
        y = functools.reduce(jnp.add, turned, y_sum).astype(BF16)
        return y, dx, *[a[None] for a in dw]

    return jax.shard_map(local_step, mesh=grid, in_specs=(spec,) * 7, out_specs=(spec,) * 5, check_vma=False)
```

```python
import functools

import jax
import jax.numpy as jnp
from jax import lax
from jax.experimental import pallas as pl
from jax.experimental.pallas import tpu as pltpu
from jax.sharding import Mesh, PartitionSpec as P

F32 = jnp.float32
BF16 = jnp.bfloat16
TILE = 256
HEAD = 8
WIN = 128
ALIGN = 16
ROWS = 512


def dot(a, b, dims=((1,), (0,))):
    return lax.dot_general(a, b, (dims, ((), ())), preferred_element_type=F32)


MESH = pl.DeviceIdType.MESH


def hop(src, dst, send_sem, recv_sem, **where):
    return pltpu.make_async_remote_copy(
        src_ref=src, dst_ref=dst, send_sem=send_sem, recv_sem=recv_sem, device_id=where, device_id_type=MESH
    )


def meet(depth, z, y, x, c):
    barrier = pltpu.get_barrier_semaphore()
    for where in ({'y': 1 - y}, {'x': 1 - x}, {'c': 1 - c}):
        pl.semaphore_signal(barrier, inc=1, device_id=where, device_id_type=MESH)

    @pl.when(z > 0)
    def _():
        pl.semaphore_signal(barrier, inc=1, device_id={'z': z - 1}, device_id_type=MESH)

    @pl.when(z < depth - 1)
    def _():
        pl.semaphore_signal(barrier, inc=1, device_id={'z': z + 1}, device_id_type=MESH)

    inner = (z > 0) & (z < depth - 1)

    @pl.when(inner)
    def _():
        pl.semaphore_wait(barrier, 5)

    @pl.when(jnp.logical_not(inner))
    def _():
        pl.semaphore_wait(barrier, 4)


def make_plan(experts, route_ref, gate_ref, plan):
    top_k, toks = route_ref.shape
    route = route_ref[...]
    gates = gate_ref[...].astype(F32)
    below = lax.broadcasted_iota(jnp.int32, (TILE, TILE), 0) < lax.broadcasted_iota(jnp.int32, (TILE, TILE), 1)
    below = jnp.where(below, 1.0, 0.0).astype(BF16)
    ones = jnp.ones((16, TILE), BF16)
    ids = lax.broadcasted_iota(jnp.int32, (experts, toks), 0)
    member = jnp.zeros((experts, toks), F32)
    gate = jnp.zeros((experts, toks), F32)
    for k in range(top_k):
        hit = jnp.broadcast_to(route[k : k + 1, :], (experts, toks)) == ids
        member = jnp.where(hit, 1.0, member)
        gate = jnp.where(hit, jnp.broadcast_to(gates[k : k + 1, :], (experts, toks)), gate)
    ranks, counts = [], []
    for t in range(toks // TILE):
        part = member[:, t * TILE : (t + 1) * TILE]
        ranks.append(jnp.where(part > 0.5, dot(part.astype(BF16), below), -4096.0))
        counts.append(dot(ones, part.astype(BF16), ((1,), (1,))))
    rank = jnp.concatenate(ranks, axis=1)
    for p in range(experts // 8):
        both = jnp.concatenate([rank[8 * p : 8 * p + 8], gate[8 * p : 8 * p + 8]], axis=0)
        plan[16 * p : 16 * p + 16, :] = both.astype(BF16)
    which = lax.broadcasted_iota(jnp.int32, (16, experts), 0)
    count = functools.reduce(jnp.add, [jnp.where(which == t, c, 0.0) for t, c in enumerate(counts)])
    plan[2 * experts :, :] = jnp.zeros((16, toks), BF16)
    plan[2 * experts :, :experts] = count.astype(BF16)


def spread_kernel(
    depth, experts, x_ref, dy_ref, route_ref, gate_ref, wg_ref, wu_ref, wd_ref,
    x_out, dy_out, tail_out, plan_out, wg_out, wu_out, wd_out,
    stage_t, stage_w, stage_d, plan, own_sem, z_send, z_recv, p_send, p_recv, c_send, c_recv,
):
    z, y, x, c = (lax.axis_index(a) for a in 'zyxc')
    slot = lambda yy, xx: yy * 4 + xx * 2 + c
    own, by_x, by_y, far = slot(y, x), slot(y, 1 - x), slot(1 - y, x), slot(1 - y, 1 - x)
    weights = ((wg_ref, wg_out), (wu_ref, wu_out), (wd_ref, wd_out))
    dy_head = dy_ref.at[pl.ds(0, dy_out.shape[1]), :]
    arrays = ((x_ref, x_out), (plan, plan_out), (dy_head, dy_out))
    sent = []

    def half(ref, where, h):
        rows = ref.shape[1] // 2
        return ref.at[where, pl.ds(h * rows, rows), :]

    def own_half(part, h, side):
        src, out = weights[part]
        where = {'x': 1 - x} if side == 0 else {'y': 1 - y}
        return hop(half(src, 0, h), half(out, own, h), p_send.at[side, part, h], p_recv.at[side, part, h], **where)

    def onward(part, h):
        at = half(weights[part][1], by_x if h == 0 else by_y, h)
        where = {'y': 1 - y} if h == 0 else {'x': 1 - x}
        return hop(at, at, p_send.at[2, part, h], p_recv.at[2, part, h], **where)

    def landed(part, h, kind):
        at = half(weights[part][1], (by_x, by_y, far)[kind], h)
        hop(at, at, p_send.at[kind, part, h], p_recv.at[kind, part, h], c=1 - c).wait_recv()

    def across(part, h, kind):
        at = half(weights[part][1], (by_x, by_y, far)[kind], h)
        return hop(at, at, c_send.at[kind, part, h], c_recv.at[kind, part, h], c=1 - c)

    def across_own(part, h):
        src, out = weights[part]
        return hop(half(src, 0, h), half(out, own, h), c_send.at[3, part, h], c_recv.at[3, part, h], c=1 - c)

    def crossed(part, h, kind):
        twin = lambda yy, xx: yy * 4 + xx * 2 + 1 - c
        where = (twin(y, 1 - x), twin(1 - y, x), twin(1 - y, 1 - x), twin(y, x))[kind]
        at = half(weights[part][1], where, h)
        hop(at, at, c_send.at[kind, part, h], c_recv.at[kind, part, h], c=1 - c).wait_recv()

    def go(copy):
        copy.start()
        sent.append((None, copy))

    def along(k, dist, up):
        src, out = arrays[k]
        at = out.at[z - dist if up else z + dist]
        side = 0 if up else 1
        return hop(src if dist == 0 else at, at, z_send.at[side, k, dist], z_recv.at[side, k, dist], z=z + 1 if up else z - 1)

    def start_along(k, dist):
        for up in (True, False):
            cond = (z >= dist) & (z < depth - 1) if up else (z + dist < depth) & (z > 0)

            @pl.when(cond)
            def _(up=up):
                along(k, dist, up).start()

            sent.append((cond, along(k, dist, up)))

    def await_along(k, dist):
        for up in (True, False):
            @pl.when(z > dist if up else z + dist + 1 < depth)
            def _(up=up):
                at = arrays[k][1].at[z - dist - 1 if up else z + dist + 1]
                side = 0 if up else 1
                hop(at, at, z_send.at[side, k, dist], z_recv.at[side, k, dist], c=1 - c).wait_recv()

        if dist + 1 < depth - 1:
            start_along(k, dist + 1)

    copies = []
    for i, (src, buf, out) in enumerate((
        (x_ref, stage_t.at[0], x_out.at[z]), (dy_head, stage_t.at[1, pl.ds(0, dy_out.shape[1]), :], dy_out.at[z]),
        (dy_ref.at[pl.ds(dy_out.shape[1], tail_out.shape[0]), :], stage_t.at[1, pl.ds(dy_out.shape[1], tail_out.shape[0]), :], tail_out),
        (wg_ref.at[0], stage_w.at[0], wg_out.at[own]), (wu_ref.at[0], stage_w.at[1], wu_out.at[own]),
        (wd_ref.at[0], stage_d, wd_out.at[own]),
    )):
        copies.append((pltpu.make_async_copy(src, buf, own_sem.at[i]), pltpu.make_async_copy(buf, out, own_sem.at[i])))
        copies[-1][0].start()

    meet(depth, z, y, x, c)
    start_along(0, 0)
    for part in range(3):
        go(own_half(part, 0, 0))
        go(own_half(part, 1, 1))
    for part in range(3):
        go(own_half(part, 1, 0))
        go(own_half(part, 0, 1))
    for part in range(3):
        for h in range(2):
            go(across_own(part, h))
    make_plan(experts, route_ref, gate_ref, plan)
    start_along(1, 0)
    start_along(2, 0)
    copies.append((None, pltpu.make_async_copy(plan, plan_out.at[z], own_sem.at[6])))
    for i, (load, store) in enumerate(copies):
        if load is not None:
            load.wait()
        store.start()

    def relay(part, h):
        landed(part, h, h)
        go(onward(part, h))
        go(across(part, h, h))

    def relay_twin(part, h):
        landed(part, h, 1 - h)
        go(across(part, h, 1 - h))

    def relay_far(part):
        for h in range(2):
            landed(part, h, 2)
            go(across(part, h, 2))

    for part in range(2):
        relay(part, 0)
        relay(part, 1)
    await_along(0, 0)
    await_along(1, 0)
    relay(2, 0)
    relay(2, 1)
    await_along(2, 0)
    for part in range(2):
        relay_twin(part, 1)
        relay_twin(part, 0)
    await_along(0, 1)
    await_along(1, 1)
    relay_twin(2, 1)
    relay_twin(2, 0)
    await_along(2, 1)
    relay_far(0)
    relay_far(1)
    await_along(0, 2)
    await_along(1, 2)
    relay_far(2)
    await_along(2, 2)
    for part in range(3):
        for h in range(2):
            for kind in range(4):
                crossed(part, h, kind)
    for cond, copy in sent:
        if cond is None:
            copy.wait_send()
        else:
            @pl.when(cond)
            def _(copy=copy):
                copy.wait_send()
    for _, store in copies:
        store.wait()


def spread(depth, experts, head, x_tok, dy_tok, route, gate, w_gate, w_up, w_down):
    toks, dim = x_tok.shape
    ff = w_down.shape[1]
    any_space = pl.BlockSpec(memory_space=pl.ANY)
    vmem = pl.BlockSpec(memory_space=pltpu.VMEM)
    rows = 2 * experts + 16
    shape = jax.ShapeDtypeStruct
    dma = pltpu.SemaphoreType.DMA
    return pl.pallas_call(
        functools.partial(spread_kernel, depth, experts),
        in_specs=[any_space, any_space, vmem, vmem, any_space, any_space, any_space],
        out_specs=[any_space] * 7,
        out_shape=[
            shape((depth, toks, dim), BF16), shape((depth, head, dim), BF16), shape((toks - head, dim), BF16), shape((depth, rows, toks), BF16),
            shape((8, dim, ff), BF16), shape((8, dim, ff), BF16), shape((8, ff, dim), BF16),
        ],
        scratch_shapes=[
            pltpu.VMEM((2, toks, dim), BF16), pltpu.VMEM((2, dim, ff), BF16), pltpu.VMEM((ff, dim), BF16),
            pltpu.VMEM((rows, toks), BF16), dma((7,)), dma((2, 3, depth)), dma((2, 3, depth)),
            dma((3, 3, 2)), dma((3, 3, 2)), dma((4, 3, 2)), dma((4, 3, 2)),
        ],
        compiler_params=pltpu.CompilerParams(collective_id=0, has_side_effects=True),
        name="spread",
    )(x_tok, dy_tok, route, gate, w_gate, w_up, w_down)


CHUNK = 128
BAND = 64
TURNS = (4, 14, 20, 22)
FINISH = 3
RING = 6


def collect_kernel(
    depth, dx_ref, g_ref, dx_out, gate_out, up_out, down_out, twin,
    z_land, x_land, y_land, x_last, y_last, total, x_buf, y_buf, f_buf, z_buf,
    t_sem, x_load, y_load, f_load, z_load, z_send, z_recv, x_send, x_recv, y_send, y_recv, c_send, c_recv,
):
    z, y, x, c = (lax.axis_index(a) for a in 'zyxc')
    cell = lambda yy, xx: yy * 2 + xx
    mine, by_x, by_y, far = cell(y, x), cell(y, 1 - x), cell(1 - y, x), cell(1 - y, 1 - x)
    bands = dx_ref.shape[1] // BAND
    n_part = g_ref.shape[1] // CHUNK // 2
    n_col = (depth - 1) * bands
    n_link = 3 * n_part
    piece = 4 * CHUNK
    order = (far, by_x, by_y, mine)
    rows = lambda i: pl.ds(pl.multiple_of(i * CHUNK, CHUNK), CHUNK)

    def swap(kind, q):
        at = pl.ds(q * piece, piece)
        return hop(g_ref.at[2 * order[kind] + 1 - c, at, :], twin.at[order[kind], at, :], c_send.at[kind, q], c_recv.at[kind, q], c=1 - c)

    half = n_part // 4
    swaps = [(0, q + h * half) for q in range(half) for h in range(2)]
    swaps += [(1 + h, q + h * half) for q in range(half) for h in range(2)]
    swaps += [(2 - h, q + h * half) for q in range(half) for h in range(2)]
    swaps += [(3, q + h * half) for q in range(half) for h in range(2)]

    own_total = pltpu.make_async_copy(dx_ref.at[z], total, t_sem)
    own_total.start()
    meet(depth, z, y, x, c)
    for kind, q in swaps:
        swap(kind, q).start()

    def link_item(side, i):
        leg = i // n_part
        j = i % n_part
        near, other = (by_x, by_y) if side == 0 else (by_y, by_x)
        kind_near, kind_other = (1, 2) if side == 0 else (2, 1)
        first = jnp.where(leg < 2, side, 1 - side)
        chunk = first * n_part + j
        expert = jnp.where(leg == 0, far, near)
        kind = jnp.where(leg == 0, 0, kind_near)
        return leg, j, chunk, expert, kind

    def fetch(chunk, expert, kind, fresh, buf, sems):
        @pl.when(fresh)
        def _():
            for k in range(4):
                @pl.when(kind == k)
                def _(k=k):
                    at = pl.ds(pl.multiple_of(chunk // 4 * piece, piece), piece)
                    q = chunk // 4
                    hop(twin.at[order[k], at, :], twin.at[order[k], at, :], c_send.at[k, q], c_recv.at[k, q], c=1 - c).wait_recv()

        pltpu.make_async_copy(g_ref.at[2 * expert + c, rows(chunk), :], buf.at[0], sems.at[0]).start()
        pltpu.make_async_copy(twin.at[expert, rows(chunk), :], buf.at[1], sems.at[1]).start()

    def fetched(buf, sems):
        pltpu.make_async_copy(g_ref.at[0, rows(0), :], buf.at[0], sems.at[0]).wait()
        pltpu.make_async_copy(twin.at[0, rows(0), :], buf.at[1], sems.at[1]).wait()

    links = (
        (x_buf, x_load, x_send, x_recv, x_land, x_last, {'x': 1 - x}),
        (y_buf, y_load, y_send, y_recv, y_land, y_last, {'y': 1 - y}),
    )

    def landing(side, i):
        land, last = links[side][4], links[side][5]
        return land, last

    def link_send(side, i, wait_only=False):
        buf, _, send, recv, land, last, where = links[side]
        src = buf.at[i % RING, 0]

        @pl.when(i < 2 * n_part)
        def _():
            copy = hop(src, land.at[jnp.minimum(i, 2 * n_part - 1)], send.at[i], recv.at[i], **where)
            copy.wait_send() if wait_only else copy.start()

        @pl.when(i >= 2 * n_part)
        def _():
            copy = hop(src, last.at[jnp.maximum(i - 2 * n_part, 0)], send.at[i], recv.at[i], **where)
            copy.wait_send() if wait_only else copy.start()

    def landed(side, ref, i):
        recv, send = links[side][3], links[side][2]
        hop(ref, ref, send.at[i], recv.at[i], c=1 - c).wait_recv()

    def link_prepare(side, i):
        buf, load = links[side][0], links[side][1]

        @pl.when((i >= RING) & (i < n_link))
        def _():
            link_send(side, i - RING, wait_only=True)

        @pl.when(i < n_link)
        def _():
            leg, j, chunk, expert, kind = link_item(side, i)
            fetch(chunk, expert, kind, j % 4 == 0, buf.at[i % RING], load.at[i % RING])

    def link_turn(side, i):
        buf, load = links[side][0], links[side][1]
        other_land = links[1 - side][4]

        @pl.when(i < n_link)
        def _():
            b = i % RING
            fetched(buf.at[b], load.at[b])
            buf[b, 0] += buf[b, 1]

            @pl.when(i >= 2 * n_part)
            def _():
                j = i - 2 * n_part
                landed(1 - side, other_land.at[j], j)
                buf[b, 0] += other_land[j]

            link_send(side, i)

    def last_prepare(h, j):
        @pl.when((j >= 0) & (j < n_part))
        def _():
            fetch(h * n_part + j, mine, 3, j % 4 == 0, f_buf.at[h, j % 2], f_load.at[h, j % 2])

    def last_turn(h, j):
        @pl.when((j >= 0) & (j < n_part))
        def _():
            land, last = links[h][4], links[1 - h][5]
            fetched(f_buf.at[h, j % 2], f_load.at[h, j % 2])
            landed(h, land.at[n_part + j], n_part + j)
            landed(1 - h, last.at[j], 2 * n_part + j)
            value = f_buf[h, j % 2, 0] + f_buf[h, j % 2, 1] + (land[n_part + j] + last[j])
            chunk = h * n_part + j
            tall = gate_out.shape[0] // CHUNK
            places = ((0, tall, gate_out, 0), (tall, 2 * tall, up_out, 0), (2 * tall, 5 * tall // 2, down_out, 0), (5 * tall // 2, 3 * tall, down_out, 1))
            for first, end, out, side in places:
                if first < (h + 1) * n_part and end > h * n_part:
                    @pl.when((chunk >= first) & (chunk < end))
                    def _(first=first, out=out, side=side):
                        cols = pl.ds(side * value.shape[1], value.shape[1])
                        out[rows(chunk - first), cols] = value

    def column(side, k):
        role = z if side == 0 else depth - 1 - z
        goal = depth - 1 - k // bands
        block = goal if side == 0 else depth - 1 - goal
        slot = block + 1 if side == 0 else block
        at = pl.ds(pl.multiple_of(k % bands * BAND, BAND), BAND)
        return role, goal, block, slot, at

    def column_copy(side, k, src):
        _, _, _, slot, at = column(side, k)
        return hop(src, z_land.at[slot, at, :], z_send.at[side, k], z_recv.at[side, k], z=z + 1 if side == 0 else z - 1)

    def turn_of(side, t):
        role = z if side == 0 else depth - 1 - z
        return t - functools.reduce(lambda late, r: jnp.where(role == r, TURNS[r], late), range(1, depth), TURNS[0])

    def column_prepare(side, t):
        k = turn_of(side, t)
        kk = jnp.clip(k, 0, n_col - 1)
        role, goal, block, slot, at = column(side, kk)

        @pl.when((k >= 0) & (k < n_col) & (role > 0) & (goal > role))
        def _():
            pltpu.make_async_copy(dx_ref.at[block, at, :], z_buf.at[side, kk % 2], z_load.at[side, kk % 2]).start()

    def column_turn(side, t):
        k = turn_of(side, t)
        kk = jnp.clip(k, 0, n_col - 1)
        role, goal, block, slot, at = column(side, kk)
        live = (k >= 0) & (k < n_col) & (goal >= role)

        @pl.when(live & (role == 0))
        def _():
            column_copy(side, kk, dx_ref.at[block, at, :]).start()

        @pl.when(live & (role > 0))
        def _():
            here = z_land.at[slot, at, :]
            hop(here, here, z_send.at[side, kk], z_recv.at[side, kk], c=1 - c).wait_recv()

            @pl.when(goal > role)
            def _():
                pltpu.make_async_copy(dx_ref.at[block, at, :], z_buf.at[side, kk % 2], z_load.at[side, kk % 2]).wait()
                z_land[slot, at, :] += z_buf[side, kk % 2]
                column_copy(side, kk, here).start()

            @pl.when(goal == role)
            def _():
                total[at, :] += z_land[slot, at, :]

    def prepare(t):
        for side in range(2):
            link_prepare(side, t)
            column_prepare(side, t)
            last_prepare(side, t - 2 * n_part - FINISH)

    prepare(jnp.int32(0))
    own_total.wait()
    steps = max(max(TURNS) + n_col, n_link + FINISH)

    @pl.loop(0, steps)
    def _(t):
        prepare(t + 1)
        for side in range(2):
            link_turn(side, t)
        for side in range(2):
            column_turn(side, t)
        for side in range(2):
            last_turn(side, t - 2 * n_part - FINISH)

    dx_out[...] = total[...].astype(BF16)

    @pl.loop(n_link - RING, n_link)
    def _(i):
        for side in range(2):
            link_send(side, i, wait_only=True)

    @pl.loop(0, n_col)
    def _(k):
        for side in range(2):
            role, goal, block, slot, at = column(side, k)

            @pl.when(goal > role)
            def _():
                column_copy(side, k, z_land.at[slot, at, :]).wait_send()

    for kind, q in swaps:
        swap(kind, q).wait_send()


def collect(depth, dx_part, grads):
    toks, dim = dx_part.shape[1:]
    height, ff = grads.shape[1:]
    n_part = height // CHUNK // 2
    n_col = (depth - 1) * (toks // BAND)
    any_space = pl.BlockSpec(memory_space=pl.ANY)
    vmem = pl.BlockSpec(memory_space=pltpu.VMEM)
    shape = jax.ShapeDtypeStruct
    dma = pltpu.SemaphoreType.DMA
    message = (CHUNK, ff)
    return pl.pallas_call(
        functools.partial(collect_kernel, depth),
        in_specs=[any_space, any_space],
        out_specs=[vmem, vmem, vmem, vmem, any_space],
        out_shape=[pltpu.VMEM((toks, dim), BF16), pltpu.VMEM((dim, ff), F32), pltpu.VMEM((dim, ff), F32), pltpu.VMEM((ff, dim), F32), shape((4, height, ff), F32)],
        scratch_shapes=[
            pltpu.VMEM((depth + 1, toks, dim), F32),
            pltpu.VMEM((2 * n_part, *message), F32), pltpu.VMEM((2 * n_part, *message), F32),
            pltpu.VMEM((n_part, *message), F32), pltpu.VMEM((n_part, *message), F32),
            pltpu.VMEM((toks, dim), F32),
            pltpu.VMEM((RING, 2, *message), F32), pltpu.VMEM((RING, 2, *message), F32),
            pltpu.VMEM((2, 2, 2, *message), F32), pltpu.VMEM((2, 2, BAND, dim), F32),
            dma, dma((RING, 2)), dma((RING, 2)), dma((2, 2, 2)), dma((2, 2)),
            dma((2, n_col)), dma((2, n_col)), dma((3 * n_part,)), dma((3 * n_part,)), dma((3 * n_part,)), dma((3 * n_part,)),
            dma((4, height // CHUNK // 4)), dma((4, height // CHUNK // 4)),
        ],
        compiler_params=pltpu.CompilerParams(collective_id=1, has_side_effects=True, vmem_limit_bytes=46_000_000),
        name="collect",
    )(dx_part, grads)[:4]


def count_up(n_tiles, n_exp, count_ref, cum_ref, off_ref, blk_ref):
    base = jnp.int32(0)
    block = jnp.int32(0)
    for exp in range(n_exp):
        run = jnp.int32(0)
        cum_ref[exp] = run
        for tile in range(n_tiles):
            run += count_ref[tile * n_exp + exp]
            cum_ref[(tile + 1) * n_exp + exp] = run
        off_ref[exp] = base
        blk_ref[exp] = block
        big, rest = blocks_of(run)
        block += big
        base += jnp.maximum(big * ROWS + rest, (run + ALIGN - 1) // ALIGN * ALIGN + WIN)
    blk_ref[n_exp] = block


def blocks_of(count):
    over = count % ROWS
    big = count // ROWS + jnp.where(over > ROWS // 2, 1, 0)
    rest = jnp.where(over > ROWS // 4, ROWS // 2, jnp.where(over > 0, ROWS // 4, 0))
    return big, jnp.where(over > ROWS // 2, 0, rest)


def span(n_exp, cum_ref, tile, exp):
    lo = cum_ref[tile * n_exp + exp]
    hi = cum_ref[(tile + 1) * n_exp + exp]
    return lo, hi, (lo // ALIGN) * ALIGN


def gather_tile(n_exp, cum_ref, off_ref, plan, gated, tile, cols, toks, rows_ref):
    rank, gate = plan[:n_exp, cols], plan[n_exp:, cols]
    row = lax.broadcasted_iota(jnp.int32, (WIN, TILE), 0).astype(F32)

    def window(exp, lo, start):
        hit = rank[exp : exp + 1] == row + (start - lo).astype(F32)
        take = jnp.where(hit, gate[exp : exp + 1] if gated else 1.0, 0.0).astype(BF16)
        return dot(take, toks[...]).astype(BF16)

    def rows_at(exp, start, size):
        return pl.ds(pl.multiple_of(off_ref[exp] + start, ALIGN), size)

    spans = [span(n_exp, cum_ref, tile, exp) for exp in range(n_exp)]
    for exp, (lo, hi, start) in enumerate(spans):
        value = window(exp, lo, start)
        head = rows_at(exp, start, ALIGN)
        fresh = lax.broadcasted_iota(jnp.int32, (ALIGN, 1), 0) + start >= lo
        rows_ref[head, :] = jnp.where(fresh, value[:ALIGN], rows_ref[head, :])
        rows_ref[rows_at(exp, start + ALIGN, WIN - ALIGN), :] = value[ALIGN:]
    most = functools.reduce(jnp.maximum, [hi - start for lo, hi, start in spans])

    @pl.when(most > WIN)
    def _more():
        for exp, (lo, hi, start) in enumerate(spans):
            @pl.loop(1, (hi - start + WIN - 1) // WIN)
            def _(w):
                rows_ref[rows_at(exp, start + w * WIN, WIN), :] = window(exp, lo, start + w * WIN)


def scatter_tile(n_exp, cum_ref, off_ref, plan_t, gated, tile, cols, rows_ref, win_ref, out_ref):
    column = lax.broadcasted_iota(jnp.int32, (TILE, WIN), 1).astype(F32)

    def window(exp, lo, start):
        hit = plan_t[cols, exp : exp + 1] == column + (start - lo).astype(F32)
        put = jnp.where(hit, plan_t[cols, n_exp + exp : n_exp + exp + 1] if gated else 1.0, 0.0).astype(BF16)
        return put, rows_ref[pl.ds(pl.multiple_of(off_ref[exp] + start, ALIGN), WIN), :]

    spans = [span(n_exp, cum_ref, tile, exp) for exp in range(n_exp)]
    puts = []
    for exp, (lo, hi, start) in enumerate(spans):
        put, block = window(exp, lo, start)
        puts.append(put)
        win_ref[exp * WIN : (exp + 1) * WIN, :] = block
    out_ref[cols, :] = dot(jnp.concatenate(puts, axis=1), win_ref[...])
    most = functools.reduce(jnp.maximum, [hi - start for lo, hi, start in spans])

    @pl.when(most > WIN)
    def _more():
        for exp, (lo, hi, start) in enumerate(spans):
            @pl.loop(1, (hi - start + WIN - 1) // WIN)
            def _(w):
                put, block = window(exp, lo, start + w * WIN)
                out_ref[cols, :] += dot(put, block)


def forward_kernel(
    depth, n_tiles, n_exp, count_ref, z_ref, plan_ref, x_ref, wg_ref, wu_ref, wd_ref,
    *refs,
):
    y_refs, refs = refs[:depth], refs[depth:]
    xs_ref, uv_ref, xt_ref, uvt_ref, rows_ref, win_ref, x_out, uv_out, xt_out, uvt_out, y_buf = refs[:11]
    cum_ref, off_ref, blk_ref, tail_ref, x_sem, uv_sem, t_sem, y_sem = refs[11:]
    step = pl.program_id(0)
    per = n_tiles // depth

    @pl.when(step == 0)
    def _():
        count_up(n_tiles, n_exp, count_ref, cum_ref, off_ref, blk_ref)
        tail_ref[0] = 0

    @pl.when(step < depth)
    def _():
        plan = plan_ref[0].astype(F32)
        for i in range(per):
            cols = slice(i * TILE, (i + 1) * TILE)
            gather_tile(n_exp, cum_ref, off_ref, plan, False, step * per + i, cols, x_ref.at[cols, :], rows_ref)

    def saves(block):
        side = block % 2
        return (
            pltpu.make_async_copy(x_out.at[side], xs_ref.at[block], x_sem.at[side]),
            pltpu.make_async_copy(uv_out.at[side], uv_ref.at[block], uv_sem.at[side]),
        )

    def tail_saves(exp, size):
        at = slice(0, size)
        return (
            pltpu.make_async_copy(xt_out.at[at], xt_ref.at[exp, at], t_sem.at[0]),
            pltpu.make_async_copy(uvt_out.at[:, at], uvt_ref.at[exp, :, at], t_sem.at[1]),
        )

    def tail_saved():
        for size in (ROWS // 2, ROWS // 4):
            @pl.when(tail_ref[0] == size)
            def _(size=size):
                for copy in tail_saves(0, size):
                    copy.wait()

    @pl.when((step >= depth) & (step < depth + n_exp))
    def _():
        exp = step - depth
        count = cum_ref[n_tiles * n_exp + exp]
        big, rest = blocks_of(count)

        def run(start, x_blk, uv_blk):
            size = x_blk.shape[0]
            here = pl.ds(pl.multiple_of(off_ref[exp] + start, ALIGN), size)
            live = lax.broadcasted_iota(jnp.int32, (size, 1), 0) < count - start
            x_old = rows_ref[here, :]
            x_blk[...] = jnp.where(live, x_old, jnp.zeros_like(x_old))
            u = dot(x_blk[...], wg_ref[0])
            v = dot(x_blk[...], wu_ref[0])
            uv_blk[0] = u
            uv_blk[1] = v
            act = (u * jax.nn.sigmoid(u) * v).astype(BF16)
            rows_ref[here, :] = dot(act, wd_ref[0]).astype(BF16)

        @pl.loop(0, big)
        def _(b):
            block = blk_ref[exp] + b

            @pl.when(block >= 2)
            def _():
                for copy in saves(block - 2):
                    copy.wait()

            run(b * ROWS, x_out.at[block % 2], uv_out.at[block % 2])
            for copy in saves(block):
                copy.start()

        for size in (ROWS // 2, ROWS // 4):
            @pl.when(rest == size)
            def _(size=size):
                tail_saved()
                run(big * ROWS, xt_out.at[slice(0, size)], uvt_out.at[:, slice(0, size)])
                for copy in tail_saves(exp, size):
                    copy.start()
                tail_ref[0] = size

    @pl.when(step == depth + n_exp)
    def _():
        total = blk_ref[n_exp]
        for back in (2, 1):
            @pl.when(total >= back)
            def _():
                for copy in saves(total - back):
                    copy.wait()

        tail_saved()

    d = step - depth - n_exp

    def y_copy(d, k):
        return pltpu.make_async_copy(y_buf.at[k % 2], y_refs[k], y_sem.at[k % 2])

    @pl.when(d >= 0)
    def _():
        for k in range(2, depth):
            @pl.when(d == k)
            def _(k=k):
                y_copy(d, k - 2).wait()

        plan_t = jnp.transpose(plan_ref[0].astype(F32))
        for i in range(per):
            tile = (z_ref[0] ^ d) * per + i
            cols = slice(i * TILE, (i + 1) * TILE)
            scatter_tile(n_exp, cum_ref, off_ref, plan_t, True, tile, cols, rows_ref, win_ref, y_buf.at[d % 2])
        for k in range(depth):
            @pl.when(d == k)
            def _(k=k):
                y_copy(d, k).start()

    @pl.when(d == depth - 1)
    def _():
        y_copy(d, depth - 2).wait()
        y_copy(d, depth - 1).wait()


def backward_kernel(
    depth, n_tiles, n_exp, count_ref, z_ref, plan_ref, head_ref, *refs,
):
    tails, refs = refs[:depth], refs[depth:]
    wg_ref, wu_ref, wd_ref, xs_ref, uv_ref, xt_ref, uvt_ref, dx_ref, dw_ref = refs[:9]
    rows_ref, win_ref, x_in, uv_in, xt_in, uvt_in, tok_ref, cum_ref, off_ref, blk_ref, x_sem, uv_sem, t_sem = refs[9:]
    step = pl.program_id(0)
    per = n_tiles // depth

    @pl.when(step == 0)
    def _():
        count_up(n_tiles, n_exp, count_ref, cum_ref, off_ref, blk_ref)

    @pl.when(step < depth)
    def _():
        split = head_ref.shape[0]
        tok_ref[:split, :] = head_ref[...]
        for d in range(depth):
            @pl.when((z_ref[0] ^ step) == d)
            def _(d=d):
                tok_ref[split:, :] = tails[d][...]

        plan = plan_ref[0].astype(F32)
        for i in range(per):
            cols = slice(i * TILE, (i + 1) * TILE)
            gather_tile(n_exp, cum_ref, off_ref, plan, True, step * per + i, cols, tok_ref.at[cols, :], rows_ref)

    def loads(block):
        side = block % 2
        return (
            pltpu.make_async_copy(xs_ref.at[block], x_in.at[side], x_sem.at[side]),
            pltpu.make_async_copy(uv_ref.at[block], uv_in.at[side], uv_sem.at[side]),
        )

    @pl.when((step == depth - 1) & (blk_ref[n_exp] > 0))
    def _():
        for copy in loads(0):
            copy.start()

    def tail_loads(exp, size):
        at = slice(0, size)
        return (
            pltpu.make_async_copy(xt_ref.at[exp, at], xt_in.at[at], t_sem.at[0]),
            pltpu.make_async_copy(uvt_ref.at[exp, :, at], uvt_in.at[:, at], t_sem.at[1]),
        )

    @pl.when((step >= depth) & (step < depth + n_exp))
    def _():
        exp = step - depth
        count = cum_ref[n_tiles * n_exp + exp]
        big, rest = blocks_of(count)
        dim, ff = wg_ref.shape[1:]
        sizes = (ROWS // 2, ROWS // 4)
        for size in sizes:
            @pl.when(rest == size)
            def _(size=size):
                for copy in tail_loads(exp, size):
                    copy.start()

        @pl.when(count == 0)
        def _():
            @pl.loop(0, 3 * dim // ff)
            def _(i):
                dw_ref[0, pl.ds(i * ff, ff), :] = jnp.zeros((ff, ff), F32)

        def run(start, x_blk, uv_blk, copies):
            size = x_blk.shape[0]

            def add(at, value):
                dw_ref[0, at, :] = jnp.where(start == 0, 0.0, dw_ref[0, at, :]) + value

            here = pl.ds(pl.multiple_of(off_ref[exp] + start, ALIGN), size)
            live = lax.broadcasted_iota(jnp.int32, (size, 1), 0) < count - start
            g_old = rows_ref[here, :]
            g_blk = jnp.where(live, g_old, jnp.zeros_like(g_old))
            da = dot(g_blk, wd_ref[0], ((1,), (1,)))
            for copy in copies:
                copy.wait()
            u = uv_blk[0]
            v = uv_blk[1]
            s = jax.nn.sigmoid(u)
            act = (u * s * v).astype(BF16)
            du = (da * v * s * (1.0 + u * (1.0 - s))).astype(BF16)
            dv = (da * u * s).astype(BF16)
            add(slice(2 * dim, 2 * dim + ff), dot(act, g_blk[:, :ff], ((0,), (0,))))
            add(slice(2 * dim + ff, 3 * dim), dot(act, g_blk[:, ff:], ((0,), (0,))))
            dxr = dot(du, wg_ref[0], ((1,), (1,))) + dot(dv, wu_ref[0], ((1,), (1,)))
            rows_ref[here, :] = dxr.astype(BF16)
            add(slice(0, dim), dot(x_blk[...], du, ((0,), (0,))))
            add(slice(dim, 2 * dim), dot(x_blk[...], dv, ((0,), (0,))))

        @pl.loop(0, big)
        def _(b):
            block = blk_ref[exp] + b

            @pl.when(block + 1 < blk_ref[n_exp])
            def _():
                for copy in loads(block + 1):
                    copy.start()

            run(b * ROWS, x_in.at[block % 2], uv_in.at[block % 2], loads(block))

        for size in sizes:
            @pl.when(rest == size)
            def _(size=size):
                run(big * ROWS, xt_in.at[slice(0, size)], uvt_in.at[:, slice(0, size)], tail_loads(exp, size))

    @pl.when(step >= depth + n_exp)
    def _():
        plan_t = jnp.transpose(plan_ref[0].astype(F32))
        for i in range(per):
            tile = (step - depth - n_exp) * per + i
            cols = slice(i * TILE, (i + 1) * TILE)
            scatter_tile(n_exp, cum_ref, off_ref, plan_t, False, tile, cols, rows_ref, win_ref, dx_ref)


def layer_sizes(depth, toks, w_gate, cap):
    tokens = depth * toks
    n_exp = w_gate.shape[0]
    n_tiles = tokens // TILE
    full = lambda n: n // ROWS + (n % ROWS > ROWS // 2)
    part = lambda n: 0 if n % ROWS == 0 or n % ROWS > ROWS // 2 else ROWS // 2 if n % ROWS > ROWS // 4 else ROWS // 4
    most = max(max(full(n) * ROWS + part(n), -(-n // ALIGN) * ALIGN + WIN) for n in range(cap + 1))
    return n_tiles, n_exp, n_exp * most + ROWS, n_exp * max(1, full(cap))


def expert_forward(depth, counts, place, plan_col, x_col, w_gate, w_up, w_down, cap):
    n_tiles, n_exp, rows, blocks = layer_sizes(depth, x_col.shape[1], w_gate, cap)
    toks, dim = x_col.shape[1:]
    ff = w_gate.shape[2]
    first = lambda i: jnp.minimum(i, depth - 1)
    middle = lambda i: jnp.clip(i - depth, 0, n_exp - 1)
    last = lambda i: jnp.maximum(i - depth - n_exp, 0)

    plan_at = lambda i, counts, place: (jnp.where(i < depth, i, place[0] ^ last(i)), place[0], 0)

    wide = pl.BlockSpec((1, dim, ff), lambda i, *_: (middle(i), 0, 0))
    tall = pl.BlockSpec((1, ff, dim), lambda i, *_: (middle(i), 0, 0))
    any_space = pl.BlockSpec(memory_space=pl.ANY)
    shape = jax.ShapeDtypeStruct
    dma = pltpu.SemaphoreType.DMA
    result = pl.pallas_call(
        functools.partial(forward_kernel, depth, n_tiles, n_exp),
        grid_spec=pltpu.PrefetchScalarGridSpec(
            num_scalar_prefetch=2,
            grid=(2 * depth + n_exp,),
            in_specs=[
                pl.BlockSpec((1, 2 * n_exp, toks), plan_at),
                pl.BlockSpec((toks, dim), lambda i, *_: (first(i), 0)), wide, wide, tall,
            ],
            out_specs=[any_space] * (depth + 4),
            scratch_shapes=[
                pltpu.VMEM((rows, dim), BF16), pltpu.VMEM((n_exp * WIN, dim), BF16),
                pltpu.VMEM((2, ROWS, dim), BF16), pltpu.VMEM((2, 2, ROWS, ff), F32),
                pltpu.VMEM((ROWS // 2, dim), BF16), pltpu.VMEM((2, ROWS // 2, ff), F32), pltpu.VMEM((2, toks, dim), F32),
                pltpu.SMEM(((n_tiles + 1) * n_exp,), jnp.int32), pltpu.SMEM((n_exp,), jnp.int32),
                pltpu.SMEM((n_exp + 1,), jnp.int32), pltpu.SMEM((1,), jnp.int32), dma((2,)), dma((2,)), dma((2,)), dma((2,)),
            ],
        ),
        out_shape=[shape((toks, dim), F32)] * depth + [
            shape((blocks, ROWS, dim), BF16), shape((blocks, 2, ROWS, ff), F32),
            shape((n_exp, ROWS // 2, dim), BF16), shape((n_exp, 2, ROWS // 2, ff), F32),
        ],
        compiler_params=pltpu.CompilerParams(dimension_semantics=("arbitrary",), vmem_limit_bytes=64_000_000),
        cost_estimate=pl.CostEstimate(flops=25_000_000_000, bytes_accessed=80_000_000, transcendentals=3_000_000),
        name="forward",
    )(counts, place, plan_col, x_col.reshape(-1, dim), w_gate, w_up, w_down)
    return result[:depth], result[depth:]


def expert_backward(depth, counts, place, plan_col, dy_head, dy_tails, w_gate, w_up, w_down, saved, cap):
    n_tiles, n_exp, rows, blocks = layer_sizes(depth, plan_col.shape[2], w_gate, cap)
    head, dim = dy_head.shape[1:]
    tail = dy_tails[0].shape[0]
    toks = head + tail
    ff = w_gate.shape[2]
    first = lambda i: jnp.minimum(i, depth - 1)
    middle = lambda i: jnp.clip(i - depth, 0, n_exp - 1)
    last = lambda i: jnp.maximum(i - depth - n_exp, 0)

    plan_at = lambda i, counts, place: (jnp.where(i < depth, i, last(i)), place[0], 0)

    wide = pl.BlockSpec((1, dim, ff), lambda i, *_: (middle(i), 0, 0))
    tall = pl.BlockSpec((1, ff, dim), lambda i, *_: (middle(i), 0, 0))
    any_space = pl.BlockSpec(memory_space=pl.ANY)
    shape = jax.ShapeDtypeStruct
    dma = pltpu.SemaphoreType.DMA
    return pl.pallas_call(
        functools.partial(backward_kernel, depth, n_tiles, n_exp),
        grid_spec=pltpu.PrefetchScalarGridSpec(
            num_scalar_prefetch=2,
            grid=(2 * depth + n_exp,),
            in_specs=[
                pl.BlockSpec((1, 2 * n_exp, toks), plan_at),
                pl.BlockSpec((head, dim), lambda i, *_: (first(i), 0)),
                *[pl.BlockSpec((tail, dim), lambda i, *_: (0, 0))] * depth, wide, wide, tall, *[any_space] * 4,
            ],
            out_specs=[
                pl.BlockSpec((toks, dim), lambda i, *_: (last(i), 0)),
                pl.BlockSpec((1, 3 * dim, ff), lambda i, *_: (middle(i), 0, 0)),
            ],
            scratch_shapes=[
                pltpu.VMEM((rows, dim), BF16), pltpu.VMEM((n_exp * WIN, dim), BF16),
                pltpu.VMEM((2, ROWS, dim), BF16), pltpu.VMEM((2, 2, ROWS, ff), F32),
                pltpu.VMEM((ROWS // 2, dim), BF16), pltpu.VMEM((2, ROWS // 2, ff), F32), pltpu.VMEM((toks, dim), BF16),
                pltpu.SMEM(((n_tiles + 1) * n_exp,), jnp.int32), pltpu.SMEM((n_exp,), jnp.int32),
                pltpu.SMEM((n_exp + 1,), jnp.int32), dma((2,)), dma((2,)), dma((2,)),
            ],
        ),
        out_shape=[shape((depth * toks, dim), F32), shape((n_exp, 3 * dim, ff), F32)],
        compiler_params=pltpu.CompilerParams(dimension_semantics=("arbitrary",), vmem_limit_bytes=66_000_000),
        cost_estimate=pl.CostEstimate(flops=50_000_000_000, bytes_accessed=150_000_000, transcendentals=3_000_000),
        name="backward",
    )(counts, place, plan_col, dy_head.reshape(-1, dim), *dy_tails, w_gate, w_up, w_down, *saved)


def finish_kernel(part_refs, dx_ref, g_refs, y_out, dx_out, g_outs, bufs, out_buf, in_sem, out_sem, y_sem):
    moves = [pltpu.make_async_copy(dx_ref, dx_out, out_sem.at[0])]
    moves += [pltpu.make_async_copy(g.at[...], o.at[0], out_sem.at[1 + i]) for i, (g, o) in enumerate(zip(g_refs, g_outs))]
    n = bufs.shape[0]
    rows = bufs.shape[2]
    loads = [
        [pltpu.make_async_copy(p.at[pl.ds(k * rows, rows), :], bufs.at[k, i], in_sem.at[k, i]) for i, p in enumerate(part_refs)]
        for k in range(n)
    ]
    for copies in loads:
        for copy in copies:
            copy.start()
    for move in moves:
        move.start()
    stores = []
    for k in range(n):
        for copy in loads[k]:
            copy.wait()
        value = functools.reduce(jnp.add, [bufs[k, i] for i in range(len(part_refs))])
        out_buf[k] = value.astype(BF16)
        stores.append(pltpu.make_async_copy(out_buf.at[k], y_out.at[pl.ds(k * rows, rows), :], y_sem.at[k]))
        stores[-1].start()
    for copy in moves + stores:
        copy.wait()


def finish(parts, dx, grads):
    toks, dim = dx.shape
    n = 4
    any_space = pl.BlockSpec(memory_space=pl.ANY)
    shape = jax.ShapeDtypeStruct
    dma = pltpu.SemaphoreType.DMA
    k = len(parts)

    def body(*refs):
        finish_kernel(refs[:k], refs[k], refs[k + 1 : k + 4], refs[k + 4], refs[k + 5], refs[k + 6 : k + 9], *refs[k + 9 :])

    return pl.pallas_call(
        body,
        in_specs=[any_space] * (k + 4),
        out_specs=[any_space] * 5,
        out_shape=[shape((toks, dim), BF16), shape((toks, dim), BF16)] + [shape((1, *g.shape), F32) for g in grads],
        scratch_shapes=[
            pltpu.VMEM((n, k, toks // n, dim), F32), pltpu.VMEM((n, toks // n, dim), BF16),
            dma((n, k)), dma((4,)), dma((n,)),
        ],
        compiler_params=pltpu.CompilerParams(vmem_limit_bytes=24_000_000),
        name="finish",
    )(*parts, dx, *grads)


def solution(mesh):
    n_dev = mesh.devices.size
    depth = n_dev // 8
    grid = Mesh(mesh.devices.reshape(depth, 2, 2, 2), ('z', 'y', 'x', 'c'))
    plane = ('y', 'x', 'c')
    spec = P(('z', 'y', 'x', 'c'))

    def local_step(x_tok, route_idx, gates, dy_tok, w_gate, w_up, w_down):
        tok_loc, top_k = route_idx.shape
        cap = depth * (2 * tok_loc * top_k // (n_dev * w_gate.shape[0] - 2))
        n_exp = 8 * w_gate.shape[0]
        head = tok_loc // 16 * HEAD
        x_col, dy_head, dy_tail, plan_col, wg_all, wu_all, wd_all = spread(
            depth, n_dev, head, x_tok, dy_tok, route_idx.T, gates.T, w_gate, w_up, w_down
        )
        turn = lambda a, d: lax.ppermute(a, 'z', [(i, i ^ d) for i in range(depth)])
        dy_tails = [dy_tail] + [turn(dy_tail, d) for d in range(1, depth)]
        place = lax.axis_index('z')
        per = tok_loc // TILE
        counts = lax.dynamic_slice(plan_col[:, 2 * n_dev : 2 * n_dev + per, :n_dev], (0, 0, place * n_exp), (depth, per, n_exp))
        where = (counts.reshape(-1).astype(jnp.int32), place.reshape(1), plan_col)
        y_parts, saved = expert_forward(depth, *where, x_col, wg_all, wu_all, wd_all, cap)
        y_parts, dy_tails = lax.optimization_barrier((y_parts, dy_tails))
        y_sum = y_parts[0]
        turned = [turn(y_parts[d], d) for d in range(1, depth)]
        dx_part, grads = expert_backward(
            depth, *where, dy_head, dy_tails, wg_all, wu_all, wd_all, saved, cap
        )
        dx, *dw = collect(depth, dx_part.reshape(depth, tok_loc, -1), grads)
        return tuple(finish([y_sum, *turned], dx, dw))

    return jax.shard_map(local_step, mesh=grid, in_specs=(spec,) * 7, out_specs=(spec,) * 5, check_vma=False)
```

```python
import functools

import jax
import jax.numpy as jnp
from jax import lax
from jax.experimental import pallas as pl
from jax.experimental.pallas import tpu as pltpu
from jax.sharding import Mesh, PartitionSpec as P

F32 = jnp.float32
BF16 = jnp.bfloat16
TILE = 256
HEAD = 8
WIN = 128
ALIGN = 16
ROWS = 512


def dot(a, b, dims=((1,), (0,))):
    return lax.dot_general(a, b, (dims, ((), ())), preferred_element_type=F32)


MESH = pl.DeviceIdType.MESH


def hop(src, dst, send_sem, recv_sem, **where):
    return pltpu.make_async_remote_copy(
        src_ref=src, dst_ref=dst, send_sem=send_sem, recv_sem=recv_sem, device_id=where, device_id_type=MESH
    )


def meet(depth, z, y, x, c):
    barrier = pltpu.get_barrier_semaphore()
    for where in ({'y': 1 - y}, {'x': 1 - x}, {'c': 1 - c}):
        pl.semaphore_signal(barrier, inc=1, device_id=where, device_id_type=MESH)

    @pl.when(z > 0)
    def _():
        pl.semaphore_signal(barrier, inc=1, device_id={'z': z - 1}, device_id_type=MESH)

    @pl.when(z < depth - 1)
    def _():
        pl.semaphore_signal(barrier, inc=1, device_id={'z': z + 1}, device_id_type=MESH)

    inner = (z > 0) & (z < depth - 1)

    @pl.when(inner)
    def _():
        pl.semaphore_wait(barrier, 5)

    @pl.when(jnp.logical_not(inner))
    def _():
        pl.semaphore_wait(barrier, 4)


def make_plan(experts, route_ref, gate_ref, plan):
    top_k, toks = route_ref.shape
    route = route_ref[...]
    gates = gate_ref[...].astype(F32)
    below = lax.broadcasted_iota(jnp.int32, (TILE, TILE), 0) < lax.broadcasted_iota(jnp.int32, (TILE, TILE), 1)
    below = jnp.where(below, 1.0, 0.0).astype(BF16)
    ones = jnp.ones((16, TILE), BF16)
    ids = lax.broadcasted_iota(jnp.int32, (experts, toks), 0)
    member = jnp.zeros((experts, toks), F32)
    gate = jnp.zeros((experts, toks), F32)
    for k in range(top_k):
        hit = jnp.broadcast_to(route[k : k + 1, :], (experts, toks)) == ids
        member = jnp.where(hit, 1.0, member)
        gate = jnp.where(hit, jnp.broadcast_to(gates[k : k + 1, :], (experts, toks)), gate)
    ranks, counts = [], []
    for t in range(toks // TILE):
        part = member[:, t * TILE : (t + 1) * TILE]
        ranks.append(jnp.where(part > 0.5, dot(part.astype(BF16), below), -4096.0))
        counts.append(dot(ones, part.astype(BF16), ((1,), (1,))))
    rank = jnp.concatenate(ranks, axis=1)
    for p in range(experts // 8):
        both = jnp.concatenate([rank[8 * p : 8 * p + 8], gate[8 * p : 8 * p + 8]], axis=0)
        plan[16 * p : 16 * p + 16, :] = both.astype(BF16)
    which = lax.broadcasted_iota(jnp.int32, (16, experts), 0)
    count = functools.reduce(jnp.add, [jnp.where(which == t, c, 0.0) for t, c in enumerate(counts)])
    plan[2 * experts :, :] = jnp.zeros((16, toks), BF16)
    plan[2 * experts :, :experts] = count.astype(BF16)


def spread_kernel(
    depth, experts, x_ref, dy_ref, route_ref, gate_ref, wg_ref, wu_ref, wd_ref,
    x_out, dy_out, tail_out, plan_out, wg_out, wu_out, wd_out,
    stage_t, stage_w, stage_d, plan, own_sem, z_send, z_recv, p_send, p_recv, c_send, c_recv,
):
    z, y, x, c = (lax.axis_index(a) for a in 'zyxc')
    slot = lambda yy, xx: yy * 4 + xx * 2 + c
    own, by_x, by_y, far = slot(y, x), slot(y, 1 - x), slot(1 - y, x), slot(1 - y, 1 - x)
    weights = ((wg_ref, wg_out), (wu_ref, wu_out), (wd_ref, wd_out))
    dy_head = dy_ref.at[pl.ds(0, dy_out.shape[1]), :]
    arrays = ((x_ref, x_out), (plan, plan_out), (dy_head, dy_out))
    sent = []

    def half(ref, where, h):
        rows = ref.shape[1] // 2
        return ref.at[where, pl.ds(h * rows, rows), :]

    def own_half(part, h, side):
        src, out = weights[part]
        where = {'x': 1 - x} if side == 0 else {'y': 1 - y}
        return hop(half(src, 0, h), half(out, own, h), p_send.at[side, part, h], p_recv.at[side, part, h], **where)

    def onward(part, h):
        at = half(weights[part][1], by_x if h == 0 else by_y, h)
        where = {'y': 1 - y} if h == 0 else {'x': 1 - x}
        return hop(at, at, p_send.at[2, part, h], p_recv.at[2, part, h], **where)

    def landed(part, h, kind):
        at = half(weights[part][1], (by_x, by_y, far)[kind], h)
        hop(at, at, p_send.at[kind, part, h], p_recv.at[kind, part, h], c=1 - c).wait_recv()

    def across(part, h, kind):
        at = half(weights[part][1], (by_x, by_y, far)[kind], h)
        return hop(at, at, c_send.at[kind, part, h], c_recv.at[kind, part, h], c=1 - c)

    def across_own(part, h):
        src, out = weights[part]
        return hop(half(src, 0, h), half(out, own, h), c_send.at[3, part, h], c_recv.at[3, part, h], c=1 - c)

    def crossed(part, h, kind):
        twin = lambda yy, xx: yy * 4 + xx * 2 + 1 - c
        where = (twin(y, 1 - x), twin(1 - y, x), twin(1 - y, 1 - x), twin(y, x))[kind]
        at = half(weights[part][1], where, h)
        hop(at, at, c_send.at[kind, part, h], c_recv.at[kind, part, h], c=1 - c).wait_recv()

    def go(copy):
        copy.start()
        sent.append((None, copy))

    def along(k, dist, up):
        src, out = arrays[k]
        at = out.at[z - dist if up else z + dist]
        side = 0 if up else 1
        return hop(src if dist == 0 else at, at, z_send.at[side, k, dist], z_recv.at[side, k, dist], z=z + 1 if up else z - 1)

    def start_along(k, dist):
        for up in (True, False):
            cond = (z >= dist) & (z < depth - 1) if up else (z + dist < depth) & (z > 0)

            @pl.when(cond)
            def _(up=up):
                along(k, dist, up).start()

            sent.append((cond, along(k, dist, up)))

    def await_along(k, dist):
        for up in (True, False):
            @pl.when(z > dist if up else z + dist + 1 < depth)
            def _(up=up):
                at = arrays[k][1].at[z - dist - 1 if up else z + dist + 1]
                side = 0 if up else 1
                hop(at, at, z_send.at[side, k, dist], z_recv.at[side, k, dist], c=1 - c).wait_recv()

        if dist + 1 < depth - 1:
            start_along(k, dist + 1)

    copies = []
    for i, (src, buf, out) in enumerate((
        (x_ref, stage_t.at[0], x_out.at[z]), (dy_head, stage_t.at[1, pl.ds(0, dy_out.shape[1]), :], dy_out.at[z]),
        (dy_ref.at[pl.ds(dy_out.shape[1], tail_out.shape[0]), :], stage_t.at[1, pl.ds(dy_out.shape[1], tail_out.shape[0]), :], tail_out),
        (wg_ref.at[0], stage_w.at[0], wg_out.at[own]), (wu_ref.at[0], stage_w.at[1], wu_out.at[own]),
        (wd_ref.at[0], stage_d, wd_out.at[own]),
    )):
        copies.append((pltpu.make_async_copy(src, buf, own_sem.at[i]), pltpu.make_async_copy(buf, out, own_sem.at[i])))
        copies[-1][0].start()

    meet(depth, z, y, x, c)
    start_along(0, 0)
    for part in range(3):
        go(own_half(part, 0, 0))
        go(own_half(part, 1, 1))
    for part in range(3):
        go(own_half(part, 1, 0))
        go(own_half(part, 0, 1))
    for part in range(3):
        for h in range(2):
            go(across_own(part, h))
    make_plan(experts, route_ref, gate_ref, plan)
    start_along(1, 0)
    start_along(2, 0)
    copies.append((None, pltpu.make_async_copy(plan, plan_out.at[z], own_sem.at[6])))
    for i, (load, store) in enumerate(copies):
        if load is not None:
            load.wait()
        store.start()

    def relay(part, h):
        landed(part, h, h)
        go(onward(part, h))
        go(across(part, h, h))

    def relay_twin(part, h):
        landed(part, h, 1 - h)
        go(across(part, h, 1 - h))

    def relay_far(part):
        for h in range(2):
            landed(part, h, 2)
            go(across(part, h, 2))

    for part in range(2):
        relay(part, 0)
        relay(part, 1)
    await_along(0, 0)
    await_along(1, 0)
    relay(2, 0)
    relay(2, 1)
    await_along(2, 0)
    for part in range(2):
        relay_twin(part, 1)
        relay_twin(part, 0)
    await_along(0, 1)
    await_along(1, 1)
    relay_twin(2, 1)
    relay_twin(2, 0)
    await_along(2, 1)
    relay_far(0)
    relay_far(1)
    await_along(0, 2)
    await_along(1, 2)
    relay_far(2)
    await_along(2, 2)
    for part in range(3):
        for h in range(2):
            for kind in range(4):
                crossed(part, h, kind)
    for cond, copy in sent:
        if cond is None:
            copy.wait_send()
        else:
            @pl.when(cond)
            def _(copy=copy):
                copy.wait_send()
    for _, store in copies:
        store.wait()


def spread(depth, experts, head, x_tok, dy_tok, route, gate, w_gate, w_up, w_down):
    toks, dim = x_tok.shape
    ff = w_down.shape[1]
    any_space = pl.BlockSpec(memory_space=pl.ANY)
    vmem = pl.BlockSpec(memory_space=pltpu.VMEM)
    rows = 2 * experts + 16
    shape = jax.ShapeDtypeStruct
    dma = pltpu.SemaphoreType.DMA
    return pl.pallas_call(
        functools.partial(spread_kernel, depth, experts),
        in_specs=[any_space, any_space, vmem, vmem, any_space, any_space, any_space],
        out_specs=[any_space] * 7,
        out_shape=[
            shape((depth, toks, dim), BF16), shape((depth, head, dim), BF16), shape((toks - head, dim), BF16), shape((depth, rows, toks), BF16),
            shape((8, dim, ff), BF16), shape((8, dim, ff), BF16), shape((8, ff, dim), BF16),
        ],
        scratch_shapes=[
            pltpu.VMEM((2, toks, dim), BF16), pltpu.VMEM((2, dim, ff), BF16), pltpu.VMEM((ff, dim), BF16),
            pltpu.VMEM((rows, toks), BF16), dma((7,)), dma((2, 3, depth)), dma((2, 3, depth)),
            dma((3, 3, 2)), dma((3, 3, 2)), dma((4, 3, 2)), dma((4, 3, 2)),
        ],
        compiler_params=pltpu.CompilerParams(collective_id=0, has_side_effects=True),
        name="spread",
    )(x_tok, dy_tok, route, gate, w_gate, w_up, w_down)


CHUNK = 128
BAND = 64
TURNS = (4, 15, 22, 24)
FINISH = 3
RING = 6


def collect_kernel(
    depth, dx_ref, g_ref, dx_out, gate_out, up_out, down_out, twin,
    z_land, x_land, y_land, x_last, y_last, total, x_buf, y_buf, f_buf, z_buf,
    t_sem, x_load, y_load, f_load, z_load, z_send, z_recv, x_send, x_recv, y_send, y_recv, c_send, c_recv,
):
    z, y, x, c = (lax.axis_index(a) for a in 'zyxc')
    cell = lambda yy, xx: yy * 2 + xx
    mine, by_x, by_y, far = cell(y, x), cell(y, 1 - x), cell(1 - y, x), cell(1 - y, 1 - x)
    bands = dx_ref.shape[1] // BAND
    n_part = g_ref.shape[1] // CHUNK // 2
    n_col = (depth - 1) * bands
    n_link = 3 * n_part
    piece = 4 * CHUNK
    order = (far, by_x, by_y, mine)
    rows = lambda i: pl.ds(pl.multiple_of(i * CHUNK, CHUNK), CHUNK)

    def swap(kind, q):
        at = pl.ds(q * piece, piece)
        return hop(g_ref.at[2 * order[kind] + 1 - c, at, :], twin.at[order[kind], at, :], c_send.at[kind, q], c_recv.at[kind, q], c=1 - c)

    half = n_part // 4
    swaps = [(0, q + h * half) for q in range(half) for h in range(2)]
    swaps += [(1 + h, q + h * half) for q in range(half) for h in range(2)]
    swaps += [(2 - h, q + h * half) for q in range(half) for h in range(2)]
    swaps += [(3, q + h * half) for q in range(half) for h in range(2)]

    own_total = pltpu.make_async_copy(dx_ref.at[z], total, t_sem)
    own_total.start()
    meet(depth, z, y, x, c)
    for kind, q in swaps:
        swap(kind, q).start()

    def link_item(side, i):
        leg = i // n_part
        j = i % n_part
        near, other = (by_x, by_y) if side == 0 else (by_y, by_x)
        kind_near, kind_other = (1, 2) if side == 0 else (2, 1)
        first = jnp.where(leg < 2, side, 1 - side)
        chunk = first * n_part + j
        expert = jnp.where(leg == 0, far, near)
        kind = jnp.where(leg == 0, 0, kind_near)
        return leg, j, chunk, expert, kind

    def fetch(chunk, expert, kind, fresh, buf, sems):
        @pl.when(fresh)
        def _():
            for k in range(4):
                @pl.when(kind == k)
                def _(k=k):
                    at = pl.ds(pl.multiple_of(chunk // 4 * piece, piece), piece)
                    q = chunk // 4
                    hop(twin.at[order[k], at, :], twin.at[order[k], at, :], c_send.at[k, q], c_recv.at[k, q], c=1 - c).wait_recv()

        pltpu.make_async_copy(g_ref.at[2 * expert + c, rows(chunk), :], buf.at[0], sems.at[0]).start()
        pltpu.make_async_copy(twin.at[expert, rows(chunk), :], buf.at[1], sems.at[1]).start()

    def fetched(buf, sems):
        pltpu.make_async_copy(g_ref.at[0, rows(0), :], buf.at[0], sems.at[0]).wait()
        pltpu.make_async_copy(twin.at[0, rows(0), :], buf.at[1], sems.at[1]).wait()

    links = (
        (x_buf, x_load, x_send, x_recv, x_land, x_last, {'x': 1 - x}),
        (y_buf, y_load, y_send, y_recv, y_land, y_last, {'y': 1 - y}),
    )

    def landing(side, i):
        land, last = links[side][4], links[side][5]
        return land, last

    def link_send(side, i, wait_only=False):
        buf, _, send, recv, land, last, where = links[side]
        src = buf.at[i % RING, 0]

        @pl.when(i < 2 * n_part)
        def _():
            copy = hop(src, land.at[jnp.minimum(i, 2 * n_part - 1)], send.at[i], recv.at[i], **where)
            copy.wait_send() if wait_only else copy.start()

        @pl.when(i >= 2 * n_part)
        def _():
            copy = hop(src, last.at[jnp.maximum(i - 2 * n_part, 0)], send.at[i], recv.at[i], **where)
            copy.wait_send() if wait_only else copy.start()

    def landed(side, ref, i):
        recv, send = links[side][3], links[side][2]
        hop(ref, ref, send.at[i], recv.at[i], c=1 - c).wait_recv()

    def link_prepare(side, i):
        buf, load = links[side][0], links[side][1]

        @pl.when((i >= RING) & (i < n_link))
        def _():
            link_send(side, i - RING, wait_only=True)

        @pl.when(i < n_link)
        def _():
            leg, j, chunk, expert, kind = link_item(side, i)
            fetch(chunk, expert, kind, j % 4 == 0, buf.at[i % RING], load.at[i % RING])

    def link_turn(side, i):
        buf, load = links[side][0], links[side][1]
        other_land = links[1 - side][4]

        @pl.when(i < n_link)
        def _():
            b = i % RING
            fetched(buf.at[b], load.at[b])
            buf[b, 0] += buf[b, 1]

            @pl.when(i >= 2 * n_part)
            def _():
                j = i - 2 * n_part
                landed(1 - side, other_land.at[j], j)
                buf[b, 0] += other_land[j]

            link_send(side, i)

    def last_prepare(h, j):
        @pl.when((j >= 0) & (j < n_part))
        def _():
            fetch(h * n_part + j, mine, 3, j % 4 == 0, f_buf.at[h, j % 2], f_load.at[h, j % 2])

    def last_turn(h, j):
        @pl.when((j >= 0) & (j < n_part))
        def _():
            land, last = links[h][4], links[1 - h][5]
            fetched(f_buf.at[h, j % 2], f_load.at[h, j % 2])
            landed(h, land.at[n_part + j], n_part + j)
            landed(1 - h, last.at[j], 2 * n_part + j)
            value = f_buf[h, j % 2, 0] + f_buf[h, j % 2, 1] + (land[n_part + j] + last[j])
            chunk = h * n_part + j
            tall = gate_out.shape[0] // CHUNK
            places = ((0, tall, gate_out, 0), (tall, 2 * tall, up_out, 0), (2 * tall, 5 * tall // 2, down_out, 0), (5 * tall // 2, 3 * tall, down_out, 1))
            for first, end, out, side in places:
                if first < (h + 1) * n_part and end > h * n_part:
                    @pl.when((chunk >= first) & (chunk < end))
                    def _(first=first, out=out, side=side):
                        cols = pl.ds(side * value.shape[1], value.shape[1])
                        out[rows(chunk - first), cols] = value

    def column(side, k):
        role = z if side == 0 else depth - 1 - z
        goal = depth - 1 - k // bands
        block = goal if side == 0 else depth - 1 - goal
        slot = block + 1 if side == 0 else block
        at = pl.ds(pl.multiple_of(k % bands * BAND, BAND), BAND)
        return role, goal, block, slot, at

    def column_copy(side, k, src):
        _, _, _, slot, at = column(side, k)
        return hop(src, z_land.at[slot, at, :], z_send.at[side, k], z_recv.at[side, k], z=z + 1 if side == 0 else z - 1)

    def turn_of(side, t):
        role = z if side == 0 else depth - 1 - z
        return t - functools.reduce(lambda late, r: jnp.where(role == r, TURNS[r], late), range(1, depth), TURNS[0])

    def column_prepare(side, t):
        k = turn_of(side, t)
        kk = jnp.clip(k, 0, n_col - 1)
        role, goal, block, slot, at = column(side, kk)

        @pl.when((k >= 0) & (k < n_col) & (role > 0) & (goal > role))
        def _():
            pltpu.make_async_copy(dx_ref.at[block, at, :], z_buf.at[side, kk % 2], z_load.at[side, kk % 2]).start()

    def column_turn(side, t):
        k = turn_of(side, t)
        kk = jnp.clip(k, 0, n_col - 1)
        role, goal, block, slot, at = column(side, kk)
        live = (k >= 0) & (k < n_col) & (goal >= role)

        @pl.when(live & (role == 0))
        def _():
            column_copy(side, kk, dx_ref.at[block, at, :]).start()

        @pl.when(live & (role > 0))
        def _():
            here = z_land.at[slot, at, :]
            hop(here, here, z_send.at[side, kk], z_recv.at[side, kk], c=1 - c).wait_recv()

            @pl.when(goal > role)
            def _():
                pltpu.make_async_copy(dx_ref.at[block, at, :], z_buf.at[side, kk % 2], z_load.at[side, kk % 2]).wait()
                z_land[slot, at, :] += z_buf[side, kk % 2]
                column_copy(side, kk, here).start()

            @pl.when(goal == role)
            def _():
                total[at, :] += z_land[slot, at, :]

    def prepare(t):
        for side in range(2):
            link_prepare(side, t)
            column_prepare(side, t)
            last_prepare(side, t - 2 * n_part - FINISH)

    prepare(jnp.int32(0))
    own_total.wait()
    steps = max(max(TURNS) + n_col, n_link + FINISH)

    @pl.loop(0, steps)
    def _(t):
        prepare(t + 1)
        for side in range(2):
            link_turn(side, t)
        for side in range(2):
            column_turn(side, t)
        for side in range(2):
            last_turn(side, t - 2 * n_part - FINISH)

    dx_out[...] = total[...].astype(BF16)

    @pl.loop(n_link - RING, n_link)
    def _(i):
        for side in range(2):
            link_send(side, i, wait_only=True)

    @pl.loop(0, n_col)
    def _(k):
        for side in range(2):
            role, goal, block, slot, at = column(side, k)

            @pl.when(goal > role)
            def _():
                column_copy(side, k, z_land.at[slot, at, :]).wait_send()

    for kind, q in swaps:
        swap(kind, q).wait_send()


def collect(depth, dx_part, grads):
    toks, dim = dx_part.shape[1:]
    height, ff = grads.shape[1:]
    n_part = height // CHUNK // 2
    n_col = (depth - 1) * (toks // BAND)
    any_space = pl.BlockSpec(memory_space=pl.ANY)
    vmem = pl.BlockSpec(memory_space=pltpu.VMEM)
    shape = jax.ShapeDtypeStruct
    dma = pltpu.SemaphoreType.DMA
    message = (CHUNK, ff)
    return pl.pallas_call(
        functools.partial(collect_kernel, depth),
        in_specs=[any_space, any_space],
        out_specs=[vmem, vmem, vmem, vmem, any_space],
        out_shape=[pltpu.VMEM((toks, dim), BF16), pltpu.VMEM((dim, ff), F32), pltpu.VMEM((dim, ff), F32), pltpu.VMEM((ff, dim), F32), shape((4, height, ff), F32)],
        scratch_shapes=[
            pltpu.VMEM((depth + 1, toks, dim), F32),
            pltpu.VMEM((2 * n_part, *message), F32), pltpu.VMEM((2 * n_part, *message), F32),
            pltpu.VMEM((n_part, *message), F32), pltpu.VMEM((n_part, *message), F32),
            pltpu.VMEM((toks, dim), F32),
            pltpu.VMEM((RING, 2, *message), F32), pltpu.VMEM((RING, 2, *message), F32),
            pltpu.VMEM((2, 2, 2, *message), F32), pltpu.VMEM((2, 2, BAND, dim), F32),
            dma, dma((RING, 2)), dma((RING, 2)), dma((2, 2, 2)), dma((2, 2)),
            dma((2, n_col)), dma((2, n_col)), dma((3 * n_part,)), dma((3 * n_part,)), dma((3 * n_part,)), dma((3 * n_part,)),
            dma((4, height // CHUNK // 4)), dma((4, height // CHUNK // 4)),
        ],
        compiler_params=pltpu.CompilerParams(collective_id=1, has_side_effects=True, vmem_limit_bytes=46_000_000),
        name="collect",
    )(dx_part, grads)[:4]


def count_up(n_tiles, n_exp, count_ref, cum_ref, off_ref, blk_ref):
    base = jnp.int32(0)
    block = jnp.int32(0)
    for exp in range(n_exp):
        run = jnp.int32(0)
        cum_ref[exp] = run
        for tile in range(n_tiles):
            run += count_ref[tile * n_exp + exp]
            cum_ref[(tile + 1) * n_exp + exp] = run
        off_ref[exp] = base
        blk_ref[exp] = block
        big, rest = blocks_of(run)
        block += big
        base += jnp.maximum(big * ROWS + rest, (run + ALIGN - 1) // ALIGN * ALIGN + WIN)
    blk_ref[n_exp] = block


def blocks_of(count):
    over = count % ROWS
    big = count // ROWS + jnp.where(over > ROWS // 2, 1, 0)
    rest = jnp.where(over > ROWS // 4, ROWS // 2, jnp.where(over > 0, ROWS // 4, 0))
    return big, jnp.where(over > ROWS // 2, 0, rest)


def span(n_exp, cum_ref, tile, exp):
    lo = cum_ref[tile * n_exp + exp]
    hi = cum_ref[(tile + 1) * n_exp + exp]
    return lo, hi, (lo // ALIGN) * ALIGN


def gather_tile(n_exp, cum_ref, off_ref, plan, gated, tile, cols, toks, rows_ref):
    rank, gate = plan[:n_exp, cols], plan[n_exp:, cols]
    row = lax.broadcasted_iota(jnp.int32, (WIN, TILE), 0).astype(F32)

    def window(exp, lo, start):
        hit = rank[exp : exp + 1] == row + (start - lo).astype(F32)
        take = jnp.where(hit, gate[exp : exp + 1] if gated else 1.0, 0.0).astype(BF16)
        return dot(take, toks[...]).astype(BF16)

    def rows_at(exp, start, size):
        return pl.ds(pl.multiple_of(off_ref[exp] + start, ALIGN), size)

    spans = [span(n_exp, cum_ref, tile, exp) for exp in range(n_exp)]
    for exp, (lo, hi, start) in enumerate(spans):
        value = window(exp, lo, start)
        head = rows_at(exp, start, ALIGN)
        fresh = lax.broadcasted_iota(jnp.int32, (ALIGN, 1), 0) + start >= lo
        rows_ref[head, :] = jnp.where(fresh, value[:ALIGN], rows_ref[head, :])
        rows_ref[rows_at(exp, start + ALIGN, WIN - ALIGN), :] = value[ALIGN:]
    most = functools.reduce(jnp.maximum, [hi - start for lo, hi, start in spans])

    @pl.when(most > WIN)
    def _more():
        for exp, (lo, hi, start) in enumerate(spans):
            @pl.loop(1, (hi - start + WIN - 1) // WIN)
            def _(w):
                rows_ref[rows_at(exp, start + w * WIN, WIN), :] = window(exp, lo, start + w * WIN)


def scatter_tile(n_exp, cum_ref, off_ref, plan_t, gated, tile, cols, rows_ref, win_ref, out_ref):
    column = lax.broadcasted_iota(jnp.int32, (TILE, WIN), 1).astype(F32)

    def window(exp, lo, start):
        hit = plan_t[cols, exp : exp + 1] == column + (start - lo).astype(F32)
        put = jnp.where(hit, plan_t[cols, n_exp + exp : n_exp + exp + 1] if gated else 1.0, 0.0).astype(BF16)
        return put, rows_ref[pl.ds(pl.multiple_of(off_ref[exp] + start, ALIGN), WIN), :]

    spans = [span(n_exp, cum_ref, tile, exp) for exp in range(n_exp)]
    puts = []
    for exp, (lo, hi, start) in enumerate(spans):
        put, block = window(exp, lo, start)
        puts.append(put)
        win_ref[exp * WIN : (exp + 1) * WIN, :] = block
    out_ref[cols, :] = dot(jnp.concatenate(puts, axis=1), win_ref[...])
    most = functools.reduce(jnp.maximum, [hi - start for lo, hi, start in spans])

    @pl.when(most > WIN)
    def _more():
        for exp, (lo, hi, start) in enumerate(spans):
            @pl.loop(1, (hi - start + WIN - 1) // WIN)
            def _(w):
                put, block = window(exp, lo, start + w * WIN)
                out_ref[cols, :] += dot(put, block)


def forward_kernel(
    depth, n_tiles, n_exp, count_ref, z_ref, plan_ref, x_ref, wg_ref, wu_ref, wd_ref,
    *refs,
):
    y_refs, refs = refs[:depth], refs[depth:]
    xs_ref, uv_ref, xt_ref, uvt_ref, rows_ref, win_ref, x_out, uv_out, xt_out, uvt_out, y_buf = refs[:11]
    cum_ref, off_ref, blk_ref, tail_ref, x_sem, uv_sem, t_sem, y_sem = refs[11:]
    step = pl.program_id(0)
    per = n_tiles // depth

    @pl.when(step == 0)
    def _():
        count_up(n_tiles, n_exp, count_ref, cum_ref, off_ref, blk_ref)
        tail_ref[0] = 0

    @pl.when(step < depth)
    def _():
        plan = plan_ref[0].astype(F32)
        for i in range(per):
            cols = slice(i * TILE, (i + 1) * TILE)
            gather_tile(n_exp, cum_ref, off_ref, plan, False, step * per + i, cols, x_ref.at[cols, :], rows_ref)

    def saves(block):
        side = block % 2
        return (
            pltpu.make_async_copy(x_out.at[side], xs_ref.at[block], x_sem.at[side]),
            pltpu.make_async_copy(uv_out.at[side], uv_ref.at[block], uv_sem.at[side]),
        )

    def tail_saves(exp, size):
        at = slice(0, size)
        return (
            pltpu.make_async_copy(xt_out.at[at], xt_ref.at[exp, at], t_sem.at[0]),
            pltpu.make_async_copy(uvt_out.at[:, at], uvt_ref.at[exp, :, at], t_sem.at[1]),
        )

    def tail_saved():
        for size in (ROWS // 2, ROWS // 4):
            @pl.when(tail_ref[0] == size)
            def _(size=size):
                for copy in tail_saves(0, size):
                    copy.wait()

    @pl.when((step >= depth) & (step < depth + n_exp))
    def _():
        exp = step - depth
        count = cum_ref[n_tiles * n_exp + exp]
        big, rest = blocks_of(count)

        def run(start, x_blk, uv_blk):
            size = x_blk.shape[0]
            here = pl.ds(pl.multiple_of(off_ref[exp] + start, ALIGN), size)
            live = lax.broadcasted_iota(jnp.int32, (size, 1), 0) < count - start
            x_old = rows_ref[here, :]
            x_blk[...] = jnp.where(live, x_old, jnp.zeros_like(x_old))
            u = dot(x_blk[...], wg_ref[0])
            v = dot(x_blk[...], wu_ref[0])
            uv_blk[0] = u
            uv_blk[1] = v
            act = (u * jax.nn.sigmoid(u) * v).astype(BF16)
            rows_ref[here, :] = dot(act, wd_ref[0]).astype(BF16)

        @pl.loop(0, big)
        def _(b):
            block = blk_ref[exp] + b

            @pl.when(block >= 2)
            def _():
                for copy in saves(block - 2):
                    copy.wait()

            run(b * ROWS, x_out.at[block % 2], uv_out.at[block % 2])
            for copy in saves(block):
                copy.start()

        for size in (ROWS // 2, ROWS // 4):
            @pl.when(rest == size)
            def _(size=size):
                tail_saved()
                run(big * ROWS, xt_out.at[slice(0, size)], uvt_out.at[:, slice(0, size)])
                for copy in tail_saves(exp, size):
                    copy.start()
                tail_ref[0] = size

    @pl.when(step == depth + n_exp)
    def _():
        total = blk_ref[n_exp]
        for back in (2, 1):
            @pl.when(total >= back)
            def _():
                for copy in saves(total - back):
                    copy.wait()

        tail_saved()

    d = step - depth - n_exp

    def y_copy(d, k):
        return pltpu.make_async_copy(y_buf.at[k % 2], y_refs[k], y_sem.at[k % 2])

    @pl.when(d >= 0)
    def _():
        for k in range(2, depth):
            @pl.when(d == k)
            def _(k=k):
                y_copy(d, k - 2).wait()

        plan_t = jnp.transpose(plan_ref[0].astype(F32))
        for i in range(per):
            tile = (z_ref[0] ^ d) * per + i
            cols = slice(i * TILE, (i + 1) * TILE)
            scatter_tile(n_exp, cum_ref, off_ref, plan_t, True, tile, cols, rows_ref, win_ref, y_buf.at[d % 2])
        for k in range(depth):
            @pl.when(d == k)
            def _(k=k):
                y_copy(d, k).start()

    @pl.when(d == depth - 1)
    def _():
        y_copy(d, depth - 2).wait()
        y_copy(d, depth - 1).wait()


def backward_kernel(
    depth, n_tiles, n_exp, count_ref, z_ref, plan_ref, head_ref, *refs,
):
    tails, refs = refs[:depth], refs[depth:]
    wg_ref, wu_ref, wd_ref, xs_ref, uv_ref, xt_ref, uvt_ref, dx_ref, dw_ref = refs[:9]
    rows_ref, win_ref, x_in, uv_in, xt_in, uvt_in, tok_ref, cum_ref, off_ref, blk_ref, x_sem, uv_sem, t_sem = refs[9:]
    step = pl.program_id(0)
    per = n_tiles // depth

    @pl.when(step == 0)
    def _():
        count_up(n_tiles, n_exp, count_ref, cum_ref, off_ref, blk_ref)

    @pl.when(step < depth)
    def _():
        split = head_ref.shape[0]
        tok_ref[:split, :] = head_ref[...]
        for d in range(depth):
            @pl.when((z_ref[0] ^ step) == d)
            def _(d=d):
                tok_ref[split:, :] = tails[d][...]

        plan = plan_ref[0].astype(F32)
        for i in range(per):
            cols = slice(i * TILE, (i + 1) * TILE)
            gather_tile(n_exp, cum_ref, off_ref, plan, True, step * per + i, cols, tok_ref.at[cols, :], rows_ref)

    def loads(block):
        side = block % 2
        return (
            pltpu.make_async_copy(xs_ref.at[block], x_in.at[side], x_sem.at[side]),
            pltpu.make_async_copy(uv_ref.at[block], uv_in.at[side], uv_sem.at[side]),
        )

    @pl.when((step == depth - 1) & (blk_ref[n_exp] > 0))
    def _():
        for copy in loads(0):
            copy.start()

    def tail_loads(exp, size):
        at = slice(0, size)
        return (
            pltpu.make_async_copy(xt_ref.at[exp, at], xt_in.at[at], t_sem.at[0]),
            pltpu.make_async_copy(uvt_ref.at[exp, :, at], uvt_in.at[:, at], t_sem.at[1]),
        )

    @pl.when((step >= depth) & (step < depth + n_exp))
    def _():
        exp = step - depth
        count = cum_ref[n_tiles * n_exp + exp]
        big, rest = blocks_of(count)
        dim, ff = wg_ref.shape[1:]
        sizes = (ROWS // 2, ROWS // 4)
        for size in sizes:
            @pl.when(rest == size)
            def _(size=size):
                for copy in tail_loads(exp, size):
                    copy.start()

        @pl.when(count == 0)
        def _():
            @pl.loop(0, 3 * dim // ff)
            def _(i):
                dw_ref[0, pl.ds(i * ff, ff), :] = jnp.zeros((ff, ff), F32)

        def run(start, x_blk, uv_blk, copies):
            size = x_blk.shape[0]

            def add(at, value):
                dw_ref[0, at, :] = jnp.where(start == 0, 0.0, dw_ref[0, at, :]) + value

            here = pl.ds(pl.multiple_of(off_ref[exp] + start, ALIGN), size)
            live = lax.broadcasted_iota(jnp.int32, (size, 1), 0) < count - start
            g_old = rows_ref[here, :]
            g_blk = jnp.where(live, g_old, jnp.zeros_like(g_old))
            da = dot(g_blk, wd_ref[0], ((1,), (1,)))
            for copy in copies:
                copy.wait()
            u = uv_blk[0]
            v = uv_blk[1]
            s = jax.nn.sigmoid(u)
            act = (u * s * v).astype(BF16)
            du = (da * v * s * (1.0 + u * (1.0 - s))).astype(BF16)
            dv = (da * u * s).astype(BF16)
            add(slice(2 * dim, 2 * dim + ff), dot(act, g_blk[:, :ff], ((0,), (0,))))
            add(slice(2 * dim + ff, 3 * dim), dot(act, g_blk[:, ff:], ((0,), (0,))))
            dxr = dot(du, wg_ref[0], ((1,), (1,))) + dot(dv, wu_ref[0], ((1,), (1,)))
            rows_ref[here, :] = dxr.astype(BF16)
            add(slice(0, dim), dot(x_blk[...], du, ((0,), (0,))))
            add(slice(dim, 2 * dim), dot(x_blk[...], dv, ((0,), (0,))))

        @pl.loop(0, big)
        def _(b):
            block = blk_ref[exp] + b

            @pl.when(block + 1 < blk_ref[n_exp])
            def _():
                for copy in loads(block + 1):
                    copy.start()

            run(b * ROWS, x_in.at[block % 2], uv_in.at[block % 2], loads(block))

        for size in sizes:
            @pl.when(rest == size)
            def _(size=size):
                run(big * ROWS, xt_in.at[slice(0, size)], uvt_in.at[:, slice(0, size)], tail_loads(exp, size))

    @pl.when(step >= depth + n_exp)
    def _():
        plan_t = jnp.transpose(plan_ref[0].astype(F32))
        for i in range(per):
            tile = (step - depth - n_exp) * per + i
            cols = slice(i * TILE, (i + 1) * TILE)
            scatter_tile(n_exp, cum_ref, off_ref, plan_t, False, tile, cols, rows_ref, win_ref, dx_ref)


def layer_sizes(depth, toks, w_gate, cap):
    tokens = depth * toks
    n_exp = w_gate.shape[0]
    n_tiles = tokens // TILE
    full = lambda n: n // ROWS + (n % ROWS > ROWS // 2)
    part = lambda n: 0 if n % ROWS == 0 or n % ROWS > ROWS // 2 else ROWS // 2 if n % ROWS > ROWS // 4 else ROWS // 4
    most = max(max(full(n) * ROWS + part(n), -(-n // ALIGN) * ALIGN + WIN) for n in range(cap + 1))
    return n_tiles, n_exp, n_exp * most + ROWS, n_exp * max(1, full(cap))


def expert_forward(depth, counts, place, plan_col, x_col, w_gate, w_up, w_down, cap):
    n_tiles, n_exp, rows, blocks = layer_sizes(depth, x_col.shape[1], w_gate, cap)
    toks, dim = x_col.shape[1:]
    ff = w_gate.shape[2]
    first = lambda i: jnp.minimum(i, depth - 1)
    middle = lambda i: jnp.clip(i - depth, 0, n_exp - 1)
    last = lambda i: jnp.maximum(i - depth - n_exp, 0)

    plan_at = lambda i, counts, place: (jnp.where(i < depth, i, place[0] ^ last(i)), place[0], 0)

    wide = pl.BlockSpec((1, dim, ff), lambda i, *_: (middle(i), 0, 0))
    tall = pl.BlockSpec((1, ff, dim), lambda i, *_: (middle(i), 0, 0))
    any_space = pl.BlockSpec(memory_space=pl.ANY)
    shape = jax.ShapeDtypeStruct
    dma = pltpu.SemaphoreType.DMA
    result = pl.pallas_call(
        functools.partial(forward_kernel, depth, n_tiles, n_exp),
        grid_spec=pltpu.PrefetchScalarGridSpec(
            num_scalar_prefetch=2,
            grid=(2 * depth + n_exp,),
            in_specs=[
                pl.BlockSpec((1, 2 * n_exp, toks), plan_at),
                pl.BlockSpec((toks, dim), lambda i, *_: (first(i), 0)), wide, wide, tall,
            ],
            out_specs=[any_space] * (depth + 4),
            scratch_shapes=[
                pltpu.VMEM((rows, dim), BF16), pltpu.VMEM((n_exp * WIN, dim), BF16),
                pltpu.VMEM((2, ROWS, dim), BF16), pltpu.VMEM((2, 2, ROWS, ff), F32),
                pltpu.VMEM((ROWS // 2, dim), BF16), pltpu.VMEM((2, ROWS // 2, ff), F32), pltpu.VMEM((2, toks, dim), F32),
                pltpu.SMEM(((n_tiles + 1) * n_exp,), jnp.int32), pltpu.SMEM((n_exp,), jnp.int32),
                pltpu.SMEM((n_exp + 1,), jnp.int32), pltpu.SMEM((1,), jnp.int32), dma((2,)), dma((2,)), dma((2,)), dma((2,)),
            ],
        ),
        out_shape=[shape((toks, dim), F32)] * depth + [
            shape((blocks, ROWS, dim), BF16), shape((blocks, 2, ROWS, ff), F32),
            shape((n_exp, ROWS // 2, dim), BF16), shape((n_exp, 2, ROWS // 2, ff), F32),
        ],
        compiler_params=pltpu.CompilerParams(dimension_semantics=("arbitrary",), vmem_limit_bytes=64_000_000),
        cost_estimate=pl.CostEstimate(flops=25_000_000_000, bytes_accessed=80_000_000, transcendentals=3_000_000),
        name="forward",
    )(counts, place, plan_col, x_col.reshape(-1, dim), w_gate, w_up, w_down)
    return result[:depth], result[depth:]


def expert_backward(depth, counts, place, plan_col, dy_head, dy_tails, w_gate, w_up, w_down, saved, cap):
    n_tiles, n_exp, rows, blocks = layer_sizes(depth, plan_col.shape[2], w_gate, cap)
    head, dim = dy_head.shape[1:]
    tail = dy_tails[0].shape[0]
    toks = head + tail
    ff = w_gate.shape[2]
    first = lambda i: jnp.minimum(i, depth - 1)
    middle = lambda i: jnp.clip(i - depth, 0, n_exp - 1)
    last = lambda i: jnp.maximum(i - depth - n_exp, 0)

    plan_at = lambda i, counts, place: (jnp.where(i < depth, i, last(i)), place[0], 0)

    wide = pl.BlockSpec((1, dim, ff), lambda i, *_: (middle(i), 0, 0))
    tall = pl.BlockSpec((1, ff, dim), lambda i, *_: (middle(i), 0, 0))
    any_space = pl.BlockSpec(memory_space=pl.ANY)
    shape = jax.ShapeDtypeStruct
    dma = pltpu.SemaphoreType.DMA
    return pl.pallas_call(
        functools.partial(backward_kernel, depth, n_tiles, n_exp),
        grid_spec=pltpu.PrefetchScalarGridSpec(
            num_scalar_prefetch=2,
            grid=(2 * depth + n_exp,),
            in_specs=[
                pl.BlockSpec((1, 2 * n_exp, toks), plan_at),
                pl.BlockSpec((head, dim), lambda i, *_: (first(i), 0)),
                *[pl.BlockSpec((tail, dim), lambda i, *_: (0, 0))] * depth, wide, wide, tall, *[any_space] * 4,
            ],
            out_specs=[
                pl.BlockSpec((toks, dim), lambda i, *_: (last(i), 0)),
                pl.BlockSpec((1, 3 * dim, ff), lambda i, *_: (middle(i), 0, 0)),
            ],
            scratch_shapes=[
                pltpu.VMEM((rows, dim), BF16), pltpu.VMEM((n_exp * WIN, dim), BF16),
                pltpu.VMEM((2, ROWS, dim), BF16), pltpu.VMEM((2, 2, ROWS, ff), F32),
                pltpu.VMEM((ROWS // 2, dim), BF16), pltpu.VMEM((2, ROWS // 2, ff), F32), pltpu.VMEM((toks, dim), BF16),
                pltpu.SMEM(((n_tiles + 1) * n_exp,), jnp.int32), pltpu.SMEM((n_exp,), jnp.int32),
                pltpu.SMEM((n_exp + 1,), jnp.int32), dma((2,)), dma((2,)), dma((2,)),
            ],
        ),
        out_shape=[shape((depth * toks, dim), F32), shape((n_exp, 3 * dim, ff), F32)],
        compiler_params=pltpu.CompilerParams(dimension_semantics=("arbitrary",), vmem_limit_bytes=66_000_000),
        cost_estimate=pl.CostEstimate(flops=50_000_000_000, bytes_accessed=150_000_000, transcendentals=3_000_000),
        name="backward",
    )(counts, place, plan_col, dy_head.reshape(-1, dim), *dy_tails, w_gate, w_up, w_down, *saved)


def finish_kernel(part_refs, dx_ref, g_refs, y_out, dx_out, g_outs, bufs, out_buf, in_sem, out_sem, y_sem):
    moves = [pltpu.make_async_copy(dx_ref, dx_out, out_sem.at[0])]
    moves += [pltpu.make_async_copy(g.at[...], o.at[0], out_sem.at[1 + i]) for i, (g, o) in enumerate(zip(g_refs, g_outs))]
    n = bufs.shape[0]
    rows = bufs.shape[2]
    loads = [
        [pltpu.make_async_copy(p.at[pl.ds(k * rows, rows), :], bufs.at[k, i], in_sem.at[k, i]) for i, p in enumerate(part_refs)]
        for k in range(n)
    ]
    for copies in loads:
        for copy in copies:
            copy.start()
    for move in moves:
        move.start()
    stores = []
    for k in range(n):
        for copy in loads[k]:
            copy.wait()
        value = functools.reduce(jnp.add, [bufs[k, i] for i in range(len(part_refs))])
        out_buf[k] = value.astype(BF16)
        stores.append(pltpu.make_async_copy(out_buf.at[k], y_out.at[pl.ds(k * rows, rows), :], y_sem.at[k]))
        stores[-1].start()
    for copy in moves + stores:
        copy.wait()


def finish(parts, dx, grads):
    toks, dim = dx.shape
    n = 4
    any_space = pl.BlockSpec(memory_space=pl.ANY)
    shape = jax.ShapeDtypeStruct
    dma = pltpu.SemaphoreType.DMA
    k = len(parts)

    def body(*refs):
        finish_kernel(refs[:k], refs[k], refs[k + 1 : k + 4], refs[k + 4], refs[k + 5], refs[k + 6 : k + 9], *refs[k + 9 :])

    return pl.pallas_call(
        body,
        in_specs=[any_space] * (k + 4),
        out_specs=[any_space] * 5,
        out_shape=[shape((toks, dim), BF16), shape((toks, dim), BF16)] + [shape((1, *g.shape), F32) for g in grads],
        scratch_shapes=[
            pltpu.VMEM((n, k, toks // n, dim), F32), pltpu.VMEM((n, toks // n, dim), BF16),
            dma((n, k)), dma((4,)), dma((n,)),
        ],
        compiler_params=pltpu.CompilerParams(vmem_limit_bytes=24_000_000),
        name="finish",
    )(*parts, dx, *grads)


def solution(mesh):
    n_dev = mesh.devices.size
    depth = n_dev // 8
    grid = Mesh(mesh.devices.reshape(depth, 2, 2, 2), ('z', 'y', 'x', 'c'))
    plane = ('y', 'x', 'c')
    spec = P(('z', 'y', 'x', 'c'))

    def local_step(x_tok, route_idx, gates, dy_tok, w_gate, w_up, w_down):
        tok_loc, top_k = route_idx.shape
        cap = depth * (2 * tok_loc * top_k // (n_dev * w_gate.shape[0] - 2))
        n_exp = 8 * w_gate.shape[0]
        head = tok_loc // 16 * HEAD
        x_col, dy_head, dy_tail, plan_col, wg_all, wu_all, wd_all = spread(
            depth, n_dev, head, x_tok, dy_tok, route_idx.T, gates.T, w_gate, w_up, w_down
        )
        turn = lambda a, d: lax.ppermute(a, 'z', [(i, i ^ d) for i in range(depth)])
        dy_tails = [dy_tail] + [turn(dy_tail, d) for d in range(1, depth)]
        place = lax.axis_index('z')
        per = tok_loc // TILE
        counts = lax.dynamic_slice(plan_col, (0, 2 * n_dev, place * n_exp), (depth, per, n_exp))
        where = (counts.reshape(-1).astype(jnp.int32), place.reshape(1), plan_col)
        y_parts, saved = expert_forward(depth, *where, x_col, wg_all, wu_all, wd_all, cap)
        y_parts, dy_tails = lax.optimization_barrier((y_parts, dy_tails))
        y_sum = y_parts[0]
        turned = [turn(y_parts[d], d) for d in range(1, depth)]
        dx_part, grads = expert_backward(
            depth, *where, dy_head, dy_tails, wg_all, wu_all, wd_all, saved, cap
        )
        dx, *dw = collect(depth, dx_part.reshape(depth, tok_loc, -1), grads)
        return tuple(finish([y_sum, *turned], dx, dw))

    return jax.shard_map(local_step, mesh=grid, in_specs=(spec,) * 7, out_specs=(spec,) * 5, check_vma=False)
```
